8 devices in a mesh: rows: 2 (over z, y), terms: 4 (over x, core).
Axes of the slice: x: 2, y: 2, z: 1, core: 2. Of those that a mesh axis runs over, the one named last changes fastest.
Arguments:
- wavefunc: float32 [256, 4, 4, 256], replicated
- left_env: bfloat16 [64, 256, 256], P('terms')
- two_site: bfloat16 [64, 16, 16], P('terms')
- right_env: bfloat16 [64, 256, 256], P('terms', 'rows')
Outputs:
- output 1: float32 [7, 256, 4, 4, 256], P(None, 'terms', None, None, 'rows')
- output 2: float32 [6], replicated
- output 3: float32 [6], replicated
All inputs are finite; a program needn't handle non-finite values.
Results may differ from the reference program's by a relative error of at most 0.0120408.
Values are sent between devices in bfloat16 or wider.
A program may use at most 1 GiB of HBM per device.

```python
import jax
import jax.numpy as jnp
from jax import lax

BOND_DIM = 256
PHYS_DIM = 4
NUM_TERMS = 64
LANCZOS_STEPS = 6


def symmetric_draw(draw_key, term_count, mat_size):
    raw_draw = jax.random.normal(draw_key, (term_count, mat_size, mat_size), jnp.float32)
    return (raw_draw + jnp.swapaxes(raw_draw, 1, 2)) * (2.0 * mat_size) ** -0.5


def setup_inputs(seed: int = 0) -> dict:
    base_key = jax.random.key(seed)
    key_psi, key_left, key_two, key_right, key_shift = jax.random.split(base_key, 5)
    pair_dim = PHYS_DIM * PHYS_DIM
    eye_bond = jnp.eye(BOND_DIM, dtype=jnp.float32)
    eye_pair = jnp.eye(pair_dim, dtype=jnp.float32)
    wavefunc = jax.random.normal(key_psi, (BOND_DIM, PHYS_DIM, PHYS_DIM, BOND_DIM), jnp.float32)
    left_env = (symmetric_draw(key_left, NUM_TERMS, BOND_DIM) + eye_bond).astype(jnp.bfloat16)
    right_env = (symmetric_draw(key_right, NUM_TERMS, BOND_DIM) + eye_bond).astype(jnp.bfloat16)
    shifts = NUM_TERMS ** -0.5 + 0.5 * jax.random.normal(key_shift, (NUM_TERMS,), jnp.float32)
    two_site = ((symmetric_draw(key_two, NUM_TERMS, pair_dim) + shifts[:, None, None] * eye_pair) * NUM_TERMS ** -0.5).astype(jnp.bfloat16)
    return {'wavefunc': wavefunc, 'left_env': left_env, 'two_site': two_site, 'right_env': right_env}


def reference(wavefunc, left_env, two_site, right_env):
    pair_dim = PHYS_DIM * PHYS_DIM
    vec_shape = (BOND_DIM, pair_dim, BOND_DIM)

    def apply_ham(in_vec):
        u_mat = in_vec.astype(jnp.bfloat16).reshape(BOND_DIM * pair_dim, BOND_DIM)

        def add_term(running, term_ops):
            left_mat, two_mat, right_mat = term_ops
            right_part = jnp.dot(u_mat, right_mat.T, preferred_element_type=jnp.float32).astype(jnp.bfloat16)
            mid_part = jnp.einsum('qp,cpb->cqb', two_mat.astype(jnp.float32), right_part.reshape(vec_shape).astype(jnp.float32)).astype(jnp.bfloat16)
            left_part = jnp.dot(left_mat, mid_part.reshape(BOND_DIM, pair_dim * BOND_DIM), preferred_element_type=jnp.float32)
            return running + left_part.reshape(vec_shape), None

        sigma_vec, _ = lax.scan(add_term, jnp.zeros(vec_shape, jnp.float32), (left_env, two_site, right_env))
        return sigma_vec

    init_scale = jnp.sqrt(jnp.mean(wavefunc * wavefunc))
    first_vec = (wavefunc / init_scale).reshape(vec_shape)

    def lanczos_step(state_in, unused):
        prev_vec, cur_vec, prev_beta = state_in
        w_vec = apply_ham(cur_vec)
        alpha_val = jnp.mean(w_vec * cur_vec)
        w_vec = w_vec - alpha_val * cur_vec - prev_beta * prev_vec
        beta_val = jnp.sqrt(jnp.mean(w_vec * w_vec))
        next_vec = w_vec / beta_val
        return (cur_vec, next_vec, beta_val), (next_vec, alpha_val, beta_val)

    start_state = (jnp.zeros(vec_shape, jnp.float32), first_vec, jnp.zeros((), jnp.float32))
    _, (later_vecs, alpha_diag, beta_offdiag) = lax.scan(lanczos_step, start_state, None, length=LANCZOS_STEPS)
    krylov = jnp.concatenate([first_vec[None], later_vecs], axis=0).reshape(LANCZOS_STEPS + 1, BOND_DIM, PHYS_DIM, PHYS_DIM, BOND_DIM)
    return krylov, alpha_diag, beta_offdiag
```

```python
import functools

import jax
import jax.numpy as jnp
from jax import lax
from jax.experimental import pallas as pl
from jax.experimental.pallas import tpu as pltpu
from jax.sharding import PartitionSpec as P

STEPS = 6
PAIR = 16
BOND = 256
TERMS = 64
GROUP = 8
NGROUPS = TERMS // GROUP
HALF = 128
QUART = 64
ELEMS = float(BOND * BOND * PAIR)
F32 = jnp.float32
BF16 = jnp.bfloat16


def lanczos_kernel(
    wf_hbm, left_hbm, two_ref, right_hbm, kry_hbm, ab_ref,
    wfv, rw, lw, bd, wt, mask, yb, zb, uT, acc, rbuf, vb, tmp, st, betas, xs, xr, osb,
    loc_sem, w_ssem, w_rsem, r_ssem, r_rsem, l_ssem, l_rsem, fw_ssem,
    u_ssem, u_rsem, p_ssem, p_rsem, st_ssem, st_rsem, x_ssem, x_rsem, o_sem,
):
    y = lax.axis_index("rows")
    t = lax.axis_index("terms")
    x = t // 2
    c = t % 2
    me = y * 4 + t
    bq = 2 * y + x
    sib = (y, 2 * x + (1 - c))
    xnb = (y, 2 * (1 - x) + c)
    xno = (y, 2 * (1 - x) + (1 - c))
    ynb = (1 - y, t)
    diag = (1 - y, 2 * (1 - x) + c)

    def rdma(src, dst, ssem, rsem, dev):
        return pltpu.make_async_remote_copy(
            src_ref=src, dst_ref=dst, send_sem=ssem, recv_sem=rsem,
            device_id=dev, device_id_type=pl.DeviceIdType.MESH)

    cp_wf = pltpu.make_async_copy(wf_hbm, wfv, loc_sem.at[0])
    cp_r = pltpu.make_async_copy(right_hbm.at[:, pl.ds(64 * x, 64), :], rw.at[pl.ds(0, 16)], loc_sem.at[1])
    cp_l = pltpu.make_async_copy(left_hbm.at[:, pl.ds(128 * c, 128), :], lw.at[pl.ds(0, 16)], loc_sem.at[2])
    cp_wf.start()
    cp_r.start()
    cp_l.start()

    barrier = pltpu.get_barrier_semaphore()
    for q in range(1, 8):
        d = (me + q) % 8
        pl.semaphore_signal(barrier, inc=1, device_id=(d // 4, d % 4), device_id_type=pl.DeviceIdType.MESH)
    pl.semaphore_wait(barrier, 7)

    def l_sib():
        return rdma(left_hbm.at[:, pl.ds(128 * (1 - c), 128), :], lw.at[pl.ds(16, 16)], l_ssem.at[0], l_rsem.at[0], sib)

    def l_dir(i):
        rows = pl.ds(128 * c, 128) if i == 0 else pl.ds(128 * (1 - c), 128)
        return rdma(left_hbm.at[pl.ds(8 * y, 8), rows, :], lw.at[pl.ds(32 + 8 * i, 8)],
                    l_ssem.at[1 + i], l_rsem.at[1 + i], xnb if i == 0 else xno)

    def l_fwd(i):
        return rdma(lw.at[pl.ds(32 + 8 * i, 8)], lw.at[pl.ds(48 + 8 * i, 8)], l_ssem.at[3 + i], l_rsem.at[3 + i], ynb)

    def r_sib():
        return rdma(right_hbm.at[:, pl.ds(64 * x, 64), :], rw.at[pl.ds(16, 16)], r_ssem.at[0], r_rsem.at[0], sib)

    def r_dir(i):
        first = 8 * y if i == 0 else 8 * (1 - y)
        return rdma(right_hbm.at[pl.ds(first, 8), pl.ds(64 * (1 - x), 64), :], rw.at[pl.ds(32 + 16 * i, 8)],
                    r_ssem.at[1 + i], r_rsem.at[1 + i], xnb)

    def r_fwd(i):
        return rdma(rw.at[pl.ds(32 + 16 * i, 8)], rw.at[pl.ds(40 + 16 * i, 8)], r_ssem.at[3 + i], r_rsem.at[3 + i], sib)

    l_dir(0).start()
    l_dir(1).start()
    r_dir(0).start()
    r_dir(1).start()
    r_sib().start()
    l_sib().start()

    row16 = lax.broadcasted_iota(jnp.int32, (PAIR, BOND), 0)
    lane16 = lax.broadcasted_iota(jnp.int32, (PAIR, BOND), 1)
    packed = jnp.zeros((PAIR, BOND), F32)
    for k in range(16):
        place = (lane16 == row16 + 16 * k).astype(F32).astype(BF16)
        packed = packed + jnp.dot(two_ref[k], place, preferred_element_type=F32)
    wt[0] = packed.astype(BF16)

    def w_send(i):
        return rdma(wt.at[0], wt.at[1 + i], w_ssem.at[i], w_rsem.at[i], (sib, xnb, xno)[i])

    for i in range(3):
        w_send(i).start()

    rr = lax.broadcasted_iota(jnp.int32, (BOND, BOND), 0) % 16
    cc = lax.broadcasted_iota(jnp.int32, (BOND, BOND), 1) % 16
    mask[...] = (rr == cc).astype(F32)

    cp_wf.wait()

    def sumsq(i, s):
        blk = wfv[pl.ds(pl.multiple_of(i * 256, 256), 256), :]
        return s + jnp.sum((blk * blk).reshape(32, 8, 128), axis=0)

    total = lax.fori_loop(0, 32, sumsq, jnp.zeros((8, 128), F32))
    total = jnp.sum(jnp.sum(total, axis=1, keepdims=True), axis=0, keepdims=True)
    scale = jnp.broadcast_to(jnp.sqrt(total * (1.0 / ELEMS)), (1, 128))

    wfh = wfv.at[pl.ds(pl.multiple_of(4096 * c, 4096), 4096), :]
    wfo = wfv.at[pl.ds(pl.multiple_of(2048 * t, 2048), 2048), :]
    for p in range(PAIR):
        for bt in range(2):
            first = (p // 4) * 8 + bt * 4 + p % 4
            blk = (wfh[pl.ds(first, 128, stride=32), :] / scale).T
            tmp[bt] = blk
            uT[p, pl.ds(128 * bt, 128), :] = blk.astype(BF16)
        vb[0, p] = tmp[y, pl.ds(pl.multiple_of(64 * x, 64), 64), :]
        first = (p // 4) * 8 + p % 4
        lo = wfo[pl.ds(first, 64, stride=32), :]
        hi = wfo[pl.ds(first + 4, 64, stride=32), :]
        osb[p] = jnp.where(y == 0, lo, hi) / scale
    vb[2] = jnp.zeros((PAIR, QUART, HALF), F32)
    betas[...] = jnp.zeros((1, 128), F32)

    def out_copy(j):
        return pltpu.make_async_copy(osb, kry_hbm.at[j], o_sem.at[0])

    out_copy(0).start()

    def u_copy(n, s):
        part = uT.at[pl.ds(2 * n, 2), pl.ds(pl.multiple_of(64 * bq, 64), 64), :]
        return rdma(part, part, u_ssem.at[n, s], u_rsem.at[n, s], (xnb, ynb, diag)[s])

    def u_wait_recv(n, s):
        src = (2 * y + (1 - x), 2 * (1 - y) + x, 2 * (1 - y) + (1 - x))[s]
        part = uT.at[pl.ds(2 * n, 2), pl.ds(pl.multiple_of(64 * src, 64), 64), :]
        rdma(part, part, u_ssem.at[n, s], u_rsem.at[n, s], (xnb, ynb, diag)[s]).wait_recv()

    def r_stage(k0, nk, n):
        lhs = rw[pl.ds(k0, nk)].reshape(nk * QUART, BOND)
        rhs = jnp.concatenate([uT[2 * n], uT[2 * n + 1]], axis=1)
        res = jnp.dot(lhs, rhs, preferred_element_type=F32).astype(BF16)
        yb[pl.ds(k0, nk), 2 * n] = res[:, :HALF].reshape(nk, QUART, HALF)
        yb[pl.ds(k0, nk), 2 * n + 1] = res[:, HALF:].reshape(nk, QUART, HALF)

    def wl_stage(g):
        k0 = g * GROUP
        for k in range(GROUP):
            mat = bd[k0 + k]
            for h in range(2):
                rhs = jnp.concatenate(
                    [yb[k0 + k, :, pl.ds(32 * h + 16 * i, 16), :].reshape(BOND, HALF) for i in range(2)], axis=1)
                res = jnp.dot(mat, rhs, preferred_element_type=F32).astype(BF16)
                for i in range(2):
                    zb[:, pl.ds(32 * h + 16 * i, 16), pl.ds(HALF * k, HALF)] = (
                        res[:, HALF * i:HALF * (i + 1)].reshape(PAIR, 16, HALF))
        lhs = zb[...].reshape(PAIR * QUART, GROUP * HALF)
        rhs = lw[pl.ds(k0, GROUP)].reshape(GROUP * HALF, BOND)
        res = jnp.dot(lhs, rhs, preferred_element_type=F32)
        acc[0] = acc[0] + res[:, :HALF].reshape(PAIR, QUART, HALF)
        acc[1] = acc[1] + res[:, HALF:].reshape(PAIR, QUART, HALF)

    def build_bd(g):
        slot = (g // 4) * 2 + (1 - g // 4) * (g // 2) + (g // 4) * (g % 2)
        part = (1 - g // 4) * (g % 2) + (g // 4) * ((y + (g - 4 * (g // 4)) // 2) % 2)
        lanes = pl.multiple_of(128 * part, 128)
        ops = wt[slot, :, pl.ds(lanes, 128)].astype(F32).T.astype(BF16)
        e_t = (lax.broadcasted_iota(jnp.int32, (PAIR, BOND), 1) // 16
               == lax.broadcasted_iota(jnp.int32, (PAIR, BOND), 0)).astype(F32).astype(BF16)
        e = (lax.broadcasted_iota(jnp.int32, (BOND, PAIR), 0) // 16
             == lax.broadcasted_iota(jnp.int32, (BOND, PAIR), 1)).astype(F32).astype(BF16)
        wide = jnp.dot(ops, e_t, preferred_element_type=F32).astype(BF16)
        for k in range(GROUP):
            full = jnp.dot(e, wide[16 * k:16 * (k + 1), :], preferred_element_type=F32)
            bd[g * GROUP + k] = (full * mask[...]).astype(BF16)

    def first_group(g, carry):
        @pl.when(g == 0)
        def _():
            cp_r.wait()
            cp_l.wait()

        @pl.when(g == 2)
        def _():
            w_send(0).wait_recv()
            r_sib().wait_recv()
            l_sib().wait_recv()

        @pl.when(g == 4)
        def _():
            w_send(1).wait_recv()
            w_send(2).wait_recv()
            l_dir(0).wait_recv()
            l_fwd(0).start()
            l_dir(1).wait_recv()
            l_fwd(1).start()
            r_dir(0).wait_recv()
            r_fwd(0).start()

        @pl.when(g == 5)
        def _():
            r_fwd(0).wait_recv()

        @pl.when(g == 6)
        def _():
            r_dir(1).wait_recv()
            r_fwd(1).start()
            l_fwd(0).wait_recv()

        @pl.when(g == 7)
        def _():
            r_fwd(1).wait_recv()
            l_fwd(1).wait_recv()

        build_bd(g)
        for n in range(8):
            r_stage(g * GROUP, GROUP, n)
        wl_stage(g)
        return carry

    def later_r(n, carry):
        for s in range(3):
            u_wait_recv(n, s)
        for i in range(4):
            r_stage(16 * i, 16, n)
        for s in range(3):
            u_copy(n, s).wait_send()
        return carry

    def later_wl(g, carry):
        wl_stage(g)
        return carry

    def part_copy():
        return rdma(acc.at[1 - c], rbuf, p_ssem.at[0], p_rsem.at[0], sib)

    def x_copy(par, h):
        return rdma(xs.at[h], xr.at[par, x], x_ssem.at[h], x_rsem.at[par, x], (y, 2 * c + h))

    def x_recv(par, slot):
        rdma(xs.at[0], xr.at[par, slot], x_ssem.at[0], x_rsem.at[par, slot], xnb).wait_recv()

    def x_wait_send(par):
        @pl.when(c == x)
        def _():
            x_copy(par, 1 - c).wait_send()

        @pl.when(c != x)
        def _():
            x_copy(par, 0).wait_send()
            x_copy(par, 1).wait_send()

    def put_out(vec, par):
        for i in range(8):
            blk = jnp.concatenate([vb[vec, i], vb[vec, i + 8]], axis=0).T
            xs[0, i] = blk[:64]
            xs[1, i] = blk[64:]

        @pl.when(c == x)
        def _():
            xr[par, x] = xs[c]
            x_copy(par, 1 - c).start()

        @pl.when(c != x)
        def _():
            x_copy(par, 0).start()
            x_copy(par, 1).start()

    def merge_out(j, par):
        x_recv(par, 1 - x)

        @pl.when(c != x)
        def _():
            x_recv(par, x)

        out_copy(0).wait()
        low = lax.broadcasted_iota(jnp.int32, (64, 128), 1) < 64
        for i in range(8):
            p0 = xr[par, 0, i]
            p1 = xr[par, 1, i]
            osb[i] = jnp.where(low, p0, pltpu.roll(p1, 64, 1))
            osb[i + 8] = jnp.where(low, pltpu.roll(p0, 64, 1), p1)
        out_copy(j).start()

    def everywhere(s):
        s = jnp.sum(jnp.sum(s, axis=1, keepdims=True), axis=0, keepdims=True)
        return jnp.broadcast_to(s, (1, 128))

    def fold(v):
        return jnp.sum(v.reshape(8, 8, 128), axis=0)

    def step(j, carry):
        acc[...] = jnp.zeros((2, PAIR, QUART, HALF), F32)

        @pl.when(j == 0)
        def _():
            lax.fori_loop(0, NGROUPS, first_group, 0)

        @pl.when(j > 0)
        def _():
            lax.fori_loop(0, 8, later_r, 0)
            lax.fori_loop(0, NGROUPS, later_wl, 0)

        part_copy().start()
        cur = j % 3
        prev = (j + 2) % 3
        nxt = (j + 1) % 3
        par = j % 2
        beta_prev = betas[...]
        part_copy().wait_recv()

        zero = jnp.zeros((8, 128), F32)

        def pass1(p, s):
            a_s, t_s, v_s = s
            w = acc[c, p] + rbuf[p]
            v = vb[cur, p]
            r = w - beta_prev * vb[prev, p]
            vb[nxt, p] = r
            return a_s + fold(w * v), t_s + fold(r * v), v_s + fold(v * v)

        a_s, t_s, v_s = lax.fori_loop(0, PAIR, pass1, (zero, zero, zero))
        a_d, t_d, v_d = everywhere(a_s), everywhere(t_s), everywhere(v_s)
        shift = jnp.where(v_d > 0.0, t_d / jnp.where(v_d > 0.0, v_d, 1.0), 0.0)

        def pass2(p, s):
            q_s, p_s = s
            v = vb[cur, p]
            r = vb[nxt, p] - shift * v
            vb[nxt, p] = r
            return q_s + fold(r * r), p_s + fold(r * v)

        q_s, p_s = lax.fori_loop(0, PAIR, pass2, (zero, zero))
        st[par, me] = jnp.concatenate(
            [a_d, shift, v_d, everywhere(q_s), everywhere(p_s), jnp.zeros((3, 128), F32)], axis=0)

        def st_copy(q):
            d = (me + q) % 8
            return rdma(st.at[par, me], st.at[par, me], st_ssem.at[q - 1], st_rsem.at[q - 1], (d // 4, d % 4))

        for q in range(1, 8):
            st_copy(q).start()
        part_copy().wait_send()
        for q in range(1, 8):
            src = (me + 8 - q) % 8
            rdma(st.at[par, me], st.at[par, src], st_ssem.at[q - 1], st_rsem.at[q - 1], sib).wait_recv()

        alpha = st[par, 0][0:1]
        for d in range(1, 8):
            alpha = alpha + st[par, d][0:1]
        alpha = alpha * (1.0 / ELEMS)
        beta2 = jnp.zeros((1, 128), F32)
        for d in range(8):
            tile = st[par, d]
            gap = alpha - tile[1:2]
            beta2 = beta2 + (tile[3:4] - 2.0 * gap * tile[4:5] + gap * gap * tile[2:3])
        beta = jnp.sqrt(beta2 * (1.0 / ELEMS))
        betas[...] = beta
        ab_ref[j] = jnp.concatenate([alpha, beta, jnp.zeros((6, 128), F32)], axis=0)
        gap = alpha - shift

        def pass3(n, carry):
            for i in range(2):
                p = 2 * n + i
                v = (vb[nxt, p] - gap * vb[cur, p]) / beta
                vb[nxt, p] = v
                uT[p, pl.ds(pl.multiple_of(64 * bq, 64), 64), :] = v.astype(BF16)

            @pl.when(j < STEPS - 1)
            def _():
                for s in range(3):
                    u_copy(n, s).start()

            return carry

        lax.fori_loop(0, 8, pass3, 0)

        @pl.when(j > 0)
        def _():
            x_wait_send(1 - par)

        put_out(nxt, par)

        @pl.when(j > 0)
        def _():
            merge_out(j, 1 - par)

        for q in range(1, 8):
            st_copy(q).wait_send()
        return carry

    lax.fori_loop(0, STEPS, step, 0)

    last = (STEPS - 1) % 2
    x_wait_send(last)
    merge_out(STEPS, last)
    out_copy(0).wait()

    for i in range(3):
        w_send(i).wait_send()
    l_sib().wait_send()
    r_sib().wait_send()
    for i in range(2):
        l_dir(i).wait_send()
        l_fwd(i).wait_send()
        r_dir(i).wait_send()
        r_fwd(i).wait_send()


def solution(mesh):
    def body_fn(wavefunc, left_loc, two_loc, right_loc):
        bond, phys = wavefunc.shape[0], wavefunc.shape[1]
        wf = wavefunc.reshape(bond, phys, phys, 2, 128).transpose(0, 1, 3, 2, 4).reshape(-1, 128)
        dma = pltpu.SemaphoreType.DMA
        kry, ab = pl.pallas_call(
            lanczos_kernel,
            out_shape=(
                jax.ShapeDtypeStruct((STEPS + 1, PAIR, 64, 128), F32),
                jax.ShapeDtypeStruct((STEPS, 8, 128), F32),
            ),
            in_specs=[
                pl.BlockSpec(memory_space=pl.ANY),
                pl.BlockSpec(memory_space=pl.ANY),
                pl.BlockSpec(memory_space=pltpu.VMEM),
                pl.BlockSpec(memory_space=pl.ANY),
            ],
            out_specs=(pl.BlockSpec(memory_space=pl.ANY), pl.BlockSpec(memory_space=pltpu.VMEM)),
            scratch_shapes=[
                pltpu.VMEM((8192, 128), F32),
                pltpu.VMEM((TERMS, QUART, BOND), BF16),
                pltpu.VMEM((TERMS, HALF, BOND), BF16),
                pltpu.VMEM((TERMS, BOND, BOND), BF16),
                pltpu.VMEM((4, PAIR, BOND), BF16),
                pltpu.VMEM((BOND, BOND), F32),
                pltpu.VMEM((TERMS, PAIR, QUART, HALF), BF16),
                pltpu.VMEM((PAIR, QUART, GROUP * HALF), BF16),
                pltpu.VMEM((PAIR, BOND, HALF), BF16),
                pltpu.VMEM((2, PAIR, QUART, HALF), F32),
                pltpu.VMEM((PAIR, QUART, HALF), F32),
                pltpu.VMEM((3, PAIR, QUART, HALF), F32),
                pltpu.VMEM((2, 128, 128), F32),
                pltpu.VMEM((2, 8, 8, 128), F32),
                pltpu.VMEM((1, 128), F32),
                pltpu.VMEM((2, 8, 64, 128), F32),
                pltpu.VMEM((2, 2, 8, 64, 128), F32),
                pltpu.VMEM((PAIR, 64, 128), F32),
                dma((3,)),
                dma((3,)), dma((3,)),
                dma((5,)), dma((5,)),
                dma((5,)), dma((5,)),
                dma((1,)),
                dma((8, 3)), dma((8, 3)),
                dma((1,)), dma((1,)),
                dma((7,)), dma((7,)),
                dma((2,)), dma((2, 2)),
                dma((1,)),
            ],
            compiler_params=pltpu.CompilerParams(
                collective_id=0, has_side_effects=True, vmem_limit_bytes=66 * 1000 * 1000),
        )(wf, left_loc, two_loc, right_loc)
        krylov = kry.transpose(0, 2, 1, 3).reshape(STEPS + 1, 64, phys, phys, 128)
        return krylov, ab[:, 0, 0], ab[:, 1, 0]

    return jax.shard_map(
        body_fn, mesh=mesh,
        in_specs=(P(), P('terms'), P('terms'), P('terms', 'rows')),
        out_specs=(P(None, 'terms', None, None, 'rows'), P(), P()), check_vma=False)
```

```python
import functools

import jax
import jax.numpy as jnp
from jax import lax
from jax.experimental import pallas as pl
from jax.experimental.pallas import tpu as pltpu
from jax.sharding import PartitionSpec as P

STEPS = 6
PAIR = 16
BOND = 256
TERMS = 64
GROUP = 8
NGROUPS = TERMS // GROUP
HALF = 128
QUART = 64
AHEAD = 3
LAG = 2
ELEMS = float(BOND * BOND * PAIR)
F32 = jnp.float32
BF16 = jnp.bfloat16


def lanczos_kernel(
    wf_hbm, left_hbm, two_ref, right_hbm, kry_hbm, ab_ref,
    wfv, rw, lw, bd, wt, mask, yb, zb, uT, acc, rbuf, vb, tmp, st, betas, xs, xr, osb,
    loc_sem, w_ssem, w_rsem, r_ssem, r_rsem, l_ssem, l_rsem, fw_ssem,
    u_ssem, u_rsem, p_ssem, p_rsem, st_ssem, st_rsem, x_ssem, x_rsem, o_sem,
):
    y = lax.axis_index("rows")
    t = lax.axis_index("terms")
    x = t // 2
    c = t % 2
    me = y * 4 + t
    bq = 2 * y + x
    sib = (y, 2 * x + (1 - c))
    xnb = (y, 2 * (1 - x) + c)
    xno = (y, 2 * (1 - x) + (1 - c))
    ynb = (1 - y, t)

    def rdma(src, dst, ssem, rsem, dev):
        return pltpu.make_async_remote_copy(
            src_ref=src, dst_ref=dst, send_sem=ssem, recv_sem=rsem,
            device_id=dev, device_id_type=pl.DeviceIdType.MESH)

    cp_wf = pltpu.make_async_copy(wf_hbm, wfv, loc_sem.at[0])
    cp_r = pltpu.make_async_copy(right_hbm.at[:, pl.ds(64 * x, 64), :], rw.at[pl.ds(0, 16)], loc_sem.at[1])
    cp_l = pltpu.make_async_copy(left_hbm.at[:, pl.ds(128 * c, 128), :], lw.at[pl.ds(0, 16)], loc_sem.at[2])
    cp_wf.start()
    cp_r.start()
    cp_l.start()

    barrier = pltpu.get_barrier_semaphore()
    for q in range(1, 8):
        d = (me + q) % 8
        pl.semaphore_signal(barrier, inc=1, device_id=(d // 4, d % 4), device_id_type=pl.DeviceIdType.MESH)
    pl.semaphore_wait(barrier, 7)

    def l_sib():
        return rdma(left_hbm.at[:, pl.ds(128 * (1 - c), 128), :], lw.at[pl.ds(16, 16)], l_ssem.at[0], l_rsem.at[0], sib)

    def l_dir(i):
        rows = pl.ds(128 * c, 128) if i == 0 else pl.ds(128 * (1 - c), 128)
        return rdma(left_hbm.at[pl.ds(8 * y, 8), rows, :], lw.at[pl.ds(32 + 8 * i, 8)],
                    l_ssem.at[1 + i], l_rsem.at[1 + i], xnb if i == 0 else xno)

    def l_fwd(i):
        return rdma(lw.at[pl.ds(32 + 8 * i, 8)], lw.at[pl.ds(48 + 8 * i, 8)], l_ssem.at[3 + i], l_rsem.at[3 + i], ynb)

    def r_sib():
        return rdma(right_hbm.at[:, pl.ds(64 * x, 64), :], rw.at[pl.ds(16, 16)], r_ssem.at[0], r_rsem.at[0], sib)

    def r_dir(i):
        first = 8 * y if i == 0 else 8 * (1 - y)
        return rdma(right_hbm.at[pl.ds(first, 8), pl.ds(64 * (1 - x), 64), :], rw.at[pl.ds(32 + 16 * i, 8)],
                    r_ssem.at[1 + i], r_rsem.at[1 + i], xnb)

    def r_fwd(i):
        return rdma(rw.at[pl.ds(32 + 16 * i, 8)], rw.at[pl.ds(40 + 16 * i, 8)], r_ssem.at[3 + i], r_rsem.at[3 + i], sib)

    l_dir(0).start()
    l_dir(1).start()
    r_dir(0).start()
    r_dir(1).start()
    r_sib().start()
    l_sib().start()

    row16 = lax.broadcasted_iota(jnp.int32, (PAIR, BOND), 0)
    lane16 = lax.broadcasted_iota(jnp.int32, (PAIR, BOND), 1)
    packed = jnp.zeros((PAIR, BOND), F32)
    for k in range(16):
        place = (lane16 == row16 + 16 * k).astype(F32).astype(BF16)
        packed = packed + jnp.dot(two_ref[k], place, preferred_element_type=F32)
    wt[0] = packed.astype(BF16)

    def w_send(i):
        return rdma(wt.at[0], wt.at[1 + i], w_ssem.at[i], w_rsem.at[i], (sib, xnb, xno)[i])

    for i in range(3):
        w_send(i).start()

    rr = lax.broadcasted_iota(jnp.int32, (BOND, BOND), 0) % 16
    cc = lax.broadcasted_iota(jnp.int32, (BOND, BOND), 1) % 16
    mask[...] = (rr == cc).astype(F32)

    cp_wf.wait()

    def sumsq(i, s):
        blk = wfv[pl.ds(pl.multiple_of(i * 256, 256), 256), :]
        return s + jnp.sum((blk * blk).reshape(32, 8, 128), axis=0)

    total = lax.fori_loop(0, 32, sumsq, jnp.zeros((8, 128), F32))
    total = jnp.sum(jnp.sum(total, axis=1, keepdims=True), axis=0, keepdims=True)
    scale = jnp.broadcast_to(jnp.sqrt(total * (1.0 / ELEMS)), (1, 128))

    wfh = wfv.at[pl.ds(pl.multiple_of(4096 * c, 4096), 4096), :]
    wfo = wfv.at[pl.ds(pl.multiple_of(2048 * t, 2048), 2048), :]
    for p in range(PAIR):
        for bt in range(2):
            first = (p // 4) * 8 + bt * 4 + p % 4
            blk = (wfh[pl.ds(first, 128, stride=32), :] / scale).T
            tmp[bt] = blk
            uT[p, pl.ds(128 * bt, 128), :] = blk.astype(BF16)
        vb[0, p] = tmp[y, pl.ds(pl.multiple_of(64 * x, 64), 64), :]
        first = (p // 4) * 8 + p % 4
        lo = wfo[pl.ds(first, 64, stride=32), :]
        hi = wfo[pl.ds(first + 4, 64, stride=32), :]
        osb[p] = jnp.where(y == 0, lo, hi) / scale
    vb[2] = jnp.zeros((PAIR, QUART, HALF), F32)
    betas[...] = jnp.zeros((1, 128), F32)

    def out_copy(j):
        return pltpu.make_async_copy(osb, kry_hbm.at[j], o_sem.at[0])

    out_copy(0).start()

    def u_part(n, quarter):
        return uT.at[pl.ds(2 * n, 2), pl.ds(pl.multiple_of(64 * quarter, 64), 64), :]

    def u_own(n, s):
        part = u_part(n, bq)
        return rdma(part, part, u_ssem.at[n, s], u_rsem.at[n, s], (xnb, ynb)[s])

    def u_got(n, s):
        part = u_part(n, (2 * y + (1 - x), 2 * (1 - y) + x)[s])
        return rdma(part, part, u_ssem.at[n, s], u_rsem.at[n, s], (xnb, ynb)[s])

    def u_fwd(n):
        odd = n % 2
        part = u_part(n, (1 - odd) * (2 * y + (1 - x)) + odd * (2 * (1 - y) + x))
        dev = ((1 - odd) * (1 - y) + odd * y, 2 * ((1 - odd) * x + odd * (1 - x)) + c)
        return rdma(part, part, u_ssem.at[n, 2], u_rsem.at[n, 2], dev)

    def u_diag(n):
        part = u_part(n, 2 * (1 - y) + (1 - x))
        return rdma(part, part, u_ssem.at[n, 2], u_rsem.at[n, 2], xnb)

    def r_stage(k0, nk, n):
        lhs = rw[pl.ds(k0, nk)].reshape(nk * QUART, BOND)
        rhs = jnp.concatenate([uT[2 * n], uT[2 * n + 1]], axis=1)
        res = jnp.dot(lhs, rhs, preferred_element_type=F32).astype(BF16)
        yb[pl.ds(k0, nk), 2 * n] = res[:, :HALF].reshape(nk, QUART, HALF)
        yb[pl.ds(k0, nk), 2 * n + 1] = res[:, HALF:].reshape(nk, QUART, HALF)

    def wl_stage(g):
        k0 = g * GROUP
        for k in range(GROUP):
            mat = bd[k0 + k]
            for h in range(2):
                rhs = jnp.concatenate(
                    [yb[k0 + k, :, pl.ds(32 * h + 16 * i, 16), :].reshape(BOND, HALF) for i in range(2)], axis=1)
                res = jnp.dot(mat, rhs, preferred_element_type=F32).astype(BF16)
                for i in range(2):
                    zb[:, pl.ds(32 * h + 16 * i, 16), pl.ds(HALF * k, HALF)] = (
                        res[:, HALF * i:HALF * (i + 1)].reshape(PAIR, 16, HALF))
        lhs = zb[...].reshape(PAIR * QUART, GROUP * HALF)
        rhs = lw[pl.ds(k0, GROUP)].reshape(GROUP * HALF, BOND)
        res = jnp.dot(lhs, rhs, preferred_element_type=F32)
        acc[0] = acc[0] + res[:, :HALF].reshape(PAIR, QUART, HALF)
        acc[1] = acc[1] + res[:, HALF:].reshape(PAIR, QUART, HALF)

    def build_bd(g):
        slot = (g // 4) * 2 + (1 - g // 4) * (g // 2) + (g // 4) * (g % 2)
        part = (1 - g // 4) * (g % 2) + (g // 4) * ((y + (g - 4 * (g // 4)) // 2) % 2)
        lanes = pl.multiple_of(128 * part, 128)
        ops = wt[slot, :, pl.ds(lanes, 128)].astype(F32).T.astype(BF16)
        e_t = (lax.broadcasted_iota(jnp.int32, (PAIR, BOND), 1) // 16
               == lax.broadcasted_iota(jnp.int32, (PAIR, BOND), 0)).astype(F32).astype(BF16)
        e = (lax.broadcasted_iota(jnp.int32, (BOND, PAIR), 0) // 16
             == lax.broadcasted_iota(jnp.int32, (BOND, PAIR), 1)).astype(F32).astype(BF16)
        wide = jnp.dot(ops, e_t, preferred_element_type=F32).astype(BF16)
        for k in range(GROUP):
            full = jnp.dot(e, wide[16 * k:16 * (k + 1), :], preferred_element_type=F32)
            bd[g * GROUP + k] = (full * mask[...]).astype(BF16)

    def first_group(g, carry):
        @pl.when(g == 0)
        def _():
            cp_r.wait()
            cp_l.wait()

        @pl.when(g == 2)
        def _():
            w_send(0).wait_recv()
            r_sib().wait_recv()
            l_sib().wait_recv()

        @pl.when(g == 4)
        def _():
            w_send(1).wait_recv()
            w_send(2).wait_recv()
            l_dir(0).wait_recv()
            l_fwd(0).start()
            l_dir(1).wait_recv()
            l_fwd(1).start()
            r_dir(0).wait_recv()
            r_fwd(0).start()

        @pl.when(g == 5)
        def _():
            r_fwd(0).wait_recv()

        @pl.when(g == 6)
        def _():
            r_dir(1).wait_recv()
            r_fwd(1).start()
            l_fwd(0).wait_recv()

        @pl.when(g == 7)
        def _():
            r_fwd(1).wait_recv()
            l_fwd(1).wait_recv()

        build_bd(g)
        for n in range(8):
            r_stage(g * GROUP, GROUP, n)
        wl_stage(g)
        return carry

    def later_r(i, carry):
        @pl.when(i < 8)
        def _():
            u_got(i, 0).wait_recv()
            u_got(i, 1).wait_recv()
            u_fwd(i).start()

        @pl.when(i < 8 - AHEAD)
        def _():
            u_own(i + AHEAD, 0).start()
            u_own(i + AHEAD, 1).start()

        @pl.when(i >= LAG)
        def _():
            n = i - LAG
            u_diag(n).wait_recv()
            for k in range(4):
                r_stage(16 * k, 16, n)
            u_own(n, 0).wait_send()
            u_own(n, 1).wait_send()
            u_fwd(n).wait_send()

        return carry

    def later_wl(g, carry):
        wl_stage(g)
        return carry

    def part_copy():
        return rdma(acc.at[1 - c], rbuf, p_ssem.at[0], p_rsem.at[0], sib)

    def x_copy(par, h):
        return rdma(xs.at[h], xr.at[par, x], x_ssem.at[h], x_rsem.at[par, x], (y, 2 * c + h))

    def x_recv(par, slot):
        rdma(xs.at[0], xr.at[par, slot], x_ssem.at[0], x_rsem.at[par, slot], xnb).wait_recv()

    def x_wait_send(par):
        @pl.when(c == x)
        def _():
            x_copy(par, 1 - c).wait_send()

        @pl.when(c != x)
        def _():
            x_copy(par, 0).wait_send()
            x_copy(par, 1).wait_send()

    def put_out(vec, par):
        for i in range(8):
            blk = jnp.concatenate([vb[vec, i], vb[vec, i + 8]], axis=0).T
            xs[0, i] = blk[:64]
            xs[1, i] = blk[64:]

        @pl.when(c == x)
        def _():
            xr[par, x] = xs[c]

    def x_start(par):
        @pl.when(c == x)
        def _():
            x_copy(par, 1 - c).start()

        @pl.when(c != x)
        def _():
            x_copy(par, 0).start()
            x_copy(par, 1).start()

    def merge_out(j, par):
        x_recv(par, 1 - x)

        @pl.when(c != x)
        def _():
            x_recv(par, x)

        out_copy(0).wait()
        low = lax.broadcasted_iota(jnp.int32, (64, 128), 1) < 64
        for i in range(8):
            p0 = xr[par, 0, i]
            p1 = xr[par, 1, i]
            osb[i] = jnp.where(low, p0, pltpu.roll(p1, 64, 1))
            osb[i + 8] = jnp.where(low, pltpu.roll(p0, 64, 1), p1)
        out_copy(j).start()

    def everywhere(s):
        s = jnp.sum(jnp.sum(s, axis=1, keepdims=True), axis=0, keepdims=True)
        return jnp.broadcast_to(s, (1, 128))

    def fold(v):
        return jnp.sum(v.reshape(8, 8, 128), axis=0)

    def step(j, carry):
        acc[...] = jnp.zeros((2, PAIR, QUART, HALF), F32)

        @pl.when(j == 0)
        def _():
            lax.fori_loop(0, NGROUPS, first_group, 0)

        @pl.when(j > 0)
        def _():
            lax.fori_loop(0, 8 + LAG, later_r, 0)
            x_start((j + 1) % 2)
            lax.fori_loop(0, NGROUPS, later_wl, 0)

        part_copy().start()
        cur = j % 3
        prev = (j + 2) % 3
        nxt = (j + 1) % 3
        par = j % 2
        beta_prev = betas[...]
        part_copy().wait_recv()

        zero = jnp.zeros((8, 128), F32)

        def pass1(p, s):
            a_s, t_s, v_s = s
            w = acc[c, p] + rbuf[p]
            v = vb[cur, p]
            r = w - beta_prev * vb[prev, p]
            vb[nxt, p] = r
            return a_s + fold(w * v), t_s + fold(r * v), v_s + fold(v * v)

        a_s, t_s, v_s = lax.fori_loop(0, PAIR, pass1, (zero, zero, zero))
        a_d, t_d, v_d = everywhere(a_s), everywhere(t_s), everywhere(v_s)
        shift = jnp.where(v_d > 0.0, t_d / jnp.where(v_d > 0.0, v_d, 1.0), 0.0)

        def pass2(p, s):
            q_s, p_s = s
            v = vb[cur, p]
            r = vb[nxt, p] - shift * v
            vb[nxt, p] = r
            return q_s + fold(r * r), p_s + fold(r * v)

        q_s, p_s = lax.fori_loop(0, PAIR, pass2, (zero, zero))
        st[par, me] = jnp.concatenate(
            [a_d, shift, v_d, everywhere(q_s), everywhere(p_s), jnp.zeros((3, 128), F32)], axis=0)

        def st_copy(q):
            d = (me + q) % 8
            return rdma(st.at[par, me], st.at[par, me], st_ssem.at[q - 1], st_rsem.at[q - 1], (d // 4, d % 4))

        for q in range(1, 8):
            st_copy(q).start()
        part_copy().wait_send()
        for q in range(1, 8):
            src = (me + 8 - q) % 8
            rdma(st.at[par, me], st.at[par, src], st_ssem.at[q - 1], st_rsem.at[q - 1], sib).wait_recv()

        alpha = st[par, 0][0:1]
        for d in range(1, 8):
            alpha = alpha + st[par, d][0:1]
        alpha = alpha * (1.0 / ELEMS)
        beta2 = jnp.zeros((1, 128), F32)
        for d in range(8):
            tile = st[par, d]
            gap = alpha - tile[1:2]
            beta2 = beta2 + (tile[3:4] - 2.0 * gap * tile[4:5] + gap * gap * tile[2:3])
        beta = jnp.sqrt(beta2 * (1.0 / ELEMS))
        betas[...] = beta
        ab_ref[j] = jnp.concatenate([alpha, beta, jnp.zeros((6, 128), F32)], axis=0)
        gap = alpha - shift

        def pass3(n, carry):
            for i in range(2):
                p = 2 * n + i
                v = (vb[nxt, p] - gap * vb[cur, p]) / beta
                vb[nxt, p] = v
                uT[p, pl.ds(pl.multiple_of(64 * bq, 64), 64), :] = v.astype(BF16)

            @pl.when((j < STEPS - 1) & (n < AHEAD))
            def _():
                u_own(n, 0).start()
                u_own(n, 1).start()

            return carry

        lax.fori_loop(0, 8, pass3, 0)

        @pl.when(j > 0)
        def _():
            x_wait_send(1 - par)

        put_out(nxt, par)

        @pl.when(j > 0)
        def _():
            merge_out(j, 1 - par)

        for q in range(1, 8):
            st_copy(q).wait_send()
        return carry

    lax.fori_loop(0, STEPS, step, 0)

    last = (STEPS - 1) % 2
    x_start(last)
    x_wait_send(last)
    merge_out(STEPS, last)
    out_copy(0).wait()

    for i in range(3):
        w_send(i).wait_send()
    l_sib().wait_send()
    r_sib().wait_send()
    for i in range(2):
        l_dir(i).wait_send()
        l_fwd(i).wait_send()
        r_dir(i).wait_send()
        r_fwd(i).wait_send()


def solution(mesh):
    def body_fn(wavefunc, left_loc, two_loc, right_loc):
        bond, phys = wavefunc.shape[0], wavefunc.shape[1]
        wf = wavefunc.reshape(bond, phys, phys, 2, 128).transpose(0, 1, 3, 2, 4).reshape(-1, 128)
        dma = pltpu.SemaphoreType.DMA
        kry, ab = pl.pallas_call(
            lanczos_kernel,
            out_shape=(
                jax.ShapeDtypeStruct((STEPS + 1, PAIR, 64, 128), F32),
                jax.ShapeDtypeStruct((STEPS, 8, 128), F32),
            ),
            in_specs=[
                pl.BlockSpec(memory_space=pl.ANY),
                pl.BlockSpec(memory_space=pl.ANY),
                pl.BlockSpec(memory_space=pltpu.VMEM),
                pl.BlockSpec(memory_space=pl.ANY),
            ],
            out_specs=(pl.BlockSpec(memory_space=pl.ANY), pl.BlockSpec(memory_space=pltpu.VMEM)),
            scratch_shapes=[
                pltpu.VMEM((8192, 128), F32),
                pltpu.VMEM((TERMS, QUART, BOND), BF16),
                pltpu.VMEM((TERMS, HALF, BOND), BF16),
                pltpu.VMEM((TERMS, BOND, BOND), BF16),
                pltpu.VMEM((4, PAIR, BOND), BF16),
                pltpu.VMEM((BOND, BOND), F32),
                pltpu.VMEM((TERMS, PAIR, QUART, HALF), BF16),
                pltpu.VMEM((PAIR, QUART, GROUP * HALF), BF16),
                pltpu.VMEM((PAIR, BOND, HALF), BF16),
                pltpu.VMEM((2, PAIR, QUART, HALF), F32),
                pltpu.VMEM((PAIR, QUART, HALF), F32),
                pltpu.VMEM((3, PAIR, QUART, HALF), F32),
                pltpu.VMEM((2, 128, 128), F32),
                pltpu.VMEM((2, 8, 8, 128), F32),
                pltpu.VMEM((1, 128), F32),
                pltpu.VMEM((2, 8, 64, 128), F32),
                pltpu.VMEM((2, 2, 8, 64, 128), F32),
                pltpu.VMEM((PAIR, 64, 128), F32),
                dma((3,)),
                dma((3,)), dma((3,)),
                dma((5,)), dma((5,)),
                dma((5,)), dma((5,)),
                dma((1,)),
                dma((8, 3)), dma((8, 3)),
                dma((1,)), dma((1,)),
                dma((7,)), dma((7,)),
                dma((2,)), dma((2, 2)),
                dma((1,)),
            ],
            compiler_params=pltpu.CompilerParams(
                collective_id=0, has_side_effects=True, vmem_limit_bytes=66 * 1000 * 1000),
        )(wf, left_loc, two_loc, right_loc)
        krylov = kry.transpose(0, 2, 1, 3).reshape(STEPS + 1, 64, phys, phys, 128)
        return krylov, ab[:, 0, 0], ab[:, 1, 0]

    return jax.shard_map(
        body_fn, mesh=mesh,
        in_specs=(P(), P('terms'), P('terms'), P('terms', 'rows')),
        out_specs=(P(None, 'terms', None, None, 'rows'), P(), P()), check_vma=False)
```

```python
import jax
import jax.numpy as jnp
from jax import lax
from jax.experimental import pallas as pl
from jax.experimental.pallas import tpu as pltpu
from jax.sharding import PartitionSpec as P

STEPS = 6
PAIR = 16
BOND = 256
TERMS = 64
BLOCK = 16
HALF = 128
COLS = 32
ELEMS = float(BOND * BOND * PAIR)
F32 = jnp.float32
BF16 = jnp.bfloat16


def lanczos_kernel(
    wf_hbm, left_hbm, two_ref, right_hbm, kry_hbm, ab_ref,
    wfv, rw, lw, bd, wt, mask, yb, zb, uT, acc, vb, tmp, st, betas, xs, xr, osb,
    loc_sem, w_ssem, w_rsem, r_ssem, r_rsem, l_ssem, l_rsem, lx_ssem, lx_rsem,
    u_ssem, u_rsem, f_ssem, f_rsem, st_ssem, st_rsem, x_ssem, x_rsem, o_sem,
):
    y = lax.axis_index("rows")
    t = lax.axis_index("terms")
    x = t // 2
    c = t % 2
    me = y * 4 + t
    sib = (y, 2 * x + (1 - c))
    xnb = (y, 2 * (1 - x) + c)
    xno = (y, 2 * (1 - x) + (1 - c))
    ynb = (1 - y, t)
    diag = (1 - y, 2 * (1 - x) + c)
    flip = 1 - 2 * c
    near = (4 * y + 2 * (1 - x) + c, 4 * (1 - y) + t, 4 * (1 - y) + 2 * (1 - x) + c)

    def rdma(src, dst, ssem, rsem, dev):
        return pltpu.make_async_remote_copy(
            src_ref=src, dst_ref=dst, send_sem=ssem, recv_sem=rsem,
            device_id=dev, device_id_type=pl.DeviceIdType.MESH)

    cp_wf = pltpu.make_async_copy(wf_hbm, wfv, loc_sem.at[0])
    cp_r = pltpu.make_async_copy(right_hbm.at[:, pl.ds(32 * t, 32), :], rw.at[pl.ds(0, 16)], loc_sem.at[1])
    cp_l = pltpu.make_async_copy(left_hbm, lw.at[pl.ds(0, 16)], loc_sem.at[2])
    cp_wf.start()
    cp_r.start()
    cp_l.start()

    barrier = pltpu.get_barrier_semaphore()
    for q in range(1, 8):
        d = (me + q) % 8
        pl.semaphore_signal(barrier, inc=1, device_id=(d // 4, d % 4), device_id_type=pl.DeviceIdType.MESH)
    pl.semaphore_wait(barrier, 7)

    def l_sib():
        return rdma(left_hbm, lw.at[pl.ds(16, 16)], l_ssem.at[0], l_rsem.at[0], sib)

    def l_dir(i):
        return rdma(left_hbm.at[pl.ds(8 * y + 2 * i, 2)], lw.at[pl.ds(32 + 2 * i, 2)],
                    l_ssem.at[1 + i], l_rsem.at[1 + i], xnb)

    def l_step(i, kind):
        src, dst, dev = ((32, 40, sib), (32, 48, ynb), (48, 56, sib))[kind]
        return rdma(lw.at[pl.ds(src + 2 * i, 2)], lw.at[pl.ds(dst + 2 * i, 2)],
                    lx_ssem.at[kind, i], lx_rsem.at[kind, i], dev)

    def r_send(i):
        first, rows, dst, dev = (
            (0, 2 * x + (1 - c), 16, sib),
            (8 * y, 2 * (1 - x) + c, 32, xnb),
            (8 * y, 2 * (1 - x) + (1 - c), 40, xno),
            (8 * (1 - y), 2 * (1 - x) + c, 48, xnb),
            (8 * (1 - y), 2 * (1 - x) + (1 - c), 56, xno),
        )[i]
        n = 16 if i == 0 else 8
        return rdma(right_hbm.at[pl.ds(first, n), pl.ds(32 * rows, 32), :], rw.at[pl.ds(dst, n)],
                    r_ssem.at[i], r_rsem.at[i], dev)

    for i in range(4):
        l_dir(i).start()
    for i in range(5):
        r_send(i).start()
    l_sib().start()

    row16 = lax.broadcasted_iota(jnp.int32, (PAIR, BOND), 0)
    lane16 = lax.broadcasted_iota(jnp.int32, (PAIR, BOND), 1)
    packed = jnp.zeros((PAIR, BOND), F32)
    for k in range(16):
        place = (lane16 == row16 + 16 * k).astype(F32).astype(BF16)
        packed = packed + jnp.dot(two_ref[k], place, preferred_element_type=F32)
    wt[0] = packed.astype(BF16)

    def w_send(i):
        return rdma(wt.at[0], wt.at[1 + i], w_ssem.at[i], w_rsem.at[i], (sib, xnb, xno)[i])

    for i in range(3):
        w_send(i).start()

    rr = lax.broadcasted_iota(jnp.int32, (BOND, BOND), 0) % 16
    cc = lax.broadcasted_iota(jnp.int32, (BOND, BOND), 1) % 16
    mask[...] = (rr == cc).astype(F32)

    cp_wf.wait()

    def sumsq(i, s):
        blk = wfv[pl.ds(pl.multiple_of(i * 256, 256), 256), :]
        return s + jnp.sum((blk * blk).reshape(32, 8, 128), axis=0)

    total = lax.fori_loop(0, 32, sumsq, jnp.zeros((8, 128), F32))
    total = jnp.sum(jnp.sum(total, axis=1, keepdims=True), axis=0, keepdims=True)
    scale = jnp.broadcast_to(jnp.sqrt(total * (1.0 / ELEMS)), (1, 128))

    wfo = wfv.at[pl.ds(pl.multiple_of(2048 * t, 2048), 2048), :]
    own = pl.ds(pl.multiple_of(32 * t, 32), 32)
    for p in range(PAIR):
        for h in range(2):
            for bt in range(2):
                first = 4096 * h + (p // 4) * 8 + bt * 4 + p % 4
                blk = (wfv[pl.ds(first, 128, stride=32), :] / scale).T
                tmp[bt] = blk
                uT[h, p, pl.ds(128 * bt, 128), :] = blk.astype(BF16)
            vb[0, p, :, pl.ds(128 * h, 128)] = tmp[y, own, :]
        first = (p // 4) * 8 + p % 4
        lo = wfo[pl.ds(first, 64, stride=32), :]
        hi = wfo[pl.ds(first + 4, 64, stride=32), :]
        osb[p] = jnp.where(y == 0, lo, hi) / scale
    vb[2] = jnp.zeros((PAIR, COLS, BOND), F32)
    betas[...] = jnp.zeros((1, 128), F32)

    def out_copy(j):
        return pltpu.make_async_copy(osb, kry_hbm.at[j], o_sem.at[0])

    out_copy(0).start()

    def u_part(h, m, dev):
        return uT.at[h, pl.ds(4 * m, 4), pl.ds(pl.multiple_of(32 * dev, 32), 32), :]

    def u_own(h, m, s):
        part = u_part(h, m, me)
        return rdma(part, part, u_ssem.at[h, m, s], u_rsem.at[h, m, s], (xnb, ynb, diag, sib)[s])

    def u_got(h, m, s):
        part = u_part(h, m, (near + (me + flip,))[s])
        return rdma(part, part, u_ssem.at[h, m, s], u_rsem.at[h, m, s], (xnb, ynb, diag, sib)[s])

    def u_relay(h, m, s):
        part = u_part(h, m, near[s])
        return rdma(part, part, f_ssem.at[h, m, s], f_rsem.at[h, m, s], sib)

    def u_relayed(h, m, s):
        part = u_part(h, m, near[s] + flip)
        return rdma(part, part, f_ssem.at[h, m, s], f_rsem.at[h, m, s], sib)

    def relay_all(h, m):
        for s in range(3):
            u_got(h, m, s).wait_recv()
            u_relay(h, m, s).start()

    def r_stage(h, k0, nk, n):
        lhs = rw[pl.ds(k0, nk)].reshape(nk * COLS, BOND)
        rhs = jnp.concatenate([uT[h, 2 * n], uT[h, 2 * n + 1]], axis=1)
        res = jnp.dot(lhs, rhs, preferred_element_type=F32).astype(BF16)
        yb[pl.ds(k0, nk), 2 * n] = res[:, :HALF].reshape(nk, COLS, HALF)
        yb[pl.ds(k0, nk), 2 * n + 1] = res[:, HALF:].reshape(nk, COLS, HALF)

    def wl_stage(h, s):
        k0 = s * BLOCK
        for k in range(BLOCK):
            rhs = jnp.concatenate(
                [yb[k0 + k, :, pl.ds(16 * i, 16), :].reshape(BOND, HALF) for i in range(2)], axis=1)
            res = jnp.dot(bd[k0 + k], rhs, preferred_element_type=F32).astype(BF16)
            for i in range(2):
                zb[:, pl.ds(16 * i, 16), pl.ds(HALF * k, HALF)] = (
                    res[:, HALF * i:HALF * (i + 1)].reshape(PAIR, 16, HALF))
        lhs = zb[...].reshape(PAIR * COLS, BLOCK * HALF)
        rhs = lw[pl.ds(k0, BLOCK), pl.ds(pl.multiple_of(HALF * h, HALF), HALF), :].reshape(BLOCK * HALF, BOND)
        res = jnp.dot(lhs, rhs, preferred_element_type=F32)
        acc[...] = acc[...] + res.reshape(PAIR, COLS, BOND)

    def build_bd(g):
        slot = (g // 4) * 2 + (1 - g // 4) * (g // 2) + (g // 4) * (g % 2)
        part = (1 - g // 4) * (g % 2) + (g // 4) * ((y + (g - 4 * (g // 4)) // 2) % 2)
        lanes = pl.multiple_of(128 * part, 128)
        ops = wt[slot, :, pl.ds(lanes, 128)].astype(F32).T.astype(BF16)
        e_t = (lax.broadcasted_iota(jnp.int32, (PAIR, BOND), 1) // 16
               == lax.broadcasted_iota(jnp.int32, (PAIR, BOND), 0)).astype(F32).astype(BF16)
        e = (lax.broadcasted_iota(jnp.int32, (BOND, PAIR), 0) // 16
             == lax.broadcasted_iota(jnp.int32, (BOND, PAIR), 1)).astype(F32).astype(BF16)
        wide = jnp.dot(ops, e_t, preferred_element_type=F32).astype(BF16)
        for k in range(8):
            full = jnp.dot(e, wide[16 * k:16 * (k + 1), :], preferred_element_type=F32)
            bd[g * 8 + k] = (full * mask[...]).astype(BF16)

    def bd_group(i, s):
        build_bd(2 * s + i)
        return s

    def first_block(s, carry):
        @pl.when(s == 0)
        def _():
            cp_r.wait()
            cp_l.wait()

        @pl.when(s == 1)
        def _():
            w_send(0).wait_recv()
            r_send(0).wait_recv()
            l_sib().wait_recv()

        @pl.when(s == 2)
        def _():
            w_send(1).wait_recv()
            w_send(2).wait_recv()

        lax.fori_loop(0, 2, bd_group, s)

        @pl.when(s < 2)
        def _():
            l_dir(s).wait_recv()
            l_step(s, 0).start()
            l_step(s, 1).start()

        @pl.when(s == 2)
        def _():
            for i in range(2, 4):
                l_dir(i).wait_recv()
                l_step(i, 0).start()
                l_step(i, 1).start()
            r_send(1).wait_recv()
            r_send(2).wait_recv()
            for i in range(4):
                l_step(i, 0).wait_recv()

        @pl.when(s == 3)
        def _():
            for i in range(4):
                l_step(i, 1).wait_recv()
                l_step(i, 2).start()
            r_send(3).wait_recv()
            r_send(4).wait_recv()
            for i in range(4):
                l_step(i, 2).wait_recv()

        def half(h, carry):
            for n in range(8):
                r_stage(h, s * BLOCK, BLOCK, n)
            wl_stage(h, s)
            return carry

        lax.fori_loop(0, 2, half, 0)
        return carry

    def gather_r(i, carry):
        @pl.when(i < 4)
        def _():
            relay_all(0, i)

        @pl.when(i >= 1)
        def _():
            later_r(0, i - 1)

        return carry

    def later_r(h, m):
        u_got(h, m, 3).wait_recv()
        for s in range(3):
            u_relayed(h, m, s).wait_recv()
        for n in range(2):
            r_stage(h, 0, TERMS, 2 * m + n)

    def gather_wl(s, carry):
        relay_all(1, s)
        wl_stage(0, s)
        return carry

    def second_r(m, carry):
        later_r(1, m)
        for h in range(2):
            for s in range(4):
                u_own(h, m, s).wait_send()
            for s in range(3):
                u_relay(h, m, s).wait_send()
        return carry

    def second_wl(s, carry):
        wl_stage(1, s)
        return carry

    def x_copy(par, q):
        dest = (t + q) % 4
        return rdma(xs.at[dest], xr.at[par, t], x_ssem.at[q - 1], x_rsem.at[par, q - 1], (y, dest))

    def x_recv(par, q):
        rdma(xs.at[0], xr.at[par, (t + 4 - q) % 4], x_ssem.at[q - 1], x_rsem.at[par, q - 1], sib).wait_recv()

    def put_out(vec, par):
        for d in range(2):
            for i in range(4):
                blk = jnp.concatenate(
                    [vb[vec, 4 * i + k, :, pl.ds(128 * d, 128)] for k in range(4)], axis=0).T
                xs[2 * d, i] = blk[:64]
                xs[2 * d + 1, i] = blk[64:]
        xr[par, t] = xs[t]

    def x_start(par):
        for q in range(1, 4):
            x_copy(par, q).start()

    def x_wait_send(par):
        for q in range(1, 4):
            x_copy(par, q).wait_send()

    def merge_out(j, par):
        for q in range(1, 4):
            x_recv(par, q)
        out_copy(0).wait()
        seg = lax.broadcasted_iota(jnp.int32, (64, 128), 1) // 32
        for i in range(4):
            parts = [xr[par, src, i] for src in range(4)]
            for k in range(4):
                res = parts[k]
                for src in range(4):
                    if src != k:
                        res = jnp.where(seg == src, pltpu.roll(parts[src], (32 * (src - k)) % 128, 1), res)
                osb[4 * i + k] = res
        out_copy(j).start()

    def everywhere(s):
        s = jnp.sum(jnp.sum(s, axis=1, keepdims=True), axis=0, keepdims=True)
        return jnp.broadcast_to(s, (1, 128))

    def fold(v):
        v = v[:, :HALF] + v[:, HALF:]
        return jnp.sum(v.reshape(COLS // 8, 8, 128), axis=0)

    def wide(row):
        return jnp.concatenate([row, row], axis=1)

    def step(j, carry):
        acc[...] = jnp.zeros((PAIR, COLS, BOND), F32)

        @pl.when(j == 0)
        def _():
            lax.fori_loop(0, 4, first_block, 0)

        @pl.when(j > 0)
        def _():
            lax.fori_loop(0, 5, gather_r, 0)
            lax.fori_loop(0, 4, gather_wl, 0)
            x_start((j + 1) % 2)
            lax.fori_loop(0, 4, second_r, 0)
            lax.fori_loop(0, 4, second_wl, 0)

        cur = j % 3
        prev = (j + 2) % 3
        nxt = (j + 1) % 3
        par = j % 2
        beta_prev = wide(betas[...])
        zero = jnp.zeros((8, 128), F32)

        def pass1(p, s):
            a_s, t_s, v_s = s
            w = acc[p]
            v = vb[cur, p]
            r = w - beta_prev * vb[prev, p]
            vb[nxt, p] = r
            return a_s + fold(w * v), t_s + fold(r * v), v_s + fold(v * v)

        a_s, t_s, v_s = lax.fori_loop(0, PAIR, pass1, (zero, zero, zero))
        a_d, t_d, v_d = everywhere(a_s), everywhere(t_s), everywhere(v_s)
        shift = jnp.where(v_d > 0.0, t_d / jnp.where(v_d > 0.0, v_d, 1.0), 0.0)
        shift_w = wide(shift)

        def pass2(p, s):
            q_s, p_s = s
            v = vb[cur, p]
            r = vb[nxt, p] - shift_w * v
            vb[nxt, p] = r
            return q_s + fold(r * r), p_s + fold(r * v)

        q_s, p_s = lax.fori_loop(0, PAIR, pass2, (zero, zero))
        st[par, me] = jnp.concatenate(
            [a_d, shift, v_d, everywhere(q_s), everywhere(p_s), jnp.zeros((3, 128), F32)], axis=0)

        def st_copy(q):
            d = (me + q) % 8
            return rdma(st.at[par, me], st.at[par, me], st_ssem.at[q - 1], st_rsem.at[q - 1], (d // 4, d % 4))

        for q in range(1, 8):
            st_copy(q).start()
        for q in range(1, 8):
            src = (me + 8 - q) % 8
            rdma(st.at[par, me], st.at[par, src], st_ssem.at[q - 1], st_rsem.at[q - 1], sib).wait_recv()

        alpha = st[par, 0][0:1]
        for d in range(1, 8):
            alpha = alpha + st[par, d][0:1]
        alpha = alpha * (1.0 / ELEMS)
        beta2 = jnp.zeros((1, 128), F32)
        for d in range(8):
            tile = st[par, d]
            gap = alpha - tile[1:2]
            beta2 = beta2 + (tile[3:4] - 2.0 * gap * tile[4:5] + gap * gap * tile[2:3])
        beta = jnp.sqrt(beta2 * (1.0 / ELEMS))
        betas[...] = beta
        ab_ref[j] = jnp.concatenate([alpha, beta, jnp.zeros((6, 128), F32)], axis=0)
        gap_w = wide(alpha - shift)
        beta_w = wide(beta)
        rows = pl.ds(pl.multiple_of(32 * me, 32), 32)

        def pass3(m, carry):
            for i in range(4):
                p = 4 * m + i
                v = (vb[nxt, p] - gap_w * vb[cur, p]) / beta_w
                vb[nxt, p] = v
                uT[0, p, rows, :] = v[:, :HALF].astype(BF16)
                uT[1, p, rows, :] = v[:, HALF:].astype(BF16)

            @pl.when(j < STEPS - 1)
            def _():
                for s in range(4):
                    u_own(0, m, s).start()

            return carry

        lax.fori_loop(0, 4, pass3, 0)

        @pl.when(j < STEPS - 1)
        def _():
            for m in range(4):
                for s in range(4):
                    u_own(1, m, s).start()

        @pl.when(j > 0)
        def _():
            x_wait_send(1 - par)

        put_out(nxt, par)

        @pl.when(j > 0)
        def _():
            merge_out(j, 1 - par)

        for q in range(1, 8):
            st_copy(q).wait_send()
        return carry

    lax.fori_loop(0, STEPS, step, 0)

    last = (STEPS - 1) % 2
    x_start(last)
    x_wait_send(last)
    merge_out(STEPS, last)
    out_copy(0).wait()

    l_sib().wait_send()
    for i in range(3):
        w_send(i).wait_send()
    for i in range(5):
        r_send(i).wait_send()
    for i in range(4):
        l_dir(i).wait_send()
        for kind in range(3):
            l_step(i, kind).wait_send()


def solution(mesh):
    def body_fn(wavefunc, left_loc, two_loc, right_loc):
        bond, phys = wavefunc.shape[0], wavefunc.shape[1]
        wf = wavefunc.reshape(bond, phys, phys, 2, 128).transpose(0, 1, 3, 2, 4).reshape(-1, 128)
        dma = pltpu.SemaphoreType.DMA
        kry, ab = pl.pallas_call(
            lanczos_kernel,
            out_shape=(
                jax.ShapeDtypeStruct((STEPS + 1, PAIR, 64, 128), F32),
                jax.ShapeDtypeStruct((STEPS, 8, 128), F32),
            ),
            in_specs=[
                pl.BlockSpec(memory_space=pl.ANY),
                pl.BlockSpec(memory_space=pl.ANY),
                pl.BlockSpec(memory_space=pltpu.VMEM),
                pl.BlockSpec(memory_space=pl.ANY),
            ],
            out_specs=(pl.BlockSpec(memory_space=pl.ANY), pl.BlockSpec(memory_space=pltpu.VMEM)),
            scratch_shapes=[
                pltpu.VMEM((8192, 128), F32),
                pltpu.VMEM((TERMS, COLS, BOND), BF16),
                pltpu.VMEM((TERMS, BOND, BOND), BF16),
                pltpu.VMEM((TERMS, BOND, BOND), BF16),
                pltpu.VMEM((4, PAIR, BOND), BF16),
                pltpu.VMEM((BOND, BOND), F32),
                pltpu.VMEM((TERMS, PAIR, COLS, HALF), BF16),
                pltpu.VMEM((PAIR, COLS, BLOCK * HALF), BF16),
                pltpu.VMEM((2, PAIR, BOND, HALF), BF16),
                pltpu.VMEM((PAIR, COLS, BOND), F32),
                pltpu.VMEM((3, PAIR, COLS, BOND), F32),
                pltpu.VMEM((2, 128, 128), F32),
                pltpu.VMEM((2, 8, 8, 128), F32),
                pltpu.VMEM((1, 128), F32),
                pltpu.VMEM((4, 4, 64, 128), F32),
                pltpu.VMEM((2, 4, 4, 64, 128), F32),
                pltpu.VMEM((PAIR, 64, 128), F32),
                dma((3,)),
                dma((3,)), dma((3,)),
                dma((5,)), dma((5,)),
                dma((5,)), dma((5,)),
                dma((3, 4)), dma((3, 4)),
                dma((2, 4, 4)), dma((2, 4, 4)),
                dma((2, 4, 3)), dma((2, 4, 3)),
                dma((7,)), dma((7,)),
                dma((3,)), dma((2, 3)),
                dma((1,)),
            ],
            compiler_params=pltpu.CompilerParams(
                collective_id=0, has_side_effects=True, vmem_limit_bytes=66 * 1000 * 1000),
        )(wf, left_loc, two_loc, right_loc)
        krylov = kry.transpose(0, 2, 1, 3).reshape(STEPS + 1, 64, phys, phys, 128)
        return krylov, ab[:, 0, 0], ab[:, 1, 0]

    return jax.shard_map(
        body_fn, mesh=mesh,
        in_specs=(P(), P('terms'), P('terms'), P('terms', 'rows')),
        out_specs=(P(None, 'terms', None, None, 'rows'), P(), P()), check_vma=False)
```

```python
import jax
import jax.numpy as jnp
from jax import lax
from jax.experimental import pallas as pl
from jax.experimental.pallas import tpu as pltpu
from jax.sharding import PartitionSpec as P

STEPS = 6
PAIR = 16
BOND = 256
TERMS = 64
BLOCK = 16
HALF = 128
COLS = 32
ELEMS = float(BOND * BOND * PAIR)
F32 = jnp.float32
BF16 = jnp.bfloat16


def lanczos_kernel(
    wf_hbm, left_hbm, two_ref, right_hbm, kry_hbm, ab_ref,
    wfv, rw, lw, lx, bd, wt, mask, yb, zb, uT, acc, vb, tmp, st, betas, coef, xs, xr, osb,
    loc_sem, w_ssem, w_rsem, r_ssem, r_rsem, l_ssem, l_rsem, lx_ssem, lx_rsem,
    u_ssem, u_rsem, f_ssem, f_rsem, st_ssem, st_rsem, x_ssem, x_rsem, o_sem,
):
    y = lax.axis_index("rows")
    t = lax.axis_index("terms")
    x = t // 2
    c = t % 2
    me = y * 4 + t
    sib = (y, 2 * x + (1 - c))
    xnb = (y, 2 * (1 - x) + c)
    xno = (y, 2 * (1 - x) + (1 - c))
    ynb = (1 - y, t)
    diag = (1 - y, 2 * (1 - x) + c)
    flip = 1 - 2 * c
    near = (4 * y + 2 * (1 - x) + c, 4 * (1 - y) + t, 4 * (1 - y) + 2 * (1 - x) + c)

    def rdma(src, dst, ssem, rsem, dev):
        return pltpu.make_async_remote_copy(
            src_ref=src, dst_ref=dst, send_sem=ssem, recv_sem=rsem,
            device_id=dev, device_id_type=pl.DeviceIdType.MESH)

    cp_wf = pltpu.make_async_copy(wf_hbm, wfv, loc_sem.at[0])
    cp_r = pltpu.make_async_copy(right_hbm.at[:, pl.ds(32 * t, 32), :], rw.at[pl.ds(0, 16)], loc_sem.at[1])
    cp_l = pltpu.make_async_copy(left_hbm, lw.at[pl.ds(0, 16)], loc_sem.at[2])
    cp_wf.start()
    cp_r.start()
    cp_l.start()

    barrier = pltpu.get_barrier_semaphore()
    for q in range(1, 8):
        d = (me + q) % 8
        pl.semaphore_signal(barrier, inc=1, device_id=(d // 4, d % 4), device_id_type=pl.DeviceIdType.MESH)
    pl.semaphore_wait(barrier, 7)

    def l_sib():
        return rdma(left_hbm, lw.at[pl.ds(16, 16)], l_ssem.at[0], l_rsem.at[0], sib)

    def l_dir(i, part):
        rows = pl.ds(0, 256) if part == 0 else pl.ds(128, 128)
        return rdma(left_hbm.at[pl.ds(8 * y + 2 * i, 2), rows, pl.ds(128 * part, 128)],
                    lx.at[pl.ds(2 * i, 2), pl.ds(256 * part, 256 - 128 * part), :],
                    l_ssem.at[1 + 2 * i + part], l_rsem.at[1 + 2 * i + part], xnb)

    def l_step(i, kind):
        src, dst, dev = ((0, 8, sib), (0, 16, ynb), (16, 24, sib))[kind]
        return rdma(lx.at[pl.ds(src + 2 * i, 2)], lx.at[pl.ds(dst + 2 * i, 2)],
                    lx_ssem.at[kind, i], lx_rsem.at[kind, i], dev)

    def l_take(i):
        for part in range(2):
            l_dir(i, part).wait_recv()
        l_step(i, 0).start()
        l_step(i, 1).start()

    def l_unpack(k, s):
        src = 16 * (s - 2) + k
        dst = 16 * s + k
        low = lx[src, pl.ds(128, 128), :]
        lw[dst, pl.ds(0, 128), pl.ds(0, 128)] = lx[src, pl.ds(0, 128), :]
        lw[dst, pl.ds(128, 128), pl.ds(0, 128)] = low
        lw[dst, pl.ds(0, 128), pl.ds(128, 128)] = low.astype(F32).T.astype(BF16)
        lw[dst, pl.ds(128, 128), pl.ds(128, 128)] = lx[src, pl.ds(256, 128), :]
        return s

    def r_send(i):
        first, rows, dst, dev = (
            (0, 2 * x + (1 - c), 16, sib),
            (8 * y, 2 * (1 - x) + c, 32, xnb),
            (8 * y, 2 * (1 - x) + (1 - c), 40, xno),
            (8 * (1 - y), 2 * (1 - x) + c, 48, xnb),
            (8 * (1 - y), 2 * (1 - x) + (1 - c), 56, xno),
        )[i]
        n = 16 if i == 0 else 8
        return rdma(right_hbm.at[pl.ds(first, n), pl.ds(32 * rows, 32), :], rw.at[pl.ds(dst, n)],
                    r_ssem.at[i], r_rsem.at[i], dev)

    for i in range(4):
        for part in range(2):
            l_dir(i, part).start()
    for i in range(5):
        r_send(i).start()
    l_sib().start()

    row16 = lax.broadcasted_iota(jnp.int32, (PAIR, BOND), 0)
    lane16 = lax.broadcasted_iota(jnp.int32, (PAIR, BOND), 1)
    packed = jnp.zeros((PAIR, BOND), F32)
    for k in range(16):
        place = (lane16 == row16 + 16 * k).astype(F32).astype(BF16)
        packed = packed + jnp.dot(two_ref[k], place, preferred_element_type=F32)
    wt[0] = packed.astype(BF16)

    def w_send(i):
        return rdma(wt.at[0], wt.at[1 + i], w_ssem.at[i], w_rsem.at[i], (sib, xnb, xno)[i])

    for i in range(3):
        w_send(i).start()

    rr = lax.broadcasted_iota(jnp.int32, (BOND, BOND), 0) % 16
    cc = lax.broadcasted_iota(jnp.int32, (BOND, BOND), 1) % 16
    mask[...] = (rr == cc).astype(F32)

    cp_wf.wait()

    def sumsq(i, s):
        blk = wfv[pl.ds(pl.multiple_of(i * 256, 256), 256), :]
        return s + jnp.sum((blk * blk).reshape(32, 8, 128), axis=0)

    total = lax.fori_loop(0, 32, sumsq, jnp.zeros((8, 128), F32))
    total = jnp.sum(jnp.sum(total, axis=1, keepdims=True), axis=0, keepdims=True)
    scale = jnp.broadcast_to(jnp.sqrt(total * (1.0 / ELEMS)), (1, 128))

    wfo = wfv.at[pl.ds(pl.multiple_of(2048 * t, 2048), 2048), :]
    own = pl.ds(pl.multiple_of(32 * t, 32), 32)
    for p in range(PAIR):
        for h in range(2):
            for bt in range(2):
                first = 4096 * h + (p // 4) * 8 + bt * 4 + p % 4
                blk = (wfv[pl.ds(first, 128, stride=32), :] / scale).T
                tmp[bt] = blk
                uT[h, p, pl.ds(128 * bt, 128), :] = blk.astype(BF16)
            vb[0, p, :, pl.ds(128 * h, 128)] = tmp[y, own, :]
        first = (p // 4) * 8 + p % 4
        lo = wfo[pl.ds(first, 64, stride=32), :]
        hi = wfo[pl.ds(first + 4, 64, stride=32), :]
        osb[0, pl.ds(p, 64, stride=16), :] = jnp.where(y == 0, lo, hi) / scale
    vb[2] = jnp.zeros((PAIR, COLS, BOND), F32)
    betas[...] = jnp.zeros((1, 128), F32)

    def out_copy(j):
        return pltpu.make_async_copy(osb.at[j % 2], kry_hbm.at[j], o_sem.at[j % 2])

    out_copy(0).start()

    def u_part(h, m, dev):
        return uT.at[h, pl.ds(4 * m, 4), pl.ds(pl.multiple_of(32 * dev, 32), 32), :]

    def u_own(h, m, s):
        part = u_part(h, m, me)
        return rdma(part, part, u_ssem.at[h, m, s], u_rsem.at[h, m, s], (xnb, ynb, diag, sib)[s])

    def u_got(h, m, s):
        part = u_part(h, m, (near + (me + flip,))[s])
        return rdma(part, part, u_ssem.at[h, m, s], u_rsem.at[h, m, s], (xnb, ynb, diag, sib)[s])

    def u_relay(h, m, s):
        part = u_part(h, m, near[s])
        return rdma(part, part, f_ssem.at[h, m, s], f_rsem.at[h, m, s], sib)

    def u_relayed(h, m, s):
        part = u_part(h, m, near[s] + flip)
        return rdma(part, part, f_ssem.at[h, m, s], f_rsem.at[h, m, s], sib)

    def relay_all(h, m):
        for s in range(3):
            u_got(h, m, s).wait_recv()
            u_relay(h, m, s).start()

    def r_stage(h, k0, nk, n):
        lhs = rw[pl.ds(k0, nk)].reshape(nk * COLS, BOND)
        rhs = jnp.concatenate([uT[h, 2 * n], uT[h, 2 * n + 1]], axis=1)
        res = jnp.dot(lhs, rhs, preferred_element_type=F32).astype(BF16)
        yb[pl.ds(k0, nk), 2 * n] = res[:, :HALF].reshape(nk, COLS, HALF)
        yb[pl.ds(k0, nk), 2 * n + 1] = res[:, HALF:].reshape(nk, COLS, HALF)

    def wl_stage(h, s):
        k0 = s * BLOCK
        for k in range(BLOCK):
            rhs = jnp.concatenate(
                [yb[k0 + k, :, pl.ds(16 * i, 16), :].reshape(BOND, HALF) for i in range(2)], axis=1)
            res = jnp.dot(bd[k0 + k], rhs, preferred_element_type=F32).astype(BF16)
            for i in range(2):
                zb[:, pl.ds(16 * i, 16), pl.ds(HALF * k, HALF)] = (
                    res[:, HALF * i:HALF * (i + 1)].reshape(PAIR, 16, HALF))
        lhs = zb[...].reshape(PAIR * COLS, BLOCK * HALF)
        rhs = lw[pl.ds(k0, BLOCK), pl.ds(pl.multiple_of(HALF * h, HALF), HALF), :].reshape(BLOCK * HALF, BOND)
        res = jnp.dot(lhs, rhs, preferred_element_type=F32)
        acc[...] = acc[...] + res.reshape(PAIR, COLS, BOND)

    def build_bd(g):
        slot = (g // 4) * 2 + (1 - g // 4) * (g // 2) + (g // 4) * (g % 2)
        part = (1 - g // 4) * (g % 2) + (g // 4) * ((y + (g - 4 * (g // 4)) // 2) % 2)
        lanes = pl.multiple_of(128 * part, 128)
        ops = wt[slot, :, pl.ds(lanes, 128)].astype(F32).T.astype(BF16)
        e_t = (lax.broadcasted_iota(jnp.int32, (PAIR, BOND), 1) // 16
               == lax.broadcasted_iota(jnp.int32, (PAIR, BOND), 0)).astype(F32).astype(BF16)
        e = (lax.broadcasted_iota(jnp.int32, (BOND, PAIR), 0) // 16
             == lax.broadcasted_iota(jnp.int32, (BOND, PAIR), 1)).astype(F32).astype(BF16)
        wide = jnp.dot(ops, e_t, preferred_element_type=F32).astype(BF16)
        for k in range(8):
            full = jnp.dot(e, wide[16 * k:16 * (k + 1), :], preferred_element_type=F32)
            bd[g * 8 + k] = (full * mask[...]).astype(BF16)

    def bd_group(i, s):
        build_bd(2 * s + i)
        return s

    def first_block(s, carry):
        @pl.when(s == 0)
        def _():
            cp_r.wait()
            cp_l.wait()

        @pl.when(s == 1)
        def _():
            w_send(0).wait_recv()
            r_send(0).wait_recv()
            l_sib().wait_recv()

        @pl.when(s == 2)
        def _():
            w_send(1).wait_recv()
            w_send(2).wait_recv()

        lax.fori_loop(0, 2, bd_group, s)

        @pl.when(s < 2)
        def _():
            for i in range(2):
                @pl.when(s == i)
                def _(i=i):
                    l_take(i)

        @pl.when(s == 2)
        def _():
            l_take(2)
            l_take(3)
            for i in range(4):
                l_step(i, 0).wait_recv()
            lax.fori_loop(0, 16, l_unpack, s)
            r_send(1).wait_recv()
            r_send(2).wait_recv()

        @pl.when(s == 3)
        def _():
            for i in range(4):
                l_step(i, 1).wait_recv()
                l_step(i, 2).start()
            for i in range(4):
                l_step(i, 2).wait_recv()
            lax.fori_loop(0, 16, l_unpack, s)
            r_send(3).wait_recv()
            r_send(4).wait_recv()

        def half(h, carry):
            for n in range(8):
                r_stage(h, s * BLOCK, BLOCK, n)
            wl_stage(h, s)
            return carry

        lax.fori_loop(0, 2, half, 0)
        return carry

    def gather_r(i, carry):
        @pl.when(i < 4)
        def _():
            relay_all(0, i)

        @pl.when(i >= 1)
        def _():
            later_r(0, i - 1)

        return carry

    def later_r(h, m):
        u_got(h, m, 3).wait_recv()
        for s in range(3):
            u_relayed(h, m, s).wait_recv()
        for n in range(2):
            r_stage(h, 0, TERMS, 2 * m + n)

    def gather_wl(s, carry):
        relay_all(1, s)
        wl_stage(0, s)
        return carry

    def second_r(m, carry):
        later_r(1, m)
        for h in range(2):
            for s in range(4):
                u_own(h, m, s).wait_send()
            for s in range(3):
                u_relay(h, m, s).wait_send()
        return carry

    def second_wl(s, carry):
        wl_stage(1, s)
        return carry

    def x_copy(par, q):
        dest = (t + q) % 4
        return rdma(xs.at[dest], xr.at[par, t], x_ssem.at[q - 1], x_rsem.at[par, q - 1], (y, dest))

    def x_recv(par, q):
        rdma(xs.at[0], xr.at[par, (t + 4 - q) % 4], x_ssem.at[q - 1], x_rsem.at[par, q - 1], sib).wait_recv()

    def put_out(vec, par):
        for d in range(2):
            for i in range(4):
                blk = jnp.concatenate(
                    [vec[4 * i + k, :, pl.ds(128 * d, 128)] for k in range(4)], axis=0).T
                xs[2 * d, i] = blk[:64]
                xs[2 * d + 1, i] = blk[64:]
        xr[par, t] = xs[t]

    def x_start(par):
        for q in range(1, 4):
            x_copy(par, q).start()

    def x_wait_send(par):
        for q in range(1, 4):
            x_copy(par, q).wait_send()

    def merged(par):
        seg = lax.broadcasted_iota(jnp.int32, (64, 128), 1) // 32
        for i in range(4):
            parts = [xr[par, src, i] for src in range(4)]
            for k in range(4):
                res = parts[k]
                for src in range(4):
                    if src != k:
                        res = jnp.where(seg == src, pltpu.roll(parts[src], (32 * (src - k)) % 128, 1), res)
                yield 4 * i + k, res

    def merge_out(j, par):
        for q in range(1, 4):
            x_recv(par, q)

        @pl.when(j > 1)
        def _():
            out_copy(j - 2).wait()

        for p, res in merged(par):
            osb[j % 2, pl.ds(p, 64, stride=16), :] = res
        out_copy(j).start()

    def everywhere(s):
        s = jnp.sum(jnp.sum(s, axis=1, keepdims=True), axis=0, keepdims=True)
        return jnp.broadcast_to(s, (1, 128))

    def fold(v):
        v = v[:, :HALF] + v[:, HALF:]
        return jnp.sum(v.reshape(COLS // 8, 8, 128), axis=0)

    def wide(row):
        return jnp.concatenate([row, row], axis=1)

    def step(j, carry):
        acc[...] = jnp.zeros((PAIR, COLS, BOND), F32)

        @pl.when(j == 0)
        def _():
            lax.fori_loop(0, 4, first_block, 0)

        @pl.when(j > 0)
        def _():
            lax.fori_loop(0, 5, gather_r, 0)
            lax.fori_loop(0, 4, gather_wl, 0)
            x_start((j + 1) % 2)
            lax.fori_loop(0, 4, second_r, 0)
            lax.fori_loop(0, 4, second_wl, 0)

        cur = j % 3
        prev = (j + 2) % 3
        nxt = (j + 1) % 3
        par = j % 2

        @pl.when(j == STEPS - 1)
        def _():
            x_wait_send(1 - par)
            put_out(acc, par)
            x_start(par)

        beta_prev = wide(betas[...])
        zero = jnp.zeros((8, 128), F32)

        def pass1(p, s):
            a_s, t_s, v_s = s
            w = acc[p]
            v = vb[cur, p]
            r = w - beta_prev * vb[prev, p]
            vb[nxt, p] = r
            return a_s + fold(w * v), t_s + fold(r * v), v_s + fold(v * v)

        a_s, t_s, v_s = lax.fori_loop(0, PAIR, pass1, (zero, zero, zero))
        a_d, t_d, v_d = everywhere(a_s), everywhere(t_s), everywhere(v_s)
        shift = jnp.where(v_d > 0.0, t_d / jnp.where(v_d > 0.0, v_d, 1.0), 0.0)
        shift_w = wide(shift)

        def pass2(p, s):
            q_s, p_s = s
            v = vb[cur, p]
            r = vb[nxt, p] - shift_w * v
            vb[nxt, p] = r
            return q_s + fold(r * r), p_s + fold(r * v)

        q_s, p_s = lax.fori_loop(0, PAIR, pass2, (zero, zero))
        st[par, me] = jnp.concatenate(
            [a_d, shift, v_d, everywhere(q_s), everywhere(p_s), jnp.zeros((3, 128), F32)], axis=0)

        def st_copy(q):
            d = (me + q) % 8
            return rdma(st.at[par, me], st.at[par, me], st_ssem.at[q - 1], st_rsem.at[q - 1], (d // 4, d % 4))

        for q in range(1, 8):
            st_copy(q).start()

        @pl.when(j > 0)
        def _():
            merge_out(j, 1 - par)

        for q in range(1, 8):
            src = (me + 8 - q) % 8
            rdma(st.at[par, me], st.at[par, src], st_ssem.at[q - 1], st_rsem.at[q - 1], sib).wait_recv()

        alpha = st[par, 0][0:1]
        for d in range(1, 8):
            alpha = alpha + st[par, d][0:1]
        alpha = alpha * (1.0 / ELEMS)
        beta2 = jnp.zeros((1, 128), F32)
        for d in range(8):
            tile = st[par, d]
            gap = alpha - tile[1:2]
            beta2 = beta2 + (tile[3:4] - 2.0 * gap * tile[4:5] + gap * gap * tile[2:3])
        beta = jnp.sqrt(beta2 * (1.0 / ELEMS))
        betas[...] = beta
        coef[0] = alpha
        coef[1] = beta_prev[:, :HALF]
        ab_ref[j] = jnp.concatenate([alpha, beta, jnp.zeros((6, 128), F32)], axis=0)
        gap_w = wide(alpha - shift)
        beta_w = wide(beta)
        rows = pl.ds(pl.multiple_of(32 * me, 32), 32)

        def pass3(m, carry):
            for i in range(4):
                p = 4 * m + i
                v = (vb[nxt, p] - gap_w * vb[cur, p]) / beta_w
                vb[nxt, p] = v
                uT[0, p, rows, :] = v[:, :HALF].astype(BF16)
                uT[1, p, rows, :] = v[:, HALF:].astype(BF16)

            for s in range(4):
                u_own(0, m, s).start()
            return carry

        @pl.when(j < STEPS - 1)
        def _():
            lax.fori_loop(0, 4, pass3, 0)
            for m in range(4):
                for s in range(4):
                    u_own(1, m, s).start()

        @pl.when((j > 0) & (j < STEPS - 1))
        def _():
            x_wait_send(1 - par)

        @pl.when(j < STEPS - 1)
        def _():
            put_out(vb.at[nxt], par)

        for q in range(1, 8):
            st_copy(q).wait_send()
        return carry

    lax.fori_loop(0, STEPS, step, 0)

    last = (STEPS - 1) % 2
    for q in range(1, 4):
        x_recv(last, q)
    out_copy(STEPS - 2).wait()
    for p, res in merged(last):
        at = pl.ds(p, 64, stride=16)
        res = res - coef[0] * osb[(STEPS - 1) % 2, at, :] - coef[1] * osb[STEPS % 2, at, :]
        osb[STEPS % 2, at, :] = res / betas[...]
    out_copy(STEPS).start()
    x_wait_send(last)
    out_copy(STEPS - 1).wait()
    out_copy(STEPS).wait()

    l_sib().wait_send()
    for i in range(3):
        w_send(i).wait_send()
    for i in range(5):
        r_send(i).wait_send()
    for i in range(4):
        for part in range(2):
            l_dir(i, part).wait_send()
        for kind in range(3):
            l_step(i, kind).wait_send()


def solution(mesh):
    def body_fn(wavefunc, left_loc, two_loc, right_loc):
        bond, phys = wavefunc.shape[0], wavefunc.shape[1]
        wf = wavefunc.reshape(bond, phys, phys, 2, 128).transpose(0, 1, 3, 2, 4).reshape(-1, 128)
        dma = pltpu.SemaphoreType.DMA
        kry, ab = pl.pallas_call(
            lanczos_kernel,
            out_shape=(
                jax.ShapeDtypeStruct((STEPS + 1, 64 * PAIR, 128), F32),
                jax.ShapeDtypeStruct((STEPS, 8, 128), F32),
            ),
            in_specs=[
                pl.BlockSpec(memory_space=pl.ANY),
                pl.BlockSpec(memory_space=pl.ANY),
                pl.BlockSpec(memory_space=pltpu.VMEM),
                pl.BlockSpec(memory_space=pl.ANY),
            ],
            out_specs=(pl.BlockSpec(memory_space=pl.ANY), pl.BlockSpec(memory_space=pltpu.VMEM)),
            scratch_shapes=[
                pltpu.VMEM((8192, 128), F32),
                pltpu.VMEM((TERMS, COLS, BOND), BF16),
                pltpu.VMEM((TERMS, BOND, BOND), BF16),
                pltpu.VMEM((32, 384, 128), BF16),
                pltpu.VMEM((TERMS, BOND, BOND), BF16),
                pltpu.VMEM((4, PAIR, BOND), BF16),
                pltpu.VMEM((BOND, BOND), F32),
                pltpu.VMEM((TERMS, PAIR, COLS, HALF), BF16),
                pltpu.VMEM((PAIR, COLS, BLOCK * HALF), BF16),
                pltpu.VMEM((2, PAIR, BOND, HALF), BF16),
                pltpu.VMEM((PAIR, COLS, BOND), F32),
                pltpu.VMEM((3, PAIR, COLS, BOND), F32),
                pltpu.VMEM((2, 128, 128), F32),
                pltpu.VMEM((2, 8, 8, 128), F32),
                pltpu.VMEM((1, 128), F32),
                pltpu.VMEM((2, 1, 128), F32),
                pltpu.VMEM((4, 4, 64, 128), F32),
                pltpu.VMEM((2, 4, 4, 64, 128), F32),
                pltpu.VMEM((2, 64 * PAIR, 128), F32),
                dma((3,)),
                dma((3,)), dma((3,)),
                dma((5,)), dma((5,)),
                dma((9,)), dma((9,)),
                dma((3, 4)), dma((3, 4)),
                dma((2, 4, 4)), dma((2, 4, 4)),
                dma((2, 4, 3)), dma((2, 4, 3)),
                dma((7,)), dma((7,)),
                dma((3,)), dma((2, 3)),
                dma((2,)),
            ],
            compiler_params=pltpu.CompilerParams(
                collective_id=0, has_side_effects=True, vmem_limit_bytes=66 * 1000 * 1000),
        )(wf, left_loc, two_loc, right_loc)
        krylov = kry.reshape(STEPS + 1, 64, phys, phys, 128)
        return krylov, ab[:, 0, 0], ab[:, 1, 0]

    return jax.shard_map(
        body_fn, mesh=mesh,
        in_specs=(P(), P('terms'), P('terms'), P('terms', 'rows')),
        out_specs=(P(None, 'terms', None, None, 'rows'), P(), P()), check_vma=False)
```

```python
import jax
import jax.numpy as jnp
from jax import lax
from jax.experimental import pallas as pl
from jax.experimental.pallas import tpu as pltpu
from jax.sharding import PartitionSpec as P

STEPS = 6
PAIR = 16
BOND = 256
TERMS = 64
BLOCK = 16
HALF = 128
COLS = 32
ELEMS = float(BOND * BOND * PAIR)
F32 = jnp.float32
BF16 = jnp.bfloat16


def lanczos_kernel(
    wf_hbm, left_hbm, two_ref, right_hbm, kry_hbm, ab_ref,
    wfv, rw, lw, lx, bd, wt, mask, yb, zb, uT, acc, vb, tmp, st, betas, coef, xs, xr, osb,
    loc_sem, w_ssem, w_rsem, r_ssem, r_rsem, l_ssem, l_rsem, lx_ssem, lx_rsem,
    u_ssem, u_rsem, f_ssem, f_rsem, st_ssem, st_rsem, x_ssem, x_rsem, o_sem,
):
    y = lax.axis_index("rows")
    t = lax.axis_index("terms")
    x = t // 2
    c = t % 2
    me = y * 4 + t
    sib = (y, 2 * x + (1 - c))
    xnb = (y, 2 * (1 - x) + c)
    xno = (y, 2 * (1 - x) + (1 - c))
    ynb = (1 - y, t)
    diag = (1 - y, 2 * (1 - x) + c)
    flip = 1 - 2 * c
    near = (4 * y + 2 * (1 - x) + c, 4 * (1 - y) + t, 4 * (1 - y) + 2 * (1 - x) + c)

    def rdma(src, dst, ssem, rsem, dev):
        return pltpu.make_async_remote_copy(
            src_ref=src, dst_ref=dst, send_sem=ssem, recv_sem=rsem,
            device_id=dev, device_id_type=pl.DeviceIdType.MESH)

    cp_wf = pltpu.make_async_copy(wf_hbm, wfv, loc_sem.at[0])
    cp_r = pltpu.make_async_copy(right_hbm.at[:, pl.ds(32 * t, 32), :], rw.at[pl.ds(0, 16)], loc_sem.at[1])
    cp_l = pltpu.make_async_copy(left_hbm, lw.at[pl.ds(0, 16)], loc_sem.at[2])
    cp_wf.start()
    cp_r.start()
    cp_l.start()

    barrier = pltpu.get_barrier_semaphore()
    for q in range(1, 8):
        d = (me + q) % 8
        pl.semaphore_signal(barrier, inc=1, device_id=(d // 4, d % 4), device_id_type=pl.DeviceIdType.MESH)
    pl.semaphore_wait(barrier, 7)

    def l_sib():
        return rdma(left_hbm, lw.at[pl.ds(16, 16)], l_ssem.at[0], l_rsem.at[0], sib)

    def l_dir(i, part):
        rows = pl.ds(0, 256) if part == 0 else pl.ds(128, 128)
        return rdma(left_hbm.at[pl.ds(8 * y + 2 * i, 2), rows, pl.ds(128 * part, 128)],
                    lx.at[pl.ds(2 * i, 2), pl.ds(256 * part, 256 - 128 * part), :],
                    l_ssem.at[1 + 2 * i + part], l_rsem.at[1 + 2 * i + part], xnb)

    def l_step(i, kind):
        src, dst, dev = ((0, 8, sib), (0, 16, ynb), (16, 24, sib))[kind]
        return rdma(lx.at[pl.ds(src + 2 * i, 2)], lx.at[pl.ds(dst + 2 * i, 2)],
                    lx_ssem.at[kind, i], lx_rsem.at[kind, i], dev)

    def l_take(i):
        for part in range(2):
            l_dir(i, part).wait_recv()
        l_step(i, 0).start()
        l_step(i, 1).start()

    def l_unpack(k, s):
        src = 16 * (s - 2) + k
        dst = 16 * s + k
        low = lx[src, pl.ds(128, 128), :]
        lw[dst, pl.ds(0, 128), pl.ds(0, 128)] = lx[src, pl.ds(0, 128), :]
        lw[dst, pl.ds(128, 128), pl.ds(0, 128)] = low
        lw[dst, pl.ds(0, 128), pl.ds(128, 128)] = low.astype(F32).T.astype(BF16)
        lw[dst, pl.ds(128, 128), pl.ds(128, 128)] = lx[src, pl.ds(256, 128), :]
        return s

    def r_send(i):
        first, rows, dst, dev = (
            (0, 2 * x + (1 - c), 16, sib),
            (8 * y, 2 * (1 - x) + c, 32, xnb),
            (8 * y, 2 * (1 - x) + (1 - c), 40, xno),
            (8 * (1 - y), 2 * (1 - x) + c, 48, xnb),
            (8 * (1 - y), 2 * (1 - x) + (1 - c), 56, xno),
        )[i]
        n = 16 if i == 0 else 8
        return rdma(right_hbm.at[pl.ds(first, n), pl.ds(32 * rows, 32), :], rw.at[pl.ds(dst, n)],
                    r_ssem.at[i], r_rsem.at[i], dev)

    for i in range(4):
        for part in range(2):
            l_dir(i, part).start()
    for i in range(5):
        r_send(i).start()
    l_sib().start()

    row16 = lax.broadcasted_iota(jnp.int32, (PAIR, BOND), 0)
    lane16 = lax.broadcasted_iota(jnp.int32, (PAIR, BOND), 1)
    packed = jnp.zeros((PAIR, BOND), F32)
    for k in range(16):
        place = (lane16 == row16 + 16 * k).astype(F32).astype(BF16)
        packed = packed + jnp.dot(two_ref[k], place, preferred_element_type=F32)
    wt[0] = packed.astype(BF16)

    def w_send(i):
        return rdma(wt.at[0], wt.at[1 + i], w_ssem.at[i], w_rsem.at[i], (sib, xnb, xno)[i])

    for i in range(3):
        w_send(i).start()

    rr = lax.broadcasted_iota(jnp.int32, (BOND, BOND), 0) % 16
    cc = lax.broadcasted_iota(jnp.int32, (BOND, BOND), 1) % 16
    mask[...] = (rr == cc).astype(F32)

    cp_wf.wait()

    def sumsq(i, s):
        blk = wfv[pl.ds(pl.multiple_of(i * 256, 256), 256), :]
        return s + jnp.sum((blk * blk).reshape(32, 8, 128), axis=0)

    total = lax.fori_loop(0, 32, sumsq, jnp.zeros((8, 128), F32))
    total = jnp.sum(jnp.sum(total, axis=1, keepdims=True), axis=0, keepdims=True)
    scale = jnp.broadcast_to(jnp.sqrt(total * (1.0 / ELEMS)), (1, 128))

    wfo = wfv.at[pl.ds(pl.multiple_of(2048 * t, 2048), 2048), :]
    own = pl.ds(pl.multiple_of(32 * t, 32), 32)
    for p in range(PAIR):
        for h in range(2):
            for bt in range(2):
                first = 4096 * h + (p // 4) * 8 + bt * 4 + p % 4
                blk = (wfv[pl.ds(first, 128, stride=32), :] / scale).T
                tmp[bt] = blk
                uT[h, p, pl.ds(128 * bt, 128), :] = blk.astype(BF16)
            vb[0, p, :, pl.ds(128 * h, 128)] = tmp[y, own, :]
        first = (p // 4) * 8 + p % 4
        lo = wfo[pl.ds(first, 64, stride=32), :]
        hi = wfo[pl.ds(first + 4, 64, stride=32), :]
        osb[0, pl.ds(p, 64, stride=16), :] = jnp.where(y == 0, lo, hi) / scale
    vb[2] = jnp.zeros((PAIR, COLS, BOND), F32)
    betas[...] = jnp.zeros((1, 128), F32)

    def out_copy(j):
        return pltpu.make_async_copy(osb.at[j % 2], kry_hbm.at[j], o_sem.at[j % 2])

    out_copy(0).start()

    def u_part(h, m, dev):
        return uT.at[h, pl.ds(4 * m, 4), pl.ds(pl.multiple_of(32 * dev, 32), 32), :]

    def u_own(h, m, s):
        part = u_part(h, m, me)
        return rdma(part, part, u_ssem.at[h, m, s], u_rsem.at[h, m, s], (xnb, ynb, diag, sib)[s])

    def u_got(h, m, s):
        part = u_part(h, m, (near + (me + flip,))[s])
        return rdma(part, part, u_ssem.at[h, m, s], u_rsem.at[h, m, s], (xnb, ynb, diag, sib)[s])

    def u_relay(h, m, s):
        part = u_part(h, m, near[s])
        return rdma(part, part, f_ssem.at[h, m, s], f_rsem.at[h, m, s], sib)

    def u_relayed(h, m, s):
        part = u_part(h, m, near[s] + flip)
        return rdma(part, part, f_ssem.at[h, m, s], f_rsem.at[h, m, s], sib)

    def relay_all(h, m):
        for s in range(3):
            u_got(h, m, s).wait_recv()
            u_relay(h, m, s).start()

    def r_stage(h, k0, nk, n):
        lhs = rw[pl.ds(k0, nk)].reshape(nk * COLS, BOND)
        rhs = jnp.concatenate([uT[h, 2 * n], uT[h, 2 * n + 1]], axis=1)
        res = jnp.dot(lhs, rhs, preferred_element_type=F32).astype(BF16)
        yb[pl.ds(k0, nk), 2 * n] = res[:, :HALF].reshape(nk, COLS, HALF)
        yb[pl.ds(k0, nk), 2 * n + 1] = res[:, HALF:].reshape(nk, COLS, HALF)

    def wl_stage(h, s):
        k0 = s * BLOCK
        for k in range(BLOCK):
            rhs = jnp.concatenate(
                [yb[k0 + k, :, pl.ds(16 * i, 16), :].reshape(BOND, HALF) for i in range(2)], axis=1)
            res = jnp.dot(bd[k0 + k], rhs, preferred_element_type=F32).astype(BF16)
            for i in range(2):
                zb[:, pl.ds(16 * i, 16), pl.ds(HALF * k, HALF)] = (
                    res[:, HALF * i:HALF * (i + 1)].reshape(PAIR, 16, HALF))
        lhs = zb[...].reshape(PAIR * COLS, BLOCK * HALF)
        rhs = lw[pl.ds(k0, BLOCK), pl.ds(pl.multiple_of(HALF * h, HALF), HALF), :].reshape(BLOCK * HALF, BOND)
        res = jnp.dot(lhs, rhs, preferred_element_type=F32)
        acc[...] = acc[...] + res.reshape(PAIR, COLS, BOND)

    def build_bd(g):
        slot = (g // 4) * 2 + (1 - g // 4) * (g // 2) + (g // 4) * (g % 2)
        part = (1 - g // 4) * (g % 2) + (g // 4) * ((y + (g - 4 * (g // 4)) // 2) % 2)
        lanes = pl.multiple_of(128 * part, 128)
        ops = wt[slot, :, pl.ds(lanes, 128)].astype(F32).T.astype(BF16)
        e_t = (lax.broadcasted_iota(jnp.int32, (PAIR, BOND), 1) // 16
               == lax.broadcasted_iota(jnp.int32, (PAIR, BOND), 0)).astype(F32).astype(BF16)
        e = (lax.broadcasted_iota(jnp.int32, (BOND, PAIR), 0) // 16
             == lax.broadcasted_iota(jnp.int32, (BOND, PAIR), 1)).astype(F32).astype(BF16)
        wide = jnp.dot(ops, e_t, preferred_element_type=F32).astype(BF16)
        for k in range(8):
            full = jnp.dot(e, wide[16 * k:16 * (k + 1), :], preferred_element_type=F32)
            bd[g * 8 + k] = (full * mask[...]).astype(BF16)

    def bd_group(i, s):
        build_bd(2 * s + i)
        return s

    def first_block(s, carry):
        @pl.when(s == 0)
        def _():
            cp_r.wait()
            cp_l.wait()

        @pl.when(s == 1)
        def _():
            w_send(0).wait_recv()
            r_send(0).wait_recv()
            l_sib().wait_recv()

        @pl.when(s == 2)
        def _():
            w_send(1).wait_recv()
            w_send(2).wait_recv()

        lax.fori_loop(0, 2, bd_group, s)

        @pl.when(s < 2)
        def _():
            for i in range(2):
                @pl.when(s == i)
                def _(i=i):
                    l_take(i)

        @pl.when(s == 2)
        def _():
            l_take(2)
            l_take(3)
            for i in range(4):
                l_step(i, 0).wait_recv()
            lax.fori_loop(0, 16, l_unpack, s)
            r_send(1).wait_recv()
            r_send(2).wait_recv()

        @pl.when(s == 3)
        def _():
            for i in range(4):
                l_step(i, 1).wait_recv()
                l_step(i, 2).start()
            for i in range(4):
                l_step(i, 2).wait_recv()
            lax.fori_loop(0, 16, l_unpack, s)
            r_send(3).wait_recv()
            r_send(4).wait_recv()

        def half(h, carry):
            for n in range(8):
                r_stage(h, s * BLOCK, BLOCK, n)
            wl_stage(h, s)
            return carry

        lax.fori_loop(0, 2, half, 0)
        return carry

    def gather_r(i, carry):
        @pl.when(i < 4)
        def _():
            relay_all(0, i)
            for s in range(4):
                u_own(1, i, s).start()

        @pl.when(i >= 1)
        def _():
            later_r(0, i - 1)

        return carry

    def later_r(h, m):
        u_got(h, m, 3).wait_recv()
        for s in range(3):
            u_relayed(h, m, s).wait_recv()
        for n in range(2):
            r_stage(h, 0, TERMS, 2 * m + n)

    def gather_wl(s, carry):
        relay_all(1, s)
        wl_stage(0, s)
        return carry

    def second_r(m, carry):
        later_r(1, m)
        for h in range(2):
            for s in range(4):
                u_own(h, m, s).wait_send()
            for s in range(3):
                u_relay(h, m, s).wait_send()
        return carry

    def second_wl(s, carry):
        wl_stage(1, s)
        return carry

    def x_copy(par, q):
        dest = (t + q) % 4
        return rdma(xs.at[dest], xr.at[par, t], x_ssem.at[q - 1], x_rsem.at[par, q - 1], (y, dest))

    def x_recv(par, q):
        rdma(xs.at[0], xr.at[par, (t + 4 - q) % 4], x_ssem.at[q - 1], x_rsem.at[par, q - 1], sib).wait_recv()

    def put_out(vec, par):
        for d in range(2):
            for i in range(4):
                blk = jnp.concatenate(
                    [vec[4 * i + k, :, pl.ds(128 * d, 128)] for k in range(4)], axis=0).T
                xs[2 * d, i] = blk[:64]
                xs[2 * d + 1, i] = blk[64:]
        xr[par, t] = xs[t]

    def x_start(par):
        for q in range(1, 4):
            x_copy(par, q).start()

    def x_wait_send(par):
        for q in range(1, 4):
            x_copy(par, q).wait_send()

    def merged(par):
        seg = lax.broadcasted_iota(jnp.int32, (64, 128), 1) // 32
        for i in range(4):
            parts = [xr[par, src, i] for src in range(4)]
            for k in range(4):
                res = parts[k]
                for src in range(4):
                    if src != k:
                        res = jnp.where(seg == src, pltpu.roll(parts[src], (32 * (src - k)) % 128, 1), res)
                yield 4 * i + k, res

    def merge_out(j, par):
        for q in range(1, 4):
            x_recv(par, q)

        @pl.when(j > 1)
        def _():
            out_copy(j - 2).wait()

        for p, res in merged(par):
            osb[j % 2, pl.ds(p, 64, stride=16), :] = res
        out_copy(j).start()

    def everywhere(s):
        s = jnp.sum(jnp.sum(s, axis=1, keepdims=True), axis=0, keepdims=True)
        return jnp.broadcast_to(s, (1, 128))

    def fold(v):
        v = v[:, :HALF] + v[:, HALF:]
        return jnp.sum(v.reshape(COLS // 8, 8, 128), axis=0)

    def wide(row):
        return jnp.concatenate([row, row], axis=1)

    def step(j, carry):
        acc[...] = jnp.zeros((PAIR, COLS, BOND), F32)

        @pl.when(j == 0)
        def _():
            lax.fori_loop(0, 4, first_block, 0)

        @pl.when(j > 0)
        def _():
            lax.fori_loop(0, 5, gather_r, 0)
            lax.fori_loop(0, 4, gather_wl, 0)
            x_start((j + 1) % 2)
            lax.fori_loop(0, 4, second_r, 0)
            lax.fori_loop(0, 4, second_wl, 0)

        cur = j % 3
        prev = (j + 2) % 3
        nxt = (j + 1) % 3
        par = j % 2

        @pl.when(j == STEPS - 1)
        def _():
            x_wait_send(1 - par)
            put_out(acc, par)
            x_start(par)

        beta_prev = wide(betas[...])
        zero = jnp.zeros((8, 128), F32)

        def pass1(p, s):
            a_s, t_s, v_s = s
            w = acc[p]
            v = vb[cur, p]
            r = w - beta_prev * vb[prev, p]
            vb[nxt, p] = r
            return a_s + fold(w * v), t_s + fold(r * v), v_s + fold(v * v)

        a_s, t_s, v_s = lax.fori_loop(0, PAIR, pass1, (zero, zero, zero))
        a_d, t_d, v_d = everywhere(a_s), everywhere(t_s), everywhere(v_s)
        shift = jnp.where(v_d > 0.0, t_d / jnp.where(v_d > 0.0, v_d, 1.0), 0.0)
        shift_w = wide(shift)

        def pass2(p, s):
            q_s, p_s = s
            v = vb[cur, p]
            r = vb[nxt, p] - shift_w * v
            vb[nxt, p] = r
            return q_s + fold(r * r), p_s + fold(r * v)

        q_s, p_s = lax.fori_loop(0, PAIR, pass2, (zero, zero))
        st[par, me] = jnp.concatenate(
            [a_d, shift, v_d, everywhere(q_s), everywhere(p_s), jnp.zeros((3, 128), F32)], axis=0)

        def st_copy(q):
            d = (me + q) % 8
            return rdma(st.at[par, me], st.at[par, me], st_ssem.at[q - 1], st_rsem.at[q - 1], (d // 4, d % 4))

        for q in range(1, 8):
            st_copy(q).start()

        @pl.when(j > 0)
        def _():
            merge_out(j, 1 - par)

        for q in range(1, 8):
            src = (me + 8 - q) % 8
            rdma(st.at[par, me], st.at[par, src], st_ssem.at[q - 1], st_rsem.at[q - 1], sib).wait_recv()

        alpha = st[par, 0][0:1]
        for d in range(1, 8):
            alpha = alpha + st[par, d][0:1]
        alpha = alpha * (1.0 / ELEMS)
        beta2 = jnp.zeros((1, 128), F32)
        for d in range(8):
            tile = st[par, d]
            gap = alpha - tile[1:2]
            beta2 = beta2 + (tile[3:4] - 2.0 * gap * tile[4:5] + gap * gap * tile[2:3])
        beta = jnp.sqrt(beta2 * (1.0 / ELEMS))
        betas[...] = beta
        coef[0] = alpha
        coef[1] = beta_prev[:, :HALF]
        ab_ref[j] = jnp.concatenate([alpha, beta, jnp.zeros((6, 128), F32)], axis=0)
        gap_w = wide(alpha - shift)
        beta_w = wide(beta)
        rows = pl.ds(pl.multiple_of(32 * me, 32), 32)

        def pass3(m, carry):
            for i in range(4):
                p = 4 * m + i
                v = (vb[nxt, p] - gap_w * vb[cur, p]) / beta_w
                vb[nxt, p] = v
                uT[0, p, rows, :] = v[:, :HALF].astype(BF16)
                uT[1, p, rows, :] = v[:, HALF:].astype(BF16)

            for s in range(4):
                u_own(0, m, s).start()
            return carry

        @pl.when(j < STEPS - 1)
        def _():
            lax.fori_loop(0, 4, pass3, 0)

        @pl.when((j > 0) & (j < STEPS - 1))
        def _():
            x_wait_send(1 - par)

        @pl.when(j < STEPS - 1)
        def _():
            put_out(vb.at[nxt], par)

        for q in range(1, 8):
            st_copy(q).wait_send()
        return carry

    lax.fori_loop(0, STEPS, step, 0)

    last = (STEPS - 1) % 2
    for q in range(1, 4):
        x_recv(last, q)
    out_copy(STEPS - 2).wait()
    for p, res in merged(last):
        at = pl.ds(p, 64, stride=16)
        res = res - coef[0] * osb[(STEPS - 1) % 2, at, :] - coef[1] * osb[STEPS % 2, at, :]
        osb[STEPS % 2, at, :] = res / betas[...]
    out_copy(STEPS).start()
    x_wait_send(last)
    out_copy(STEPS - 1).wait()
    out_copy(STEPS).wait()

    l_sib().wait_send()
    for i in range(3):
        w_send(i).wait_send()
    for i in range(5):
        r_send(i).wait_send()
    for i in range(4):
        for part in range(2):
            l_dir(i, part).wait_send()
        for kind in range(3):
            l_step(i, kind).wait_send()


def solution(mesh):
    def body_fn(wavefunc, left_loc, two_loc, right_loc):
        bond, phys = wavefunc.shape[0], wavefunc.shape[1]
        wf = wavefunc.reshape(bond, phys, phys, 2, 128).transpose(0, 1, 3, 2, 4).reshape(-1, 128)
        dma = pltpu.SemaphoreType.DMA
        kry, ab = pl.pallas_call(
            lanczos_kernel,
            out_shape=(
                jax.ShapeDtypeStruct((STEPS + 1, 64 * PAIR, 128), F32),
                jax.ShapeDtypeStruct((STEPS, 8, 128), F32),
            ),
            in_specs=[
                pl.BlockSpec(memory_space=pl.ANY),
                pl.BlockSpec(memory_space=pl.ANY),
                pl.BlockSpec(memory_space=pltpu.VMEM),
                pl.BlockSpec(memory_space=pl.ANY),
            ],
            out_specs=(pl.BlockSpec(memory_space=pl.ANY), pl.BlockSpec(memory_space=pltpu.VMEM)),
            scratch_shapes=[
                pltpu.VMEM((8192, 128), F32),
                pltpu.VMEM((TERMS, COLS, BOND), BF16),
                pltpu.VMEM((TERMS, BOND, BOND), BF16),
                pltpu.VMEM((32, 384, 128), BF16),
                pltpu.VMEM((TERMS, BOND, BOND), BF16),
                pltpu.VMEM((4, PAIR, BOND), BF16),
                pltpu.VMEM((BOND, BOND), F32),
                pltpu.VMEM((TERMS, PAIR, COLS, HALF), BF16),
                pltpu.VMEM((PAIR, COLS, BLOCK * HALF), BF16),
                pltpu.VMEM((2, PAIR, BOND, HALF), BF16),
                pltpu.VMEM((PAIR, COLS, BOND), F32),
                pltpu.VMEM((3, PAIR, COLS, BOND), F32),
                pltpu.VMEM((2, 128, 128), F32),
                pltpu.VMEM((2, 8, 8, 128), F32),
                pltpu.VMEM((1, 128), F32),
                pltpu.VMEM((2, 1, 128), F32),
                pltpu.VMEM((4, 4, 64, 128), F32),
                pltpu.VMEM((2, 4, 4, 64, 128), F32),
                pltpu.VMEM((2, 64 * PAIR, 128), F32),
                dma((3,)),
                dma((3,)), dma((3,)),
                dma((5,)), dma((5,)),
                dma((9,)), dma((9,)),
                dma((3, 4)), dma((3, 4)),
                dma((2, 4, 4)), dma((2, 4, 4)),
                dma((2, 4, 3)), dma((2, 4, 3)),
                dma((7,)), dma((7,)),
                dma((3,)), dma((2, 3)),
                dma((2,)),
            ],
            compiler_params=pltpu.CompilerParams(
                collective_id=0, has_side_effects=True, vmem_limit_bytes=66 * 1000 * 1000),
        )(wf, left_loc, two_loc, right_loc)
        krylov = kry.reshape(STEPS + 1, 64, phys, phys, 128)
        return krylov, ab[:, 0, 0], ab[:, 1, 0]

    return jax.shard_map(
        body_fn, mesh=mesh,
        in_specs=(P(), P('terms'), P('terms'), P('terms', 'rows')),
        out_specs=(P(None, 'terms', None, None, 'rows'), P(), P()), check_vma=False)
```

```python
import jax
import jax.numpy as jnp
from jax import lax
from jax.experimental import pallas as pl
from jax.experimental.pallas import tpu as pltpu
from jax.sharding import PartitionSpec as P

STEPS = 6
PAIR = 16
BOND = 256
TERMS = 64
BLOCK = 16
HALF = 128
COLS = 32
ELEMS = float(BOND * BOND * PAIR)
F32 = jnp.float32
BF16 = jnp.bfloat16


def lanczos_kernel(
    wf_hbm, left_hbm, two_ref, right_hbm, kry_hbm, ab_ref,
    wfv, rw, lw, lx, bd, wt, mask, yb, zb, uT, acc, vb, tmp, st, betas, coef, xs, xr, osb,
    loc_sem, w_ssem, w_rsem, r_ssem, r_rsem, l_ssem, l_rsem, lx_ssem, lx_rsem,
    u_ssem, u_rsem, f_ssem, f_rsem, st_ssem, st_rsem, x_ssem, x_rsem, o_sem,
):
    y = lax.axis_index("rows")
    t = lax.axis_index("terms")
    x = t // 2
    c = t % 2
    me = y * 4 + t
    sib = (y, 2 * x + (1 - c))
    xnb = (y, 2 * (1 - x) + c)
    xno = (y, 2 * (1 - x) + (1 - c))
    ynb = (1 - y, t)
    diag = (1 - y, 2 * (1 - x) + c)
    flip = 1 - 2 * c
    near = (4 * y + 2 * (1 - x) + c, 4 * (1 - y) + t, 4 * (1 - y) + 2 * (1 - x) + c)

    def rdma(src, dst, ssem, rsem, dev):
        return pltpu.make_async_remote_copy(
            src_ref=src, dst_ref=dst, send_sem=ssem, recv_sem=rsem,
            device_id=dev, device_id_type=pl.DeviceIdType.MESH)

    cp_wf = pltpu.make_async_copy(wf_hbm, wfv, loc_sem.at[0])
    cp_r = pltpu.make_async_copy(right_hbm.at[:, pl.ds(32 * t, 32), :], rw.at[pl.ds(0, 16)], loc_sem.at[1])
    cp_l = pltpu.make_async_copy(left_hbm, lw.at[pl.ds(0, 16)], loc_sem.at[2])
    cp_wf.start()
    cp_r.start()
    cp_l.start()

    barrier = pltpu.get_barrier_semaphore()
    for q in range(1, 8):
        d = (me + q) % 8
        pl.semaphore_signal(barrier, inc=1, device_id=(d // 4, d % 4), device_id_type=pl.DeviceIdType.MESH)
    pl.semaphore_wait(barrier, 7)

    def l_sib():
        return rdma(left_hbm, lw.at[pl.ds(16, 16)], l_ssem.at[0], l_rsem.at[0], sib)

    def l_dir(i, part):
        rows = pl.ds(0, 256) if part == 0 else pl.ds(128, 128)
        return rdma(left_hbm.at[pl.ds(8 * y + 2 * i, 2), rows, pl.ds(128 * part, 128)],
                    lx.at[pl.ds(2 * i, 2), pl.ds(256 * part, 256 - 128 * part), :],
                    l_ssem.at[1 + 2 * i + part], l_rsem.at[1 + 2 * i + part], xnb)

    def l_step(i, kind):
        src, dst, dev = ((0, 8, sib), (0, 16, ynb), (16, 24, sib))[kind]
        return rdma(lx.at[pl.ds(src + 2 * i, 2)], lx.at[pl.ds(dst + 2 * i, 2)],
                    lx_ssem.at[kind, i], lx_rsem.at[kind, i], dev)

    def l_take(i):
        for part in range(2):
            l_dir(i, part).wait_recv()
        l_step(i, 0).start()
        l_step(i, 1).start()

    def l_unpack(k, g):
        src = 8 * (g - 4) + k
        dst = 8 * g + k
        low = lx[src, pl.ds(128, 128), :]
        lw[dst, pl.ds(0, 128), pl.ds(0, 128)] = lx[src, pl.ds(0, 128), :]
        lw[dst, pl.ds(128, 128), pl.ds(0, 128)] = low
        lw[dst, pl.ds(0, 128), pl.ds(128, 128)] = low.astype(F32).T.astype(BF16)
        lw[dst, pl.ds(128, 128), pl.ds(128, 128)] = lx[src, pl.ds(256, 128), :]
        return g

    def r_send(i):
        first, rows, dst, dev = (
            (0, 2 * x + (1 - c), 16, sib),
            (8 * y, 2 * (1 - x) + c, 32, xnb),
            (8 * y, 2 * (1 - x) + (1 - c), 40, xno),
            (8 * (1 - y), 2 * (1 - x) + c, 48, xnb),
            (8 * (1 - y), 2 * (1 - x) + (1 - c), 56, xno),
        )[i]
        n = 16 if i == 0 else 8
        return rdma(right_hbm.at[pl.ds(first, n), pl.ds(32 * rows, 32), :], rw.at[pl.ds(dst, n)],
                    r_ssem.at[i], r_rsem.at[i], dev)

    for i in range(4):
        for part in range(2):
            l_dir(i, part).start()
    for i in range(5):
        r_send(i).start()
    l_sib().start()

    row16 = lax.broadcasted_iota(jnp.int32, (PAIR, BOND), 0)
    lane16 = lax.broadcasted_iota(jnp.int32, (PAIR, BOND), 1)
    packed = jnp.zeros((PAIR, BOND), F32)
    for k in range(16):
        place = (lane16 == row16 + 16 * k).astype(F32).astype(BF16)
        packed = packed + jnp.dot(two_ref[k], place, preferred_element_type=F32)
    wt[0] = packed.astype(BF16)

    def w_send(i):
        return rdma(wt.at[0], wt.at[1 + i], w_ssem.at[i], w_rsem.at[i], (sib, xnb, xno)[i])

    for i in range(3):
        w_send(i).start()

    rr = lax.broadcasted_iota(jnp.int32, (BOND, BOND), 0) % 16
    cc = lax.broadcasted_iota(jnp.int32, (BOND, BOND), 1) % 16
    mask[...] = (rr == cc).astype(F32)

    cp_wf.wait()

    def sumsq(i, s):
        blk = wfv[pl.ds(pl.multiple_of(i * 256, 256), 256), :]
        return s + jnp.sum((blk * blk).reshape(32, 8, 128), axis=0)

    total = lax.fori_loop(0, 32, sumsq, jnp.zeros((8, 128), F32))
    total = jnp.sum(jnp.sum(total, axis=1, keepdims=True), axis=0, keepdims=True)
    scale = jnp.broadcast_to(jnp.sqrt(total * (1.0 / ELEMS)), (1, 128))

    wfo = wfv.at[pl.ds(pl.multiple_of(2048 * t, 2048), 2048), :]
    own = pl.ds(pl.multiple_of(32 * t, 32), 32)
    for p in range(PAIR):
        for h in range(2):
            for bt in range(2):
                first = 4096 * h + (p // 4) * 8 + bt * 4 + p % 4
                blk = (wfv[pl.ds(first, 128, stride=32), :] / scale).T
                tmp[bt] = blk
                uT[h, p, pl.ds(128 * bt, 128), :] = blk.astype(BF16)
            vb[0, p, :, pl.ds(128 * h, 128)] = tmp[y, own, :]
        first = (p // 4) * 8 + p % 4
        lo = wfo[pl.ds(first, 64, stride=32), :]
        hi = wfo[pl.ds(first + 4, 64, stride=32), :]
        osb[0, pl.ds(p, 64, stride=16), :] = jnp.where(y == 0, lo, hi) / scale
    vb[2] = jnp.zeros((PAIR, COLS, BOND), F32)
    betas[...] = jnp.zeros((1, 128), F32)

    def out_copy(j):
        return pltpu.make_async_copy(osb.at[j % 2], kry_hbm.at[j], o_sem.at[j % 2])

    out_copy(0).start()

    def u_part(h, m, dev):
        return uT.at[h, pl.ds(4 * m, 4), pl.ds(pl.multiple_of(32 * dev, 32), 32), :]

    def u_own(h, m, s):
        part = u_part(h, m, me)
        return rdma(part, part, u_ssem.at[h, m, s], u_rsem.at[h, m, s], (xnb, ynb, diag, sib)[s])

    def u_got(h, m, s):
        part = u_part(h, m, (near + (me + flip,))[s])
        return rdma(part, part, u_ssem.at[h, m, s], u_rsem.at[h, m, s], (xnb, ynb, diag, sib)[s])

    def u_relay(h, m, s):
        part = u_part(h, m, near[s])
        return rdma(part, part, f_ssem.at[h, m, s], f_rsem.at[h, m, s], sib)

    def u_relayed(h, m, s):
        part = u_part(h, m, near[s] + flip)
        return rdma(part, part, f_ssem.at[h, m, s], f_rsem.at[h, m, s], sib)

    def relay_all(h, m):
        for s in range(3):
            u_got(h, m, s).wait_recv()
            u_relay(h, m, s).start()

    def r_stage(h, k0, nk, m):
        lhs = rw[pl.ds(k0, nk)].reshape(nk * COLS, BOND)
        rhs = jnp.concatenate([uT[h, 4 * m + i] for i in range(4)], axis=1)
        res = jnp.dot(lhs, rhs, preferred_element_type=F32).astype(BF16)
        for i in range(4):
            yb[pl.ds(k0, nk), 4 * m + i] = res[:, HALF * i:HALF * (i + 1)].reshape(nk, COLS, HALF)

    def wl_stage(h, k0, nk, buf=0):
        for k in range(nk):
            rhs = jnp.concatenate(
                [yb[k0 + k, :, pl.ds(16 * i, 16), :].reshape(BOND, HALF) for i in range(2)], axis=1)
            res = jnp.dot(bd[k0 + k], rhs, preferred_element_type=F32).astype(BF16)
            for i in range(2):
                zb[buf, :, pl.ds(16 * i, 16), pl.ds(HALF * k, HALF)] = (
                    res[:, HALF * i:HALF * (i + 1)].reshape(PAIR, 16, HALF))
        lhs = zb[buf, :, :, pl.ds(0, nk * HALF)].reshape(PAIR * COLS, nk * HALF)
        rhs = lw[pl.ds(k0, nk), pl.ds(pl.multiple_of(HALF * h, HALF), HALF), :].reshape(nk * HALF, BOND)
        res = jnp.dot(lhs, rhs, preferred_element_type=F32)
        acc[...] = acc[...] + res.reshape(PAIR, COLS, BOND)

    def build_bd(g):
        slot = (g // 4) * 2 + (1 - g // 4) * (g // 2) + (g // 4) * (g % 2)
        part = (1 - g // 4) * (g % 2) + (g // 4) * ((y + (g - 4 * (g // 4)) // 2) % 2)
        lanes = pl.multiple_of(128 * part, 128)
        ops = wt[slot, :, pl.ds(lanes, 128)].astype(F32).T.astype(BF16)
        e_t = (lax.broadcasted_iota(jnp.int32, (PAIR, BOND), 1) // 16
               == lax.broadcasted_iota(jnp.int32, (PAIR, BOND), 0)).astype(F32).astype(BF16)
        e = (lax.broadcasted_iota(jnp.int32, (BOND, PAIR), 0) // 16
             == lax.broadcasted_iota(jnp.int32, (BOND, PAIR), 1)).astype(F32).astype(BF16)
        wide = jnp.dot(ops, e_t, preferred_element_type=F32).astype(BF16)
        for k in range(8):
            full = jnp.dot(e, wide[16 * k:16 * (k + 1), :], preferred_element_type=F32)
            bd[g * 8 + k] = (full * mask[...]).astype(BF16)

    def first_half(h, k0, nk):
        for m in range(4):
            r_stage(h, k0, nk, m)
        wl_stage(h, k0, nk)

    def bd_group(g, carry):
        build_bd(g)
        return carry

    def first_block(s, carry):
        @pl.when(s == 0)
        def _():
            cp_r.wait()
            cp_l.wait()
            lax.fori_loop(0, 2, bd_group, 0)
            l_take(0)

        @pl.when(s == 1)
        def _():
            for i in range(3):
                w_send(i).wait_recv()
            lax.fori_loop(2, 8, bd_group, 0)
            l_take(1)
            r_send(0).wait_recv()
            l_sib().wait_recv()

        @pl.when(s == 2)
        def _():
            l_take(2)
            l_take(3)
            lax.fori_loop(0, 8, l_unpack, 4)
            for i in range(4):
                l_step(i, 0).wait_recv()
            lax.fori_loop(0, 8, l_unpack, 5)
            for i in range(4):
                l_step(i, 1).wait_recv()
                l_step(i, 2).start()
            r_send(1).wait_recv()
            r_send(2).wait_recv()

        def half(h, carry):
            first_half(h, s * BLOCK, BLOCK)
            return carry

        lax.fori_loop(0, 2, half, 0)
        return carry

    def last_group(g, carry):
        @pl.when(g == 6)
        def _():
            lax.fori_loop(0, 8, l_unpack, 6)
            for i in range(4):
                l_step(i, 2).wait_recv()
            lax.fori_loop(0, 8, l_unpack, 7)
            r_send(3).wait_recv()

        @pl.when(g == 7)
        def _():
            r_send(4).wait_recv()

        def half(h, carry):
            first_half(h, g * 8, 8)
            return carry

        lax.fori_loop(0, 2, half, 0)
        return carry

    def gather_r(i, carry):
        @pl.when(i < 4)
        def _():
            relay_all(0, i)

        @pl.when(i >= 1)
        def _():
            later_r(0, i - 1)

        return carry

    def u_all(h, m):
        u_got(h, m, 3).wait_recv()
        for s in range(3):
            u_relayed(h, m, s).wait_recv()

    def later_r(h, m):
        u_all(h, m)
        r_stage(h, 0, TERMS, m)

    def gather_wl(s, carry):
        relay_all(1, s)
        wl_stage(0, s * BLOCK, BLOCK)
        return carry

    def second():
        for m in range(4):
            u_all(1, m)
        for m in range(4):
            r_stage(1, 0, TERMS, m)
        for s in range(4):
            wl_stage(1, s * BLOCK, BLOCK, s % 2)

    def sent(m, carry):
        for h in range(2):
            for s in range(4):
                u_own(h, m, s).wait_send()
            for s in range(3):
                u_relay(h, m, s).wait_send()
        return carry

    def x_copy(par, q):
        dest = (t + q) % 4
        return rdma(xs.at[dest], xr.at[par, t], x_ssem.at[q - 1], x_rsem.at[par, q - 1], (y, dest))

    def x_recv(par, q):
        rdma(xs.at[0], xr.at[par, (t + 4 - q) % 4], x_ssem.at[q - 1], x_rsem.at[par, q - 1], sib).wait_recv()

    def put_out(vec, par):
        for d in range(2):
            for i in range(4):
                blk = jnp.concatenate(
                    [vec[4 * i + k, :, pl.ds(128 * d, 128)] for k in range(4)], axis=0).T
                xs[2 * d, i] = blk[:64]
                xs[2 * d + 1, i] = blk[64:]
        xr[par, t] = xs[t]

    def x_start(par):
        for q in range(1, 4):
            x_copy(par, q).start()

    def x_wait_send(par):
        for q in range(1, 4):
            x_copy(par, q).wait_send()

    def merged(par):
        seg = lax.broadcasted_iota(jnp.int32, (64, 128), 1) // 32
        for i in range(4):
            parts = [xr[par, src, i] for src in range(4)]
            for k in range(4):
                res = parts[k]
                for src in range(4):
                    if src != k:
                        res = jnp.where(seg == src, pltpu.roll(parts[src], (32 * (src - k)) % 128, 1), res)
                yield 4 * i + k, res

    def merge_out(j, par):
        for q in range(1, 4):
            x_recv(par, q)

        @pl.when(j > 1)
        def _():
            out_copy(j - 2).wait()

        for p, res in merged(par):
            osb[j % 2, pl.ds(p, 64, stride=16), :] = res
        out_copy(j).start()

    def everywhere(s):
        s = jnp.sum(jnp.sum(s, axis=1, keepdims=True), axis=0, keepdims=True)
        return jnp.broadcast_to(s, (1, 128))

    def fold(v):
        v = v[:, :HALF] + v[:, HALF:]
        return jnp.sum(v.reshape(COLS // 8, 8, 128), axis=0)

    def wide(row):
        return jnp.concatenate([row, row], axis=1)

    def step(j, carry):
        acc[...] = jnp.zeros((PAIR, COLS, BOND), F32)

        @pl.when(j == 0)
        def _():
            lax.fori_loop(0, 3, first_block, 0)
            lax.fori_loop(6, 8, last_group, 0)

        @pl.when(j > 0)
        def _():
            lax.fori_loop(0, 5, gather_r, 0)
            lax.fori_loop(0, 4, gather_wl, 0)
            x_start((j + 1) % 2)
            second()
            lax.fori_loop(0, 4, sent, 0)

        cur = j % 3
        prev = (j + 2) % 3
        nxt = (j + 1) % 3
        par = j % 2

        @pl.when(j == STEPS - 1)
        def _():
            x_wait_send(1 - par)
            put_out(acc, par)
            x_start(par)

        beta_prev = wide(betas[...])
        zero = jnp.zeros((8, 128), F32)

        def pass1(p, s):
            a_s, t_s, v_s = s
            w = acc[p]
            v = vb[cur, p]
            r = w - beta_prev * vb[prev, p]
            vb[nxt, p] = r
            return a_s + fold(w * v), t_s + fold(r * v), v_s + fold(v * v)

        a_s, t_s, v_s = lax.fori_loop(0, PAIR, pass1, (zero, zero, zero))
        a_d, t_d, v_d = everywhere(a_s), everywhere(t_s), everywhere(v_s)
        shift = jnp.where(v_d > 0.0, t_d / jnp.where(v_d > 0.0, v_d, 1.0), 0.0)
        shift_w = wide(shift)

        def pass2(p, s):
            q_s, p_s = s
            v = vb[cur, p]
            r = vb[nxt, p] - shift_w * v
            vb[nxt, p] = r
            return q_s + fold(r * r), p_s + fold(r * v)

        q_s, p_s = lax.fori_loop(0, PAIR, pass2, (zero, zero))
        st[par, me] = jnp.concatenate(
            [a_d, shift, v_d, everywhere(q_s), everywhere(p_s), jnp.zeros((3, 128), F32)], axis=0)

        def st_copy(q):
            d = (me + q) % 8
            return rdma(st.at[par, me], st.at[par, me], st_ssem.at[q - 1], st_rsem.at[q - 1], (d // 4, d % 4))

        for q in range(1, 8):
            st_copy(q).start()

        @pl.when(j > 0)
        def _():
            merge_out(j, 1 - par)

        for q in range(1, 8):
            src = (me + 8 - q) % 8
            rdma(st.at[par, me], st.at[par, src], st_ssem.at[q - 1], st_rsem.at[q - 1], sib).wait_recv()

        alpha = st[par, 0][0:1]
        for d in range(1, 8):
            alpha = alpha + st[par, d][0:1]
        alpha = alpha * (1.0 / ELEMS)
        beta2 = jnp.zeros((1, 128), F32)
        for d in range(8):
            tile = st[par, d]
            gap = alpha - tile[1:2]
            beta2 = beta2 + (tile[3:4] - 2.0 * gap * tile[4:5] + gap * gap * tile[2:3])
        beta = jnp.sqrt(beta2 * (1.0 / ELEMS))
        betas[...] = beta
        coef[0] = alpha
        coef[1] = beta_prev[:, :HALF]
        ab_ref[j] = jnp.concatenate([alpha, beta, jnp.zeros((6, 128), F32)], axis=0)
        gap_w = wide(alpha - shift)
        beta_w = wide(beta)
        rows = pl.ds(pl.multiple_of(32 * me, 32), 32)

        def pass3(m, carry):
            for i in range(4):
                p = 4 * m + i
                v = (vb[nxt, p] - gap_w * vb[cur, p]) / beta_w
                vb[nxt, p] = v
                uT[0, p, rows, :] = v[:, :HALF].astype(BF16)
                uT[1, p, rows, :] = v[:, HALF:].astype(BF16)

            for s in (2, 0, 1, 3):
                u_own(0, m, s).start()
            return carry

        @pl.when(j < STEPS - 1)
        def _():
            lax.fori_loop(0, 4, pass3, 0)
            for m in range(4):
                for s in (2, 0, 1, 3):
                    u_own(1, m, s).start()

        @pl.when((j > 0) & (j < STEPS - 1))
        def _():
            x_wait_send(1 - par)

        @pl.when(j < STEPS - 1)
        def _():
            put_out(vb.at[nxt], par)

        for q in range(1, 8):
            st_copy(q).wait_send()
        return carry

    lax.fori_loop(0, STEPS, step, 0)

    last = (STEPS - 1) % 2
    for q in range(1, 4):
        x_recv(last, q)
    out_copy(STEPS - 2).wait()
    for p, res in merged(last):
        at = pl.ds(p, 64, stride=16)
        res = res - coef[0] * osb[(STEPS - 1) % 2, at, :] - coef[1] * osb[STEPS % 2, at, :]
        osb[STEPS % 2, at, :] = res / betas[...]
    out_copy(STEPS).start()
    x_wait_send(last)
    out_copy(STEPS - 1).wait()
    out_copy(STEPS).wait()

    l_sib().wait_send()
    for i in range(3):
        w_send(i).wait_send()
    for i in range(5):
        r_send(i).wait_send()
    for i in range(4):
        for part in range(2):
            l_dir(i, part).wait_send()
        for kind in range(3):
            l_step(i, kind).wait_send()


def solution(mesh):
    def body_fn(wavefunc, left_loc, two_loc, right_loc):
        bond, phys = wavefunc.shape[0], wavefunc.shape[1]
        wf = wavefunc.reshape(bond, phys, phys, 2, 128).transpose(0, 1, 3, 2, 4).reshape(-1, 128)
        dma = pltpu.SemaphoreType.DMA
        kry, ab = pl.pallas_call(
            lanczos_kernel,
            out_shape=(
                jax.ShapeDtypeStruct((STEPS + 1, 64 * PAIR, 128), F32),
                jax.ShapeDtypeStruct((STEPS, 8, 128), F32),
            ),
            in_specs=[
                pl.BlockSpec(memory_space=pl.ANY),
                pl.BlockSpec(memory_space=pl.ANY),
                pl.BlockSpec(memory_space=pltpu.VMEM),
                pl.BlockSpec(memory_space=pl.ANY),
            ],
            out_specs=(pl.BlockSpec(memory_space=pl.ANY), pl.BlockSpec(memory_space=pltpu.VMEM)),
            scratch_shapes=[
                pltpu.VMEM((8192, 128), F32),
                pltpu.VMEM((TERMS, COLS, BOND), BF16),
                pltpu.VMEM((TERMS, BOND, BOND), BF16),
                pltpu.VMEM((32, 384, 128), BF16),
                pltpu.VMEM((TERMS, BOND, BOND), BF16),
                pltpu.VMEM((4, PAIR, BOND), BF16),
                pltpu.VMEM((BOND, BOND), F32),
                pltpu.VMEM((TERMS, PAIR, COLS, HALF), BF16),
                pltpu.VMEM((2, PAIR, COLS, BLOCK * HALF), BF16),
                pltpu.VMEM((2, PAIR, BOND, HALF), BF16),
                pltpu.VMEM((PAIR, COLS, BOND), F32),
                pltpu.VMEM((3, PAIR, COLS, BOND), F32),
                pltpu.VMEM((2, 128, 128), F32),
                pltpu.VMEM((2, 8, 8, 128), F32),
                pltpu.VMEM((1, 128), F32),
                pltpu.VMEM((2, 1, 128), F32),
                pltpu.VMEM((4, 4, 64, 128), F32),
                pltpu.VMEM((2, 4, 4, 64, 128), F32),
                pltpu.VMEM((2, 64 * PAIR, 128), F32),
                dma((3,)),
                dma((3,)), dma((3,)),
                dma((5,)), dma((5,)),
                dma((9,)), dma((9,)),
                dma((3, 4)), dma((3, 4)),
                dma((2, 4, 4)), dma((2, 4, 4)),
                dma((2, 4, 3)), dma((2, 4, 3)),
                dma((7,)), dma((7,)),
                dma((3,)), dma((2, 3)),
                dma((2,)),
            ],
            compiler_params=pltpu.CompilerParams(
                collective_id=0, has_side_effects=True, vmem_limit_bytes=66 * 1000 * 1000),
        )(wf, left_loc, two_loc, right_loc)
        krylov = kry.reshape(STEPS + 1, 64, phys, phys, 128)
        return krylov, ab[:, 0, 0], ab[:, 1, 0]

    return jax.shard_map(
        body_fn, mesh=mesh,
        in_specs=(P(), P('terms'), P('terms'), P('terms', 'rows')),
        out_specs=(P(None, 'terms', None, None, 'rows'), P(), P()), check_vma=False)
```

```python
import jax
import jax.numpy as jnp
from jax import lax
from jax.experimental import pallas as pl
from jax.experimental.pallas import tpu as pltpu
from jax.sharding import PartitionSpec as P

STEPS = 6
PAIR = 16
BOND = 256
TERMS = 64
BLOCK = 16
HALF = 128
COLS = 32
ELEMS = float(BOND * BOND * PAIR)
F32 = jnp.float32
BF16 = jnp.bfloat16


def lanczos_kernel(
    wf_hbm, left_hbm, two_ref, right_hbm, kry_hbm, ab_ref,
    wfv, rw, lw, lx, bd, wt, mask, yb, zb, uT, acc, vb, tmp, st, betas, coef, xs, xr, osb,
    loc_sem, w_ssem, w_rsem, r_ssem, r_rsem, l_ssem, l_rsem, lx_ssem, lx_rsem,
    u_ssem, u_rsem, f_ssem, f_rsem, st_ssem, st_rsem, x_ssem, x_rsem, o_sem,
):
    y = lax.axis_index("rows")
    t = lax.axis_index("terms")
    x = t // 2
    c = t % 2
    me = y * 4 + t
    sib = (y, 2 * x + (1 - c))
    xnb = (y, 2 * (1 - x) + c)
    xno = (y, 2 * (1 - x) + (1 - c))
    ynb = (1 - y, t)
    diag = (1 - y, 2 * (1 - x) + c)
    flip = 1 - 2 * c
    near = (4 * y + 2 * (1 - x) + c, 4 * (1 - y) + t, 4 * (1 - y) + 2 * (1 - x) + c)

    def rdma(src, dst, ssem, rsem, dev):
        return pltpu.make_async_remote_copy(
            src_ref=src, dst_ref=dst, send_sem=ssem, recv_sem=rsem,
            device_id=dev, device_id_type=pl.DeviceIdType.MESH)

    cp_wf = pltpu.make_async_copy(wf_hbm, wfv, loc_sem.at[0])
    cp_r = pltpu.make_async_copy(right_hbm.at[:, pl.ds(32 * t, 32), :], rw.at[pl.ds(0, 16)], loc_sem.at[1])
    cp_l = pltpu.make_async_copy(left_hbm, lw.at[pl.ds(0, 16)], loc_sem.at[2])
    cp_wf.start()
    cp_r.start()
    cp_l.start()

    barrier = pltpu.get_barrier_semaphore()
    for q in range(1, 8):
        d = (me + q) % 8
        pl.semaphore_signal(barrier, inc=1, device_id=(d // 4, d % 4), device_id_type=pl.DeviceIdType.MESH)
    pl.semaphore_wait(barrier, 7)

    def l_sib():
        return rdma(left_hbm, lw.at[pl.ds(16, 16)], l_ssem.at[0], l_rsem.at[0], sib)

    def l_dir(i, part):
        rows = pl.ds(0, 256) if part == 0 else pl.ds(128, 128)
        return rdma(left_hbm.at[pl.ds(8 * y + 2 * i, 2), rows, pl.ds(128 * part, 128)],
                    lx.at[pl.ds(2 * i, 2), pl.ds(256 * part, 256 - 128 * part), :],
                    l_ssem.at[1 + 2 * i + part], l_rsem.at[1 + 2 * i + part], xnb)

    def l_step(i, kind):
        src, dst, dev = ((0, 8, sib), (0, 16, ynb), (16, 24, sib))[kind]
        return rdma(lx.at[pl.ds(src + 2 * i, 2)], lx.at[pl.ds(dst + 2 * i, 2)],
                    lx_ssem.at[kind, i], lx_rsem.at[kind, i], dev)

    def l_take(i):
        for part in range(2):
            l_dir(i, part).wait_recv()
        l_step(i, 0).start()
        l_step(i, 1).start()

    def l_unpack(k, g):
        src = 8 * (g - 4) + k
        dst = 8 * g + k
        low = lx[src, pl.ds(128, 128), :]
        lw[dst, pl.ds(0, 128), pl.ds(0, 128)] = lx[src, pl.ds(0, 128), :]
        lw[dst, pl.ds(128, 128), pl.ds(0, 128)] = low
        lw[dst, pl.ds(0, 128), pl.ds(128, 128)] = low.astype(F32).T.astype(BF16)
        lw[dst, pl.ds(128, 128), pl.ds(128, 128)] = lx[src, pl.ds(256, 128), :]
        return g

    def r_send(i):
        first, rows, dst, dev = (
            (0, 2 * x + (1 - c), 16, sib),
            (8 * y, 2 * (1 - x) + c, 32, xnb),
            (8 * y, 2 * (1 - x) + (1 - c), 40, xno),
            (8 * (1 - y), 2 * (1 - x) + c, 48, xnb),
            (8 * (1 - y), 2 * (1 - x) + (1 - c), 56, xno),
        )[i]
        n = 16 if i == 0 else 8
        return rdma(right_hbm.at[pl.ds(first, n), pl.ds(32 * rows, 32), :], rw.at[pl.ds(dst, n)],
                    r_ssem.at[i], r_rsem.at[i], dev)

    for i in range(4):
        for part in range(2):
            l_dir(i, part).start()
    for i in range(5):
        r_send(i).start()
    l_sib().start()

    row16 = lax.broadcasted_iota(jnp.int32, (PAIR, BOND), 0)
    lane16 = lax.broadcasted_iota(jnp.int32, (PAIR, BOND), 1)
    packed = jnp.zeros((PAIR, BOND), F32)
    for k in range(16):
        place = (lane16 == row16 + 16 * k).astype(F32).astype(BF16)
        packed = packed + jnp.dot(two_ref[k], place, preferred_element_type=F32)
    wt[0] = packed.astype(BF16)

    def w_send(i):
        return rdma(wt.at[0], wt.at[1 + i], w_ssem.at[i], w_rsem.at[i], (sib, xnb, xno)[i])

    for i in range(3):
        w_send(i).start()

    rr = lax.broadcasted_iota(jnp.int32, (BOND, BOND), 0) % 16
    cc = lax.broadcasted_iota(jnp.int32, (BOND, BOND), 1) % 16
    mask[...] = (rr == cc).astype(F32)

    cp_wf.wait()

    def sumsq(i, s):
        blk = wfv[pl.ds(pl.multiple_of(i * 256, 256), 256), :]
        return s + jnp.sum((blk * blk).reshape(32, 8, 128), axis=0)

    total = lax.fori_loop(0, 32, sumsq, jnp.zeros((8, 128), F32))
    total = jnp.sum(jnp.sum(total, axis=1, keepdims=True), axis=0, keepdims=True)
    scale = jnp.broadcast_to(jnp.sqrt(total * (1.0 / ELEMS)), (1, 128))

    wfo = wfv.at[pl.ds(pl.multiple_of(2048 * t, 2048), 2048), :]
    own = pl.ds(pl.multiple_of(32 * t, 32), 32)
    for p in range(PAIR):
        for h in range(2):
            for bt in range(2):
                first = 4096 * h + (p // 4) * 8 + bt * 4 + p % 4
                blk = (wfv[pl.ds(first, 128, stride=32), :] / scale).T
                tmp[bt] = blk
                uT[h, p, pl.ds(128 * bt, 128), :] = blk.astype(BF16)
            vb[0, p, :, pl.ds(128 * h, 128)] = tmp[y, own, :]
        first = (p // 4) * 8 + p % 4
        lo = wfo[pl.ds(first, 64, stride=32), :]
        hi = wfo[pl.ds(first + 4, 64, stride=32), :]
        osb[0, pl.ds(p, 64, stride=16), :] = jnp.where(y == 0, lo, hi) / scale
    vb[2] = jnp.zeros((PAIR, COLS, BOND), F32)
    betas[...] = jnp.zeros((1, 128), F32)

    def out_copy(j):
        return pltpu.make_async_copy(osb.at[j % 2], kry_hbm.at[j], o_sem.at[j % 2])

    out_copy(0).start()

    def u_part(h, m, dev):
        return uT.at[h, pl.ds(4 * m, 4), pl.ds(pl.multiple_of(32 * dev, 32), 32), :]

    def u_own(h, m, s):
        part = u_part(h, m, me)
        return rdma(part, part, u_ssem.at[h, m, s], u_rsem.at[h, m, s], (xnb, ynb, diag, sib)[s])

    def u_got(h, m, s):
        part = u_part(h, m, (near + (me + flip,))[s])
        return rdma(part, part, u_ssem.at[h, m, s], u_rsem.at[h, m, s], (xnb, ynb, diag, sib)[s])

    def u_relay(h, m, s):
        part = u_part(h, m, near[s])
        return rdma(part, part, f_ssem.at[h, m, s], f_rsem.at[h, m, s], sib)

    def u_relayed(h, m, s):
        part = u_part(h, m, near[s] + flip)
        return rdma(part, part, f_ssem.at[h, m, s], f_rsem.at[h, m, s], sib)

    def relay_all(h, m):
        for s in range(3):
            u_got(h, m, s).wait_recv()
            u_relay(h, m, s).start()

    def r_stage(h, k0, nk, n):
        lhs = rw[pl.ds(k0, nk)].reshape(nk * COLS, BOND)
        rhs = jnp.concatenate([uT[h, 2 * n], uT[h, 2 * n + 1]], axis=1)
        res = jnp.dot(lhs, rhs, preferred_element_type=F32).astype(BF16)
        yb[pl.ds(k0, nk), 2 * n] = res[:, :HALF].reshape(nk, COLS, HALF)
        yb[pl.ds(k0, nk), 2 * n + 1] = res[:, HALF:].reshape(nk, COLS, HALF)

    def wl_stage(h, k0, nk):
        for k in range(nk):
            rhs = jnp.concatenate(
                [yb[k0 + k, :, pl.ds(16 * i, 16), :].reshape(BOND, HALF) for i in range(2)], axis=1)
            res = jnp.dot(bd[k0 + k], rhs, preferred_element_type=F32).astype(BF16)
            for i in range(2):
                zb[:, pl.ds(16 * i, 16), pl.ds(HALF * k, HALF)] = (
                    res[:, HALF * i:HALF * (i + 1)].reshape(PAIR, 16, HALF))
        lhs = zb[:, :, pl.ds(0, nk * HALF)].reshape(PAIR * COLS, nk * HALF)
        rhs = lw[pl.ds(k0, nk), pl.ds(pl.multiple_of(HALF * h, HALF), HALF), :].reshape(nk * HALF, BOND)
        res = jnp.dot(lhs, rhs, preferred_element_type=F32)
        acc[...] = acc[...] + res.reshape(PAIR, COLS, BOND)

    def build_bd(g):
        slot = (g // 4) * 2 + (1 - g // 4) * (g // 2) + (g // 4) * (g % 2)
        part = (1 - g // 4) * (g % 2) + (g // 4) * ((y + (g - 4 * (g // 4)) // 2) % 2)
        lanes = pl.multiple_of(128 * part, 128)
        ops = wt[slot, :, pl.ds(lanes, 128)].astype(F32).T.astype(BF16)
        e_t = (lax.broadcasted_iota(jnp.int32, (PAIR, BOND), 1) // 16
               == lax.broadcasted_iota(jnp.int32, (PAIR, BOND), 0)).astype(F32).astype(BF16)
        e = (lax.broadcasted_iota(jnp.int32, (BOND, PAIR), 0) // 16
             == lax.broadcasted_iota(jnp.int32, (BOND, PAIR), 1)).astype(F32).astype(BF16)
        wide = jnp.dot(ops, e_t, preferred_element_type=F32).astype(BF16)
        for k in range(8):
            full = jnp.dot(e, wide[16 * k:16 * (k + 1), :], preferred_element_type=F32)
            bd[g * 8 + k] = (full * mask[...]).astype(BF16)

    def first_half(h, k0, nk):
        for n in range(8):
            r_stage(h, k0, nk, n)
        wl_stage(h, k0, nk)

    def bd_group(g, carry):
        build_bd(g)
        return carry

    def first_block(s, carry):
        @pl.when(s == 0)
        def _():
            cp_r.wait()
            cp_l.wait()
            lax.fori_loop(0, 2, bd_group, 0)
            l_take(0)

        @pl.when(s == 1)
        def _():
            for i in range(3):
                w_send(i).wait_recv()
            lax.fori_loop(2, 8, bd_group, 0)
            l_take(1)
            r_send(0).wait_recv()
            l_sib().wait_recv()

        @pl.when(s == 2)
        def _():
            l_take(2)
            l_take(3)
            lax.fori_loop(0, 8, l_unpack, 4)
            for i in range(4):
                l_step(i, 0).wait_recv()
            lax.fori_loop(0, 8, l_unpack, 5)
            r_send(1).wait_recv()
            r_send(2).wait_recv()

        def half(h, carry):
            first_half(h, s * BLOCK, BLOCK)
            return carry

        lax.fori_loop(0, 2, half, 0)
        return carry

    def last_group(g, carry):
        @pl.when(g == 6)
        def _():
            for i in range(4):
                l_step(i, 1).wait_recv()
                l_step(i, 2).start()
            lax.fori_loop(0, 8, l_unpack, 6)
            r_send(3).wait_recv()

        @pl.when(g == 7)
        def _():
            for i in range(4):
                l_step(i, 2).wait_recv()
            lax.fori_loop(0, 8, l_unpack, 7)
            r_send(4).wait_recv()

        def half(h, carry):
            first_half(h, g * 8, 8)
            return carry

        lax.fori_loop(0, 2, half, 0)
        return carry

    def gather_r(i, carry):
        @pl.when(i < 4)
        def _():
            relay_all(0, i)

        @pl.when(i >= 1)
        def _():
            later_r(0, i - 1)

        return carry

    def later_r(h, m):
        u_got(h, m, 3).wait_recv()
        for s in range(3):
            u_relayed(h, m, s).wait_recv()
        for n in range(2):
            r_stage(h, 0, TERMS, 2 * m + n)

    def gather_wl(s, carry):
        relay_all(1, s)
        wl_stage(0, s * BLOCK, BLOCK)
        return carry

    def second_r(m, carry):
        later_r(1, m)
        for h in range(2):
            for s in range(4):
                u_own(h, m, s).wait_send()
            for s in range(3):
                u_relay(h, m, s).wait_send()
        return carry

    def second_wl(s, carry):
        wl_stage(1, s * BLOCK, BLOCK)
        return carry

    def x_copy(par, q):
        dest = (t + q) % 4
        return rdma(xs.at[dest], xr.at[par, t], x_ssem.at[q - 1], x_rsem.at[par, q - 1], (y, dest))

    def x_recv(par, q):
        rdma(xs.at[0], xr.at[par, (t + 4 - q) % 4], x_ssem.at[q - 1], x_rsem.at[par, q - 1], sib).wait_recv()

    def put_out(vec, par):
        for d in range(2):
            for i in range(4):
                blk = jnp.concatenate(
                    [vec[4 * i + k, :, pl.ds(128 * d, 128)] for k in range(4)], axis=0).T
                xs[2 * d, i] = blk[:64]
                xs[2 * d + 1, i] = blk[64:]
        xr[par, t] = xs[t]

    def x_start(par):
        for q in range(1, 4):
            x_copy(par, q).start()

    def x_wait_send(par):
        for q in range(1, 4):
            x_copy(par, q).wait_send()

    def merged(par):
        seg = lax.broadcasted_iota(jnp.int32, (64, 128), 1) // 32
        for i in range(4):
            parts = [xr[par, src, i] for src in range(4)]
            for k in range(4):
                res = parts[k]
                for src in range(4):
                    if src != k:
                        res = jnp.where(seg == src, pltpu.roll(parts[src], (32 * (src - k)) % 128, 1), res)
                yield 4 * i + k, res

    def merge_out(j, par):
        for q in range(1, 4):
            x_recv(par, q)

        @pl.when(j > 1)
        def _():
            out_copy(j - 2).wait()

        for p, res in merged(par):
            osb[j % 2, pl.ds(p, 64, stride=16), :] = res
        out_copy(j).start()

    def everywhere(s):
        s = jnp.sum(jnp.sum(s, axis=1, keepdims=True), axis=0, keepdims=True)
        return jnp.broadcast_to(s, (1, 128))

    def fold(v):
        v = v[:, :HALF] + v[:, HALF:]
        return jnp.sum(v.reshape(COLS // 8, 8, 128), axis=0)

    def wide(row):
        return jnp.concatenate([row, row], axis=1)

    def step(j, carry):
        acc[...] = jnp.zeros((PAIR, COLS, BOND), F32)

        @pl.when(j == 0)
        def _():
            lax.fori_loop(0, 3, first_block, 0)
            lax.fori_loop(6, 8, last_group, 0)

        @pl.when(j > 0)
        def _():
            lax.fori_loop(0, 5, gather_r, 0)
            lax.fori_loop(0, 4, gather_wl, 0)
            x_start((j + 1) % 2)
            lax.fori_loop(0, 4, second_r, 0)
            lax.fori_loop(0, 4, second_wl, 0)

        cur = j % 3
        prev = (j + 2) % 3
        nxt = (j + 1) % 3
        par = j % 2

        @pl.when(j == STEPS - 1)
        def _():
            x_wait_send(1 - par)
            put_out(acc, par)
            x_start(par)

        beta_prev = wide(betas[...])
        zero = jnp.zeros((8, 128), F32)

        def pass1(p, s):
            a_s, t_s, v_s = s
            w = acc[p]
            v = vb[cur, p]
            r = w - beta_prev * vb[prev, p]
            vb[nxt, p] = r
            return a_s + fold(w * v), t_s + fold(r * v), v_s + fold(v * v)

        a_s, t_s, v_s = lax.fori_loop(0, PAIR, pass1, (zero, zero, zero))
        a_d, t_d, v_d = everywhere(a_s), everywhere(t_s), everywhere(v_s)
        shift = jnp.where(v_d > 0.0, t_d / jnp.where(v_d > 0.0, v_d, 1.0), 0.0)
        shift_w = wide(shift)

        def pass2(p, s):
            q_s, p_s = s
            v = vb[cur, p]
            r = vb[nxt, p] - shift_w * v
            vb[nxt, p] = r
            return q_s + fold(r * r), p_s + fold(r * v)

        q_s, p_s = lax.fori_loop(0, PAIR, pass2, (zero, zero))
        st[par, me] = jnp.concatenate(
            [a_d, shift, v_d, everywhere(q_s), everywhere(p_s), jnp.zeros((3, 128), F32)], axis=0)

        def st_copy(q):
            d = (me + q) % 8
            return rdma(st.at[par, me], st.at[par, me], st_ssem.at[q - 1], st_rsem.at[q - 1], (d // 4, d % 4))

        for q in range(1, 8):
            st_copy(q).start()

        @pl.when(j > 0)
        def _():
            merge_out(j, 1 - par)

        for q in range(1, 8):
            src = (me + 8 - q) % 8
            rdma(st.at[par, me], st.at[par, src], st_ssem.at[q - 1], st_rsem.at[q - 1], sib).wait_recv()

        alpha = st[par, 0][0:1]
        for d in range(1, 8):
            alpha = alpha + st[par, d][0:1]
        alpha = alpha * (1.0 / ELEMS)
        beta2 = jnp.zeros((1, 128), F32)
        for d in range(8):
            tile = st[par, d]
            gap = alpha - tile[1:2]
            beta2 = beta2 + (tile[3:4] - 2.0 * gap * tile[4:5] + gap * gap * tile[2:3])
        beta = jnp.sqrt(beta2 * (1.0 / ELEMS))
        betas[...] = beta
        coef[0] = alpha
        coef[1] = beta_prev[:, :HALF]
        ab_ref[j] = jnp.concatenate([alpha, beta, jnp.zeros((6, 128), F32)], axis=0)
        gap_w = wide(alpha - shift)
        beta_w = wide(beta)
        rows = pl.ds(pl.multiple_of(32 * me, 32), 32)

        def pass3(m, carry):
            for i in range(4):
                p = 4 * m + i
                v = (vb[nxt, p] - gap_w * vb[cur, p]) / beta_w
                vb[nxt, p] = v
                uT[0, p, rows, :] = v[:, :HALF].astype(BF16)
                uT[1, p, rows, :] = v[:, HALF:].astype(BF16)

            for s in (2, 0, 1, 3):
                u_own(0, m, s).start()
            return carry

        @pl.when(j < STEPS - 1)
        def _():
            lax.fori_loop(0, 4, pass3, 0)
            for m in range(4):
                for s in (2, 0, 1, 3):
                    u_own(1, m, s).start()

        @pl.when((j > 0) & (j < STEPS - 1))
        def _():
            x_wait_send(1 - par)

        @pl.when(j < STEPS - 1)
        def _():
            put_out(vb.at[nxt], par)

        for q in range(1, 8):
            st_copy(q).wait_send()
        return carry

    lax.fori_loop(0, STEPS, step, 0)

    last = (STEPS - 1) % 2
    for q in range(1, 4):
        x_recv(last, q)
    out_copy(STEPS - 2).wait()
    for p, res in merged(last):
        at = pl.ds(p, 64, stride=16)
        res = res - coef[0] * osb[(STEPS - 1) % 2, at, :] - coef[1] * osb[STEPS % 2, at, :]
        osb[STEPS % 2, at, :] = res / betas[...]
    out_copy(STEPS).start()
    x_wait_send(last)
    out_copy(STEPS - 1).wait()
    out_copy(STEPS).wait()

    l_sib().wait_send()
    for i in range(3):
        w_send(i).wait_send()
    for i in range(5):
        r_send(i).wait_send()
    for i in range(4):
        for part in range(2):
            l_dir(i, part).wait_send()
        for kind in range(3):
            l_step(i, kind).wait_send()


def solution(mesh):
    def body_fn(wavefunc, left_loc, two_loc, right_loc):
        bond, phys = wavefunc.shape[0], wavefunc.shape[1]
        wf = wavefunc.reshape(bond, phys, phys, 2, 128).transpose(0, 1, 3, 2, 4).reshape(-1, 128)
        dma = pltpu.SemaphoreType.DMA
        kry, ab = pl.pallas_call(
            lanczos_kernel,
            out_shape=(
                jax.ShapeDtypeStruct((STEPS + 1, 64 * PAIR, 128), F32),
                jax.ShapeDtypeStruct((STEPS, 8, 128), F32),
            ),
            in_specs=[
                pl.BlockSpec(memory_space=pl.ANY),
                pl.BlockSpec(memory_space=pl.ANY),
                pl.BlockSpec(memory_space=pltpu.VMEM),
                pl.BlockSpec(memory_space=pl.ANY),
            ],
            out_specs=(pl.BlockSpec(memory_space=pl.ANY), pl.BlockSpec(memory_space=pltpu.VMEM)),
            scratch_shapes=[
                pltpu.VMEM((8192, 128), F32),
                pltpu.VMEM((TERMS, COLS, BOND), BF16),
                pltpu.VMEM((TERMS, BOND, BOND), BF16),
                pltpu.VMEM((32, 384, 128), BF16),
                pltpu.VMEM((TERMS, BOND, BOND), BF16),
                pltpu.VMEM((4, PAIR, BOND), BF16),
                pltpu.VMEM((BOND, BOND), F32),
                pltpu.VMEM((TERMS, PAIR, COLS, HALF), BF16),
                pltpu.VMEM((PAIR, COLS, BLOCK * HALF), BF16),
                pltpu.VMEM((2, PAIR, BOND, HALF), BF16),
                pltpu.VMEM((PAIR, COLS, BOND), F32),
                pltpu.VMEM((3, PAIR, COLS, BOND), F32),
                pltpu.VMEM((2, 128, 128), F32),
                pltpu.VMEM((2, 8, 8, 128), F32),
                pltpu.VMEM((1, 128), F32),
                pltpu.VMEM((2, 1, 128), F32),
                pltpu.VMEM((4, 4, 64, 128), F32),
                pltpu.VMEM((2, 4, 4, 64, 128), F32),
                pltpu.VMEM((2, 64 * PAIR, 128), F32),
                dma((3,)),
                dma((3,)), dma((3,)),
                dma((5,)), dma((5,)),
                dma((9,)), dma((9,)),
                dma((3, 4)), dma((3, 4)),
                dma((2, 4, 4)), dma((2, 4, 4)),
                dma((2, 4, 3)), dma((2, 4, 3)),
                dma((7,)), dma((7,)),
                dma((3,)), dma((2, 3)),
                dma((2,)),
            ],
            compiler_params=pltpu.CompilerParams(
                collective_id=0, has_side_effects=True, vmem_limit_bytes=66 * 1000 * 1000),
        )(wf, left_loc, two_loc, right_loc)
        krylov = kry.reshape(STEPS + 1, 64, phys, phys, 128)
        return krylov, ab[:, 0, 0], ab[:, 1, 0]

    return jax.shard_map(
        body_fn, mesh=mesh,
        in_specs=(P(), P('terms'), P('terms'), P('terms', 'rows')),
        out_specs=(P(None, 'terms', None, None, 'rows'), P(), P()), check_vma=False)
```

```python
import jax
import jax.numpy as jnp
from jax import lax
from jax.experimental import pallas as pl
from jax.experimental.pallas import tpu as pltpu
from jax.sharding import PartitionSpec as P

STEPS = 6
PAIR = 16
BOND = 256
TERMS = 64
BLOCK = 16
HALF = 128
COLS = 32
ELEMS = float(BOND * BOND * PAIR)
F32 = jnp.float32
BF16 = jnp.bfloat16


def lanczos_kernel(
    wf_hbm, left_hbm, two_ref, right_hbm, kry_hbm, ab_ref,
    wfv, rw, lw, lx, bd, wt, mask, yb, zb, uT, acc, vb, tmp, st, betas, coef, xs, xr, osb,
    loc_sem, w_ssem, w_rsem, r_ssem, r_rsem, l_ssem, l_rsem, lx_ssem, lx_rsem,
    u_ssem, u_rsem, f_ssem, f_rsem, st_ssem, st_rsem, x_ssem, x_rsem, o_sem,
):
    y = lax.axis_index("rows")
    t = lax.axis_index("terms")
    x = t // 2
    c = t % 2
    me = y * 4 + t
    sib = (y, 2 * x + (1 - c))
    xnb = (y, 2 * (1 - x) + c)
    xno = (y, 2 * (1 - x) + (1 - c))
    ynb = (1 - y, t)
    diag = (1 - y, 2 * (1 - x) + c)
    flip = 1 - 2 * c
    near = (4 * y + 2 * (1 - x) + c, 4 * (1 - y) + t, 4 * (1 - y) + 2 * (1 - x) + c)

    def rdma(src, dst, ssem, rsem, dev):
        return pltpu.make_async_remote_copy(
            src_ref=src, dst_ref=dst, send_sem=ssem, recv_sem=rsem,
            device_id=dev, device_id_type=pl.DeviceIdType.MESH)

    cp_wf = pltpu.make_async_copy(wf_hbm, wfv, loc_sem.at[0])
    cp_r = pltpu.make_async_copy(right_hbm.at[:, pl.ds(32 * t, 32), :], rw.at[pl.ds(0, 16)], loc_sem.at[1])
    cp_l = pltpu.make_async_copy(left_hbm, lw.at[pl.ds(0, 16)], loc_sem.at[2])
    cp_wf.start()
    cp_r.start()
    cp_l.start()

    barrier = pltpu.get_barrier_semaphore()
    for q in range(1, 8):
        d = (me + q) % 8
        pl.semaphore_signal(barrier, inc=1, device_id=(d // 4, d % 4), device_id_type=pl.DeviceIdType.MESH)
    pl.semaphore_wait(barrier, 7)

    def l_sib():
        return rdma(left_hbm, lw.at[pl.ds(16, 16)], l_ssem.at[0], l_rsem.at[0], sib)

    def l_dir(i, part):
        rows = pl.ds(0, 256) if part == 0 else pl.ds(128, 128)
        return rdma(left_hbm.at[pl.ds(8 * y + 2 * i, 2), rows, pl.ds(128 * part, 128)],
                    lx.at[pl.ds(2 * i, 2), pl.ds(256 * part, 256 - 128 * part), :],
                    l_ssem.at[1 + 2 * i + part], l_rsem.at[1 + 2 * i + part], xnb)

    def l_step(i, kind):
        src, dst, dev = ((0, 8, sib), (0, 16, ynb), (16, 24, sib))[kind]
        return rdma(lx.at[pl.ds(src + 2 * i, 2)], lx.at[pl.ds(dst + 2 * i, 2)],
                    lx_ssem.at[kind, i], lx_rsem.at[kind, i], dev)

    def l_take(i):
        for part in range(2):
            l_dir(i, part).wait_recv()
        l_step(i, 0).start()
        l_step(i, 1).start()

    def l_unpack(k, s):
        src = 16 * (s - 2) + k
        dst = 16 * s + k
        low = lx[src, pl.ds(128, 128), :]
        lw[dst, pl.ds(0, 128), pl.ds(0, 128)] = lx[src, pl.ds(0, 128), :]
        lw[dst, pl.ds(128, 128), pl.ds(0, 128)] = low
        lw[dst, pl.ds(0, 128), pl.ds(128, 128)] = low.astype(F32).T.astype(BF16)
        lw[dst, pl.ds(128, 128), pl.ds(128, 128)] = lx[src, pl.ds(256, 128), :]
        return s

    def r_send(i):
        first, rows, dst, dev = (
            (0, 2 * x + (1 - c), 16, sib),
            (8 * y, 2 * (1 - x) + c, 32, xnb),
            (8 * y, 2 * (1 - x) + (1 - c), 40, xno),
            (8 * (1 - y), 2 * (1 - x) + c, 48, xnb),
            (8 * (1 - y), 2 * (1 - x) + (1 - c), 56, xno),
        )[i]
        n = 16 if i == 0 else 8
        return rdma(right_hbm.at[pl.ds(first, n), pl.ds(32 * rows, 32), :], rw.at[pl.ds(dst, n)],
                    r_ssem.at[i], r_rsem.at[i], dev)

    for i in range(4):
        for part in range(2):
            l_dir(i, part).start()
    for i in range(5):
        r_send(i).start()
    l_sib().start()

    row16 = lax.broadcasted_iota(jnp.int32, (PAIR, BOND), 0)
    lane16 = lax.broadcasted_iota(jnp.int32, (PAIR, BOND), 1)
    packed = jnp.zeros((PAIR, BOND), F32)
    for k in range(16):
        place = (lane16 == row16 + 16 * k).astype(F32).astype(BF16)
        packed = packed + jnp.dot(two_ref[k], place, preferred_element_type=F32)
    wt[0] = packed.astype(BF16)

    def w_send(i):
        return rdma(wt.at[0], wt.at[1 + i], w_ssem.at[i], w_rsem.at[i], (sib, xnb, xno)[i])

    for i in range(3):
        w_send(i).start()

    rr = lax.broadcasted_iota(jnp.int32, (BOND, BOND), 0) % 16
    cc = lax.broadcasted_iota(jnp.int32, (BOND, BOND), 1) % 16
    mask[...] = (rr == cc).astype(F32)

    cp_wf.wait()

    def sumsq(i, s):
        blk = wfv[pl.ds(pl.multiple_of(i * 256, 256), 256), :]
        return s + jnp.sum((blk * blk).reshape(32, 8, 128), axis=0)

    total = lax.fori_loop(0, 32, sumsq, jnp.zeros((8, 128), F32))
    total = jnp.sum(jnp.sum(total, axis=1, keepdims=True), axis=0, keepdims=True)
    scale = jnp.broadcast_to(jnp.sqrt(total * (1.0 / ELEMS)), (1, 128))

    wfo = wfv.at[pl.ds(pl.multiple_of(2048 * t, 2048), 2048), :]
    own = pl.ds(pl.multiple_of(32 * t, 32), 32)
    for p in range(PAIR):
        for h in range(2):
            for bt in range(2):
                first = 4096 * h + (p // 4) * 8 + bt * 4 + p % 4
                blk = (wfv[pl.ds(first, 128, stride=32), :] / scale).T
                tmp[bt] = blk
                uT[h, p, pl.ds(128 * bt, 128), :] = blk.astype(BF16)
            vb[0, p, :, pl.ds(128 * h, 128)] = tmp[y, own, :]
        first = (p // 4) * 8 + p % 4
        lo = wfo[pl.ds(first, 64, stride=32), :]
        hi = wfo[pl.ds(first + 4, 64, stride=32), :]
        osb[0, pl.ds(p, 64, stride=16), :] = jnp.where(y == 0, lo, hi) / scale
    vb[2] = jnp.zeros((PAIR, COLS, BOND), F32)
    betas[...] = jnp.zeros((1, 128), F32)

    def out_copy(j):
        return pltpu.make_async_copy(osb.at[j % 2], kry_hbm.at[j], o_sem.at[j % 2])

    out_copy(0).start()

    def u_part(h, m, dev):
        return uT.at[h, pl.ds(4 * m, 4), pl.ds(pl.multiple_of(32 * dev, 32), 32), :]

    def u_own(h, m, s):
        part = u_part(h, m, me)
        return rdma(part, part, u_ssem.at[h, m, s], u_rsem.at[h, m, s], (xnb, ynb, diag, sib)[s])

    def u_got(h, m, s):
        part = u_part(h, m, (near + (me + flip,))[s])
        return rdma(part, part, u_ssem.at[h, m, s], u_rsem.at[h, m, s], (xnb, ynb, diag, sib)[s])

    def u_relay(h, m, s):
        part = u_part(h, m, near[s])
        return rdma(part, part, f_ssem.at[h, m, s], f_rsem.at[h, m, s], sib)

    def u_relayed(h, m, s):
        part = u_part(h, m, near[s] + flip)
        return rdma(part, part, f_ssem.at[h, m, s], f_rsem.at[h, m, s], sib)

    def relay_all(h, m):
        for s in range(3):
            u_got(h, m, s).wait_recv()
            u_relay(h, m, s).start()

    def r_stage(h, k0, nk, n):
        lhs = rw[pl.ds(k0, nk)].reshape(nk * COLS, BOND)
        rhs = jnp.concatenate([uT[h, 2 * n], uT[h, 2 * n + 1]], axis=1)
        res = jnp.dot(lhs, rhs, preferred_element_type=F32).astype(BF16)
        yb[pl.ds(k0, nk), 2 * n] = res[:, :HALF].reshape(nk, COLS, HALF)
        yb[pl.ds(k0, nk), 2 * n + 1] = res[:, HALF:].reshape(nk, COLS, HALF)

    def wl_stage(h, s, buf=0):
        k0 = s * BLOCK
        for k in range(BLOCK):
            rhs = jnp.concatenate(
                [yb[k0 + k, :, pl.ds(16 * i, 16), :].reshape(BOND, HALF) for i in range(2)], axis=1)
            res = jnp.dot(bd[k0 + k], rhs, preferred_element_type=F32).astype(BF16)
            for i in range(2):
                zb[buf, :, pl.ds(16 * i, 16), pl.ds(HALF * k, HALF)] = (
                    res[:, HALF * i:HALF * (i + 1)].reshape(PAIR, 16, HALF))
        lhs = zb[buf].reshape(PAIR * COLS, BLOCK * HALF)
        rhs = lw[pl.ds(k0, BLOCK), pl.ds(pl.multiple_of(HALF * h, HALF), HALF), :].reshape(BLOCK * HALF, BOND)
        res = jnp.dot(lhs, rhs, preferred_element_type=F32)
        acc[...] = acc[...] + res.reshape(PAIR, COLS, BOND)

    def build_bd(g):
        slot = (g // 4) * 2 + (1 - g // 4) * (g // 2) + (g // 4) * (g % 2)
        part = (1 - g // 4) * (g % 2) + (g // 4) * ((y + (g - 4 * (g // 4)) // 2) % 2)
        lanes = pl.multiple_of(128 * part, 128)
        ops = wt[slot, :, pl.ds(lanes, 128)].astype(F32).T.astype(BF16)
        e_t = (lax.broadcasted_iota(jnp.int32, (PAIR, BOND), 1) // 16
               == lax.broadcasted_iota(jnp.int32, (PAIR, BOND), 0)).astype(F32).astype(BF16)
        e = (lax.broadcasted_iota(jnp.int32, (BOND, PAIR), 0) // 16
             == lax.broadcasted_iota(jnp.int32, (BOND, PAIR), 1)).astype(F32).astype(BF16)
        wide = jnp.dot(ops, e_t, preferred_element_type=F32).astype(BF16)
        for k in range(8):
            full = jnp.dot(e, wide[16 * k:16 * (k + 1), :], preferred_element_type=F32)
            bd[g * 8 + k] = (full * mask[...]).astype(BF16)

    def bd_group(i, s):
        build_bd(2 * s + i)
        return s

    def first_block(s, carry):
        @pl.when(s == 0)
        def _():
            cp_r.wait()
            cp_l.wait()

        @pl.when(s == 1)
        def _():
            w_send(0).wait_recv()
            r_send(0).wait_recv()
            l_sib().wait_recv()

        @pl.when(s == 2)
        def _():
            w_send(1).wait_recv()
            w_send(2).wait_recv()

        lax.fori_loop(0, 2, bd_group, s)

        @pl.when(s < 2)
        def _():
            for i in range(2):
                @pl.when(s == i)
                def _(i=i):
                    l_take(i)

        @pl.when(s == 2)
        def _():
            l_take(2)
            l_take(3)
            for i in range(4):
                l_step(i, 0).wait_recv()
            lax.fori_loop(0, 16, l_unpack, s)
            r_send(1).wait_recv()
            r_send(2).wait_recv()

        @pl.when(s == 3)
        def _():
            for i in range(4):
                l_step(i, 1).wait_recv()
                l_step(i, 2).start()
            for i in range(4):
                l_step(i, 2).wait_recv()
            lax.fori_loop(0, 16, l_unpack, s)
            r_send(3).wait_recv()
            r_send(4).wait_recv()

        def half(h, carry):
            for n in range(8):
                r_stage(h, s * BLOCK, BLOCK, n)
            wl_stage(h, s)
            return carry

        lax.fori_loop(0, 2, half, 0)
        return carry

    def gather_r(i, carry):
        @pl.when(i < 4)
        def _():
            relay_all(0, i)

        @pl.when(i >= 1)
        def _():
            later_r(0, i - 1)

        return carry

    def later_r(h, m):
        u_got(h, m, 3).wait_recv()
        for s in range(3):
            u_relayed(h, m, s).wait_recv()
        for n in range(2):
            r_stage(h, 0, TERMS, 2 * m + n)

    def gather_wl(s, carry):
        relay_all(1, s)
        wl_stage(0, s)
        return carry

    def second_r(m, carry):
        later_r(1, m)
        for h in range(2):
            for s in range(4):
                u_own(h, m, s).wait_send()
            for s in range(3):
                u_relay(h, m, s).wait_send()
        return carry

    def x_copy(par, q):
        dest = (t + q) % 4
        return rdma(xs.at[dest], xr.at[par, t], x_ssem.at[q - 1], x_rsem.at[par, q - 1], (y, dest))

    def x_recv(par, q):
        rdma(xs.at[0], xr.at[par, (t + 4 - q) % 4], x_ssem.at[q - 1], x_rsem.at[par, q - 1], sib).wait_recv()

    def put_out(vec, par):
        for d in range(2):
            for i in range(4):
                blk = jnp.concatenate(
                    [vec[4 * i + k, :, pl.ds(128 * d, 128)] for k in range(4)], axis=0).T
                xs[2 * d, i] = blk[:64]
                xs[2 * d + 1, i] = blk[64:]
        xr[par, t] = xs[t]

    def x_start(par):
        for q in range(1, 4):
            x_copy(par, q).start()

    def x_wait_send(par):
        for q in range(1, 4):
            x_copy(par, q).wait_send()

    def merged(par):
        seg = lax.broadcasted_iota(jnp.int32, (64, 128), 1) // 32
        for i in range(4):
            parts = [xr[par, src, i] for src in range(4)]
            for k in range(4):
                res = parts[k]
                for src in range(4):
                    if src != k:
                        res = jnp.where(seg == src, pltpu.roll(parts[src], (32 * (src - k)) % 128, 1), res)
                yield 4 * i + k, res

    def merge_out(j, par):
        for q in range(1, 4):
            x_recv(par, q)

        @pl.when(j > 1)
        def _():
            out_copy(j - 2).wait()

        for p, res in merged(par):
            osb[j % 2, pl.ds(p, 64, stride=16), :] = res
        out_copy(j).start()

    def everywhere(s):
        s = jnp.sum(jnp.sum(s, axis=1, keepdims=True), axis=0, keepdims=True)
        return jnp.broadcast_to(s, (1, 128))

    def fold(v):
        v = v[:, :HALF] + v[:, HALF:]
        return jnp.sum(v.reshape(COLS // 8, 8, 128), axis=0)

    def wide(row):
        return jnp.concatenate([row, row], axis=1)

    def step(j, carry):
        acc[...] = jnp.zeros((PAIR, COLS, BOND), F32)

        @pl.when(j == 0)
        def _():
            lax.fori_loop(0, 4, first_block, 0)

        @pl.when(j > 0)
        def _():
            lax.fori_loop(0, 5, gather_r, 0)
            lax.fori_loop(0, 4, gather_wl, 0)
            x_start((j + 1) % 2)
            lax.fori_loop(0, 4, second_r, 0)
            for s in range(4):
                wl_stage(1, s, s % 2)

        cur = j % 3
        prev = (j + 2) % 3
        nxt = (j + 1) % 3
        par = j % 2

        @pl.when(j == STEPS - 1)
        def _():
            x_wait_send(1 - par)
            put_out(acc, par)
            x_start(par)

        beta_prev = wide(betas[...])
        zero = jnp.zeros((8, 128), F32)

        def pass1(p, s):
            a_s, t_s, v_s = s
            w = acc[p]
            v = vb[cur, p]
            r = w - beta_prev * vb[prev, p]
            vb[nxt, p] = r
            return a_s + fold(w * v), t_s + fold(r * v), v_s + fold(v * v)

        a_s, t_s, v_s = lax.fori_loop(0, PAIR, pass1, (zero, zero, zero))
        a_d, t_d, v_d = everywhere(a_s), everywhere(t_s), everywhere(v_s)
        shift = jnp.where(v_d > 0.0, t_d / jnp.where(v_d > 0.0, v_d, 1.0), 0.0)
        shift_w = wide(shift)

        def pass2(p, s):
            q_s, p_s = s
            v = vb[cur, p]
            r = vb[nxt, p] - shift_w * v
            vb[nxt, p] = r
            return q_s + fold(r * r), p_s + fold(r * v)

        q_s, p_s = lax.fori_loop(0, PAIR, pass2, (zero, zero))
        st[par, me] = jnp.concatenate(
            [a_d, shift, v_d, everywhere(q_s), everywhere(p_s), jnp.zeros((3, 128), F32)], axis=0)

        def st_copy(q):
            d = (me + q) % 8
            return rdma(st.at[par, me], st.at[par, me], st_ssem.at[q - 1], st_rsem.at[q - 1], (d // 4, d % 4))

        for q in range(1, 8):
            st_copy(q).start()

        @pl.when(j > 0)
        def _():
            merge_out(j, 1 - par)

        for q in range(1, 8):
            src = (me + 8 - q) % 8
            rdma(st.at[par, me], st.at[par, src], st_ssem.at[q - 1], st_rsem.at[q - 1], sib).wait_recv()

        alpha = st[par, 0][0:1]
        for d in range(1, 8):
            alpha = alpha + st[par, d][0:1]
        alpha = alpha * (1.0 / ELEMS)
        beta2 = jnp.zeros((1, 128), F32)
        for d in range(8):
            tile = st[par, d]
            gap = alpha - tile[1:2]
            beta2 = beta2 + (tile[3:4] - 2.0 * gap * tile[4:5] + gap * gap * tile[2:3])
        beta = jnp.sqrt(beta2 * (1.0 / ELEMS))
        betas[...] = beta
        coef[0] = alpha
        coef[1] = beta_prev[:, :HALF]
        ab_ref[j] = jnp.concatenate([alpha, beta, jnp.zeros((6, 128), F32)], axis=0)
        gap_w = wide(alpha - shift)
        beta_w = wide(beta)
        rows = pl.ds(pl.multiple_of(32 * me, 32), 32)

        def pass3(m, carry):
            for i in range(4):
                p = 4 * m + i
                v = (vb[nxt, p] - gap_w * vb[cur, p]) / beta_w
                vb[nxt, p] = v
                uT[0, p, rows, :] = v[:, :HALF].astype(BF16)
                uT[1, p, rows, :] = v[:, HALF:].astype(BF16)

            for s in (2, 0, 1, 3):
                u_own(0, m, s).start()
            return carry

        @pl.when(j < STEPS - 1)
        def _():
            lax.fori_loop(0, 4, pass3, 0)
            for m in range(4):
                for s in (2, 0, 1, 3):
                    u_own(1, m, s).start()

        @pl.when((j > 0) & (j < STEPS - 1))
        def _():
            x_wait_send(1 - par)

        @pl.when(j < STEPS - 1)
        def _():
            put_out(vb.at[nxt], par)

        for q in range(1, 8):
            st_copy(q).wait_send()
        return carry

    lax.fori_loop(0, STEPS, step, 0)

    last = (STEPS - 1) % 2
    for q in range(1, 4):
        x_recv(last, q)
    out_copy(STEPS - 2).wait()
    for p, res in merged(last):
        at = pl.ds(p, 64, stride=16)
        res = res - coef[0] * osb[(STEPS - 1) % 2, at, :] - coef[1] * osb[STEPS % 2, at, :]
        osb[STEPS % 2, at, :] = res / betas[...]
    out_copy(STEPS).start()
    x_wait_send(last)
    out_copy(STEPS - 1).wait()
    out_copy(STEPS).wait()

    l_sib().wait_send()
    for i in range(3):
        w_send(i).wait_send()
    for i in range(5):
        r_send(i).wait_send()
    for i in range(4):
        for part in range(2):
            l_dir(i, part).wait_send()
        for kind in range(3):
            l_step(i, kind).wait_send()


def solution(mesh):
    def body_fn(wavefunc, left_loc, two_loc, right_loc):
        bond, phys = wavefunc.shape[0], wavefunc.shape[1]
        wf = wavefunc.reshape(bond, phys, phys, 2, 128).transpose(0, 1, 3, 2, 4).reshape(-1, 128)
        dma = pltpu.SemaphoreType.DMA
        kry, ab = pl.pallas_call(
            lanczos_kernel,
            out_shape=(
                jax.ShapeDtypeStruct((STEPS + 1, 64 * PAIR, 128), F32),
                jax.ShapeDtypeStruct((STEPS, 8, 128), F32),
            ),
            in_specs=[
                pl.BlockSpec(memory_space=pl.ANY),
                pl.BlockSpec(memory_space=pl.ANY),
                pl.BlockSpec(memory_space=pltpu.VMEM),
                pl.BlockSpec(memory_space=pl.ANY),
            ],
            out_specs=(pl.BlockSpec(memory_space=pl.ANY), pl.BlockSpec(memory_space=pltpu.VMEM)),
            scratch_shapes=[
                pltpu.VMEM((8192, 128), F32),
                pltpu.VMEM((TERMS, COLS, BOND), BF16),
                pltpu.VMEM((TERMS, BOND, BOND), BF16),
                pltpu.VMEM((32, 384, 128), BF16),
                pltpu.VMEM((TERMS, BOND, BOND), BF16),
                pltpu.VMEM((4, PAIR, BOND), BF16),
                pltpu.VMEM((BOND, BOND), F32),
                pltpu.VMEM((TERMS, PAIR, COLS, HALF), BF16),
                pltpu.VMEM((2, PAIR, COLS, BLOCK * HALF), BF16),
                pltpu.VMEM((2, PAIR, BOND, HALF), BF16),
                pltpu.VMEM((PAIR, COLS, BOND), F32),
                pltpu.VMEM((3, PAIR, COLS, BOND), F32),
                pltpu.VMEM((2, 128, 128), F32),
                pltpu.VMEM((2, 8, 8, 128), F32),
                pltpu.VMEM((1, 128), F32),
                pltpu.VMEM((2, 1, 128), F32),
                pltpu.VMEM((4, 4, 64, 128), F32),
                pltpu.VMEM((2, 4, 4, 64, 128), F32),
                pltpu.VMEM((2, 64 * PAIR, 128), F32),
                dma((3,)),
                dma((3,)), dma((3,)),
                dma((5,)), dma((5,)),
                dma((9,)), dma((9,)),
                dma((3, 4)), dma((3, 4)),
                dma((2, 4, 4)), dma((2, 4, 4)),
                dma((2, 4, 3)), dma((2, 4, 3)),
                dma((7,)), dma((7,)),
                dma((3,)), dma((2, 3)),
                dma((2,)),
            ],
            compiler_params=pltpu.CompilerParams(
                collective_id=0, has_side_effects=True, vmem_limit_bytes=66 * 1000 * 1000),
        )(wf, left_loc, two_loc, right_loc)
        krylov = kry.reshape(STEPS + 1, 64, phys, phys, 128)
        return krylov, ab[:, 0, 0], ab[:, 1, 0]

    return jax.shard_map(
        body_fn, mesh=mesh,
        in_specs=(P(), P('terms'), P('terms'), P('terms', 'rows')),
        out_specs=(P(None, 'terms', None, None, 'rows'), P(), P()), check_vma=False)
```

```python
import jax
import jax.numpy as jnp
from jax import lax
from jax.experimental import pallas as pl
from jax.experimental.pallas import tpu as pltpu
from jax.sharding import PartitionSpec as P

STEPS = 6
PAIR = 16
BOND = 256
TERMS = 64
BLOCK = 16
HALF = 128
COLS = 32
ELEMS = float(BOND * BOND * PAIR)
F32 = jnp.float32
BF16 = jnp.bfloat16


def lanczos_kernel(
    wf_hbm, left_hbm, two_ref, right_hbm, kry_hbm, ab_ref, one_ref,
    wfv, rw, lw, lx, bd, wt, mask, yb, zb, uT, acc, vb, tmp, st, betas, coef, xs, xr, osb,
    loc_sem, w_ssem, w_rsem, r_ssem, r_rsem, l_ssem, l_rsem, lx_ssem, lx_rsem,
    u_ssem, u_rsem, f_ssem, f_rsem, st_ssem, st_rsem, x_ssem, x_rsem, o_sem,
):
    y = lax.axis_index("rows")
    t = lax.axis_index("terms")
    x = t // 2
    c = t % 2
    me = y * 4 + t
    sib = (y, 2 * x + (1 - c))
    xnb = (y, 2 * (1 - x) + c)
    xno = (y, 2 * (1 - x) + (1 - c))
    ynb = (1 - y, t)
    diag = (1 - y, 2 * (1 - x) + c)
    flip = 1 - 2 * c
    near = (4 * y + 2 * (1 - x) + c, 4 * (1 - y) + t, 4 * (1 - y) + 2 * (1 - x) + c)

    def rdma(src, dst, ssem, rsem, dev):
        return pltpu.make_async_remote_copy(
            src_ref=src, dst_ref=dst, send_sem=ssem, recv_sem=rsem,
            device_id=dev, device_id_type=pl.DeviceIdType.MESH)

    cp_wf = pltpu.make_async_copy(wf_hbm, wfv, loc_sem.at[0])
    cp_r = pltpu.make_async_copy(right_hbm.at[:, pl.ds(32 * t, 32), :], rw.at[pl.ds(0, 16)], loc_sem.at[1])
    cp_l = pltpu.make_async_copy(left_hbm, lw.at[pl.ds(0, 16)], loc_sem.at[2])
    cp_wf.start()
    cp_r.start()
    cp_l.start()

    barrier = pltpu.get_barrier_semaphore()
    for q in range(1, 8):
        d = (me + q) % 8
        pl.semaphore_signal(barrier, inc=1, device_id=(d // 4, d % 4), device_id_type=pl.DeviceIdType.MESH)
    pl.semaphore_wait(barrier, 7)

    def l_sib():
        return rdma(left_hbm, lw.at[pl.ds(16, 16)], l_ssem.at[0], l_rsem.at[0], sib)

    def l_dir(i, part):
        rows = pl.ds(0, 256) if part == 0 else pl.ds(128, 128)
        return rdma(left_hbm.at[pl.ds(8 * y + 2 * i, 2), rows, pl.ds(128 * part, 128)],
                    lx.at[pl.ds(2 * i, 2), pl.ds(256 * part, 256 - 128 * part), :],
                    l_ssem.at[1 + 2 * i + part], l_rsem.at[1 + 2 * i + part], xnb)

    def l_step(i, kind):
        src, dst, dev = ((0, 8, sib), (0, 16, ynb), (16, 24, sib))[kind]
        return rdma(lx.at[pl.ds(src + 2 * i, 2)], lx.at[pl.ds(dst + 2 * i, 2)],
                    lx_ssem.at[kind, i], lx_rsem.at[kind, i], dev)

    def l_take(i):
        for part in range(2):
            l_dir(i, part).wait_recv()
        l_step(i, 0).start()
        l_step(i, 1).start()

    def l_unpack(k, s):
        src = 16 * (s - 2) + k
        dst = 16 * s + k
        low = lx[src, pl.ds(128, 128), :]
        lw[dst, pl.ds(0, 128), pl.ds(0, 128)] = lx[src, pl.ds(0, 128), :]
        lw[dst, pl.ds(128, 128), pl.ds(0, 128)] = low
        lw[dst, pl.ds(0, 128), pl.ds(128, 128)] = low.astype(F32).T.astype(BF16)
        lw[dst, pl.ds(128, 128), pl.ds(128, 128)] = lx[src, pl.ds(256, 128), :]
        return s

    def r_send(i):
        first, rows, dst, dev = (
            (0, 2 * x + (1 - c), 16, sib),
            (8 * y, 2 * (1 - x) + c, 32, xnb),
            (8 * y, 2 * (1 - x) + (1 - c), 40, xno),
            (8 * (1 - y), 2 * (1 - x) + c, 48, xnb),
            (8 * (1 - y), 2 * (1 - x) + (1 - c), 56, xno),
        )[i]
        n = 16 if i == 0 else 8
        return rdma(right_hbm.at[pl.ds(first, n), pl.ds(32 * rows, 32), :], rw.at[pl.ds(dst, n)],
                    r_ssem.at[i], r_rsem.at[i], dev)

    for i in range(4):
        for part in range(2):
            l_dir(i, part).start()
    for i in range(5):
        r_send(i).start()
    l_sib().start()

    row16 = lax.broadcasted_iota(jnp.int32, (PAIR, BOND), 0)
    lane16 = lax.broadcasted_iota(jnp.int32, (PAIR, BOND), 1)
    packed = jnp.zeros((PAIR, BOND), F32)
    for k in range(16):
        place = (lane16 == row16 + 16 * k).astype(F32).astype(BF16)
        packed = packed + jnp.dot(two_ref[k], place, preferred_element_type=F32)
    wt[0] = packed.astype(BF16)

    def w_send(i):
        return rdma(wt.at[0], wt.at[1 + i], w_ssem.at[i], w_rsem.at[i], (sib, xnb, xno)[i])

    for i in range(3):
        w_send(i).start()

    rr = lax.broadcasted_iota(jnp.int32, (BOND, BOND), 0) % 16
    cc = lax.broadcasted_iota(jnp.int32, (BOND, BOND), 1) % 16
    mask[...] = (rr == cc).astype(F32)

    cp_wf.wait()

    def sumsq(i, s):
        blk = wfv[pl.ds(pl.multiple_of(i * 256, 256), 256), :]
        return s + jnp.sum((blk * blk).reshape(32, 8, 128), axis=0)

    total = lax.fori_loop(0, 32, sumsq, jnp.zeros((8, 128), F32))
    total = jnp.sum(jnp.sum(total, axis=1, keepdims=True), axis=0, keepdims=True)
    scale = jnp.broadcast_to(jnp.sqrt(total * (1.0 / ELEMS)), (1, 128))

    wfo = wfv.at[pl.ds(pl.multiple_of(2048 * t, 2048), 2048), :]
    own = pl.ds(pl.multiple_of(32 * t, 32), 32)
    for p in range(PAIR):
        for h in range(2):
            for bt in range(2):
                first = 4096 * h + (p // 4) * 8 + bt * 4 + p % 4
                blk = (wfv[pl.ds(first, 128, stride=32), :] / scale).T
                tmp[bt] = blk
                uT[h, p, pl.ds(128 * bt, 128), :] = blk.astype(BF16)
            vb[0, p, :, pl.ds(128 * h, 128)] = tmp[y, own, :]
        first = (p // 4) * 8 + p % 4
        lo = wfo[pl.ds(first, 64, stride=32), :]
        hi = wfo[pl.ds(first + 4, 64, stride=32), :]
        osb[0, pl.ds(p, 64, stride=16), :] = jnp.where(y == 0, lo, hi) / scale
    vb[2] = jnp.zeros((PAIR, COLS, BOND), F32)
    betas[...] = jnp.zeros((1, 128), F32)
    one_ref[...] = jnp.ones((1, 128), F32)

    def out_copy(j):
        return pltpu.make_async_copy(osb.at[j % 2], kry_hbm.at[j], o_sem.at[j % 2])

    out_copy(0).start()

    def u_part(h, m, dev):
        n = 2 + 2 * h
        return uT.at[h, pl.ds(n * m, n), pl.ds(pl.multiple_of(32 * dev, 32), 32), :]

    def u_own(h, m, s):
        part = u_part(h, m, me)
        return rdma(part, part, u_ssem.at[8 * h + m, s], u_rsem.at[8 * h + m, s], (xnb, ynb, diag, sib)[s])

    def u_got(h, m, s):
        part = u_part(h, m, (near + (me + flip,))[s])
        return rdma(part, part, u_ssem.at[8 * h + m, s], u_rsem.at[8 * h + m, s], (xnb, ynb, diag, sib)[s])

    def u_relay(h, m, s):
        part = u_part(h, m, near[s])
        return rdma(part, part, f_ssem.at[8 * h + m, s], f_rsem.at[8 * h + m, s], sib)

    def u_relayed(h, m, s):
        part = u_part(h, m, near[s] + flip)
        return rdma(part, part, f_ssem.at[8 * h + m, s], f_rsem.at[8 * h + m, s], sib)

    def relay_all(h, m):
        for s in range(3):
            u_got(h, m, s).wait_recv()
            u_relay(h, m, s).start()

    def r_stage(h, k0, nk, n):
        lhs = rw[pl.ds(k0, nk)].reshape(nk * COLS, BOND)
        rhs = jnp.concatenate([uT[h, 2 * n], uT[h, 2 * n + 1]], axis=1)
        res = jnp.dot(lhs, rhs, preferred_element_type=F32).astype(BF16)
        yb[pl.ds(k0, nk), 2 * n] = res[:, :HALF].reshape(nk, COLS, HALF)
        yb[pl.ds(k0, nk), 2 * n + 1] = res[:, HALF:].reshape(nk, COLS, HALF)

    def wl_stage(h, s, buf=0):
        k0 = s * BLOCK
        for k in range(BLOCK):
            rhs = jnp.concatenate(
                [yb[k0 + k, :, pl.ds(16 * i, 16), :].reshape(BOND, HALF) for i in range(2)], axis=1)
            res = jnp.dot(bd[k0 + k], rhs, preferred_element_type=F32).astype(BF16)
            for i in range(2):
                zb[buf, :, pl.ds(16 * i, 16), pl.ds(HALF * k, HALF)] = (
                    res[:, HALF * i:HALF * (i + 1)].reshape(PAIR, 16, HALF))
        lhs = zb[buf].reshape(PAIR * COLS, BLOCK * HALF)
        rhs = lw[pl.ds(k0, BLOCK), pl.ds(pl.multiple_of(HALF * h, HALF), HALF), :].reshape(BLOCK * HALF, BOND)
        res = jnp.dot(lhs, rhs, preferred_element_type=F32)
        acc[...] = acc[...] + res.reshape(PAIR, COLS, BOND)

    def build_bd(g):
        slot = (g // 4) * 2 + (1 - g // 4) * (g // 2) + (g // 4) * (g % 2)
        part = (1 - g // 4) * (g % 2) + (g // 4) * ((y + (g - 4 * (g // 4)) // 2) % 2)
        lanes = pl.multiple_of(128 * part, 128)
        ops = wt[slot, :, pl.ds(lanes, 128)].astype(F32).T.astype(BF16)
        e_t = (lax.broadcasted_iota(jnp.int32, (PAIR, BOND), 1) // 16
               == lax.broadcasted_iota(jnp.int32, (PAIR, BOND), 0)).astype(F32).astype(BF16)
        e = (lax.broadcasted_iota(jnp.int32, (BOND, PAIR), 0) // 16
             == lax.broadcasted_iota(jnp.int32, (BOND, PAIR), 1)).astype(F32).astype(BF16)
        wide = jnp.dot(ops, e_t, preferred_element_type=F32).astype(BF16)
        for k in range(8):
            full = jnp.dot(e, wide[16 * k:16 * (k + 1), :], preferred_element_type=F32)
            bd[g * 8 + k] = (full * mask[...]).astype(BF16)

    def bd_group(i, s):
        build_bd(2 * s + i)
        return s

    def first_block(s, carry):
        @pl.when(s == 0)
        def _():
            cp_r.wait()
            cp_l.wait()

        @pl.when(s == 1)
        def _():
            w_send(0).wait_recv()
            r_send(0).wait_recv()
            l_sib().wait_recv()

        @pl.when(s == 2)
        def _():
            w_send(1).wait_recv()
            w_send(2).wait_recv()

        lax.fori_loop(0, 2, bd_group, s)

        @pl.when(s < 2)
        def _():
            for i in range(2):
                @pl.when(s == i)
                def _(i=i):
                    l_take(i)

        @pl.when(s == 2)
        def _():
            l_take(2)
            l_take(3)
            for i in range(4):
                l_step(i, 0).wait_recv()
            lax.fori_loop(0, 16, l_unpack, s)
            r_send(1).wait_recv()
            r_send(2).wait_recv()

        @pl.when(s == 3)
        def _():
            for i in range(4):
                l_step(i, 1).wait_recv()
                l_step(i, 2).start()
            for i in range(4):
                l_step(i, 2).wait_recv()
            lax.fori_loop(0, 16, l_unpack, s)
            r_send(3).wait_recv()
            r_send(4).wait_recv()

        def half(h, carry):
            for n in range(8):
                r_stage(h, s * BLOCK, BLOCK, n)
            wl_stage(h, s)
            return carry

        lax.fori_loop(0, 2, half, 0)
        return carry

    def gather_r(i, carry):
        @pl.when(i < 8)
        def _():
            relay_all(0, i)

        @pl.when(i >= 1)
        def _():
            later_r(0, i - 1)

        return carry

    def later_r(h, m):
        u_got(h, m, 3).wait_recv()
        for s in range(3):
            u_relayed(h, m, s).wait_recv()
        for n in range(1 + h):
            r_stage(h, 0, TERMS, (1 + h) * m + n)

    def gather_wl(s, carry):
        relay_all(1, s)
        wl_stage(0, s)
        return carry

    def second_r(m, carry):
        later_r(1, m)
        for h, k in ((0, 2 * m), (0, 2 * m + 1), (1, m)):
            for s in range(4):
                u_own(h, k, s).wait_send()
            for s in range(3):
                u_relay(h, k, s).wait_send()
        return carry

    def x_copy(par, q):
        dest = (t + q) % 4
        return rdma(xs.at[dest], xr.at[par, t], x_ssem.at[q - 1], x_rsem.at[par, q - 1], (y, dest))

    def x_recv(par, q):
        rdma(xs.at[0], xr.at[par, (t + 4 - q) % 4], x_ssem.at[q - 1], x_rsem.at[par, q - 1], sib).wait_recv()

    def put_out(vec, par):
        for d in range(2):
            for i in range(4):
                blk = jnp.concatenate(
                    [vec[4 * i + k, :, pl.ds(128 * d, 128)] for k in range(4)], axis=0).T
                xs[2 * d, i] = blk[:64]
                xs[2 * d + 1, i] = blk[64:]
        xr[par, t] = xs[t]

    def x_start(par):
        for q in range(1, 4):
            x_copy(par, q).start()

    def x_wait_send(par):
        for q in range(1, 4):
            x_copy(par, q).wait_send()

    def merged(par):
        seg = lax.broadcasted_iota(jnp.int32, (64, 128), 1) // 32
        for i in range(4):
            parts = [xr[par, src, i] for src in range(4)]
            for k in range(4):
                res = parts[k]
                for src in range(4):
                    if src != k:
                        res = jnp.where(seg == src, pltpu.roll(parts[src], (32 * (src - k)) % 128, 1), res)
                yield 4 * i + k, res

    def merge_out(j, par):
        for q in range(1, 4):
            x_recv(par, q)

        @pl.when(j > 1)
        def _():
            out_copy(j - 2).wait()

        for p, res in merged(par):
            osb[j % 2, pl.ds(p, 64, stride=16), :] = res
        out_copy(j).start()

    def everywhere(s):
        s = jnp.sum(jnp.sum(s, axis=1, keepdims=True), axis=0, keepdims=True)
        return jnp.broadcast_to(s, (1, 128))

    def fold(v):
        v = v[:, :HALF] + v[:, HALF:]
        return jnp.sum(v.reshape(COLS // 8, 8, 128), axis=0)

    def wide(row):
        return jnp.concatenate([row, row], axis=1)

    def step(j, carry):
        acc[...] = jnp.zeros((PAIR, COLS, BOND), F32)

        @pl.when(j == 0)
        def _():
            lax.fori_loop(0, 4, first_block, 0)

        @pl.when(j > 0)
        def _():
            lax.fori_loop(0, 9, gather_r, 0)
            lax.fori_loop(0, 4, gather_wl, 0)
            x_start((j + 1) % 2)
            lax.fori_loop(0, 4, second_r, 0)
            for s in range(4):
                wl_stage(1, s, s % 2)

        cur = j % 3
        prev = (j + 2) % 3
        nxt = (j + 1) % 3
        par = j % 2

        @pl.when(j == STEPS - 1)
        def _():
            x_wait_send(1 - par)
            put_out(acc, par)
            x_start(par)

        beta_prev = wide(betas[...])
        zero = jnp.zeros((8, 128), F32)

        def pass1(p, s):
            a_s, t_s, v_s = s
            w = acc[p]
            v = vb[cur, p]
            r = w - beta_prev * vb[prev, p]
            vb[nxt, p] = r
            return a_s + fold(w * v), t_s + fold(r * v), v_s + fold(v * v)

        a_s, t_s, v_s = lax.fori_loop(0, PAIR, pass1, (zero, zero, zero))
        a_d, t_d, v_d = everywhere(a_s), everywhere(t_s), everywhere(v_s)
        shift = jnp.where(v_d > 0.0, t_d / jnp.where(v_d > 0.0, v_d, 1.0), 0.0)
        shift_w = wide(shift)

        def pass2(p, s):
            q_s, p_s = s
            v = vb[cur, p]
            r = vb[nxt, p] - shift_w * v
            vb[nxt, p] = r
            return q_s + fold(r * r), p_s + fold(r * v)

        q_s, p_s = lax.fori_loop(0, PAIR, pass2, (zero, zero))
        st[par, me] = jnp.concatenate(
            [a_d, shift, v_d, everywhere(q_s), everywhere(p_s), jnp.zeros((3, 128), F32)], axis=0)

        def st_copy(q):
            d = (me + q) % 8
            return rdma(st.at[par, me], st.at[par, me], st_ssem.at[q - 1], st_rsem.at[q - 1], (d // 4, d % 4))

        for q in range(1, 8):
            st_copy(q).start()

        @pl.when(j > 0)
        def _():
            merge_out(j, 1 - par)

        for q in range(1, 8):
            src = (me + 8 - q) % 8
            rdma(st.at[par, me], st.at[par, src], st_ssem.at[q - 1], st_rsem.at[q - 1], sib).wait_recv()

        alpha = st[par, 0][0:1]
        for d in range(1, 8):
            alpha = alpha + st[par, d][0:1]
        alpha = alpha * (1.0 / ELEMS)
        beta2 = jnp.zeros((1, 128), F32)
        for d in range(8):
            tile = st[par, d]
            gap = alpha - tile[1:2]
            beta2 = beta2 + (tile[3:4] - 2.0 * gap * tile[4:5] + gap * gap * tile[2:3])
        beta = jnp.sqrt(beta2 * (1.0 / ELEMS))
        betas[...] = beta
        coef[0] = alpha
        coef[1] = beta_prev[:, :HALF]
        ab_ref[j] = jnp.concatenate([alpha, beta, jnp.zeros((6, 128), F32)], axis=0)
        gap_w = wide(alpha - shift)
        beta_w = wide(beta)
        rows = pl.ds(pl.multiple_of(32 * me, 32), 32)

        def pass3(m, carry):
            for i in range(4):
                p = 4 * m + i
                v = (vb[nxt, p] - gap_w * vb[cur, p]) / beta_w
                vb[nxt, p] = v
                uT[0, p, rows, :] = v[:, :HALF].astype(BF16)
                uT[1, p, rows, :] = v[:, HALF:].astype(BF16)

            for i in range(2):
                for s in (2, 0, 1, 3):
                    u_own(0, 2 * m + i, s).start()
            return carry

        @pl.when(j < STEPS - 1)
        def _():
            lax.fori_loop(0, 4, pass3, 0)
            for m in range(4):
                for s in (2, 0, 1, 3):
                    u_own(1, m, s).start()

        @pl.when((j > 0) & (j < STEPS - 1))
        def _():
            x_wait_send(1 - par)

        @pl.when(j < STEPS - 1)
        def _():
            put_out(vb.at[nxt], par)

        for q in range(1, 8):
            st_copy(q).wait_send()
        return carry

    lax.fori_loop(0, STEPS, step, 0)

    last = (STEPS - 1) % 2
    for q in range(1, 4):
        x_recv(last, q)
    out_copy(STEPS - 2).wait()
    for p, res in merged(last):
        at = pl.ds(p, 64, stride=16)
        res = res - coef[0] * osb[(STEPS - 1) % 2, at, :] - coef[1] * osb[STEPS % 2, at, :]
        osb[STEPS % 2, at, :] = res / betas[...]
    out_copy(STEPS).start()
    x_wait_send(last)
    out_copy(STEPS - 1).wait()
    out_copy(STEPS).wait()

    l_sib().wait_send()
    for i in range(3):
        w_send(i).wait_send()
    for i in range(5):
        r_send(i).wait_send()
    for i in range(4):
        for part in range(2):
            l_dir(i, part).wait_send()
        for kind in range(3):
            l_step(i, kind).wait_send()


def solution(mesh):
    def body_fn(wavefunc, left_loc, two_loc, right_loc):
        bond, phys = wavefunc.shape[0], wavefunc.shape[1]
        wf = wavefunc.reshape(bond, phys, phys, 2, 128).transpose(0, 1, 3, 2, 4).reshape(-1, 128)
        dma = pltpu.SemaphoreType.DMA
        kry, ab, one = pl.pallas_call(
            lanczos_kernel,
            out_shape=(
                jax.ShapeDtypeStruct((STEPS + 1, 64 * PAIR, 128), F32),
                jax.ShapeDtypeStruct((STEPS, 8, 128), F32),
                jax.ShapeDtypeStruct((1, 128), F32),
            ),
            in_specs=[
                pl.BlockSpec(memory_space=pl.ANY),
                pl.BlockSpec(memory_space=pl.ANY),
                pl.BlockSpec(memory_space=pltpu.VMEM),
                pl.BlockSpec(memory_space=pl.ANY),
            ],
            out_specs=(pl.BlockSpec(memory_space=pl.ANY), pl.BlockSpec(memory_space=pltpu.VMEM),
                       pl.BlockSpec(memory_space=pltpu.VMEM)),
            scratch_shapes=[
                pltpu.VMEM((8192, 128), F32),
                pltpu.VMEM((TERMS, COLS, BOND), BF16),
                pltpu.VMEM((TERMS, BOND, BOND), BF16),
                pltpu.VMEM((32, 384, 128), BF16),
                pltpu.VMEM((TERMS, BOND, BOND), BF16),
                pltpu.VMEM((4, PAIR, BOND), BF16),
                pltpu.VMEM((BOND, BOND), F32),
                pltpu.VMEM((TERMS, PAIR, COLS, HALF), BF16),
                pltpu.VMEM((2, PAIR, COLS, BLOCK * HALF), BF16),
                pltpu.VMEM((2, PAIR, BOND, HALF), BF16),
                pltpu.VMEM((PAIR, COLS, BOND), F32),
                pltpu.VMEM((3, PAIR, COLS, BOND), F32),
                pltpu.VMEM((2, 128, 128), F32),
                pltpu.VMEM((2, 8, 8, 128), F32),
                pltpu.VMEM((1, 128), F32),
                pltpu.VMEM((2, 1, 128), F32),
                pltpu.VMEM((4, 4, 64, 128), F32),
                pltpu.VMEM((2, 4, 4, 64, 128), F32),
                pltpu.VMEM((2, 64 * PAIR, 128), F32),
                dma((3,)),
                dma((3,)), dma((3,)),
                dma((5,)), dma((5,)),
                dma((9,)), dma((9,)),
                dma((3, 4)), dma((3, 4)),
                dma((12, 4)), dma((12, 4)),
                dma((12, 3)), dma((12, 3)),
                dma((7,)), dma((7,)),
                dma((3,)), dma((2, 3)),
                dma((2,)),
            ],
            compiler_params=pltpu.CompilerParams(
                collective_id=0, has_side_effects=True, vmem_limit_bytes=66 * 1000 * 1000),
        )(wf, left_loc, two_loc, right_loc)
        kry = kry * one
        krylov = kry.reshape(STEPS + 1, 64, phys, phys, 128)
        return krylov, ab[:, 0, 0], ab[:, 1, 0]

    return jax.shard_map(
        body_fn, mesh=mesh,
        in_specs=(P(), P('terms'), P('terms'), P('terms', 'rows')),
        out_specs=(P(None, 'terms', None, None, 'rows'), P(), P()), check_vma=False)
```

```python
import jax
import jax.numpy as jnp
from jax import lax
from jax.experimental import pallas as pl
from jax.experimental.pallas import tpu as pltpu
from jax.sharding import PartitionSpec as P

STEPS = 6
PAIR = 16
BOND = 256
TERMS = 64
BLOCK = 16
HALF = 128
COLS = 32
ELEMS = float(BOND * BOND * PAIR)
F32 = jnp.float32
BF16 = jnp.bfloat16


def lanczos_kernel(
    wf_hbm, left_hbm, two_ref, right_hbm, kry_hbm, ab_ref, one_ref,
    wfv, rw, lw, lx, bd, wt, mask, yb, zb, uT, acc, vb, tmp, st, betas, coef, xs, xr, osb,
    loc_sem, w_ssem, w_rsem, r_ssem, r_rsem, l_ssem, l_rsem, lx_ssem, lx_rsem,
    u_ssem, u_rsem, f_ssem, f_rsem, st_ssem, st_rsem, x_ssem, x_rsem, o_sem,
):
    y = lax.axis_index("rows")
    t = lax.axis_index("terms")
    x = t // 2
    c = t % 2
    me = y * 4 + t
    sib = (y, 2 * x + (1 - c))
    xnb = (y, 2 * (1 - x) + c)
    xno = (y, 2 * (1 - x) + (1 - c))
    ynb = (1 - y, t)
    diag = (1 - y, 2 * (1 - x) + c)
    flip = 1 - 2 * c
    near = (4 * y + 2 * (1 - x) + c, 4 * (1 - y) + t, 4 * (1 - y) + 2 * (1 - x) + c)

    def rdma(src, dst, ssem, rsem, dev):
        return pltpu.make_async_remote_copy(
            src_ref=src, dst_ref=dst, send_sem=ssem, recv_sem=rsem,
            device_id=dev, device_id_type=pl.DeviceIdType.MESH)

    cp_wf = pltpu.make_async_copy(wf_hbm, wfv, loc_sem.at[0])
    cp_r = pltpu.make_async_copy(right_hbm.at[:, pl.ds(32 * t, 32), :], rw.at[pl.ds(0, 16)], loc_sem.at[1])
    cp_l = pltpu.make_async_copy(left_hbm, lw.at[pl.ds(0, 16)], loc_sem.at[2])
    cp_wf.start()
    cp_r.start()
    cp_l.start()

    barrier = pltpu.get_barrier_semaphore()
    for q in range(1, 8):
        d = (me + q) % 8
        pl.semaphore_signal(barrier, inc=1, device_id=(d // 4, d % 4), device_id_type=pl.DeviceIdType.MESH)
    pl.semaphore_wait(barrier, 7)

    def l_sib():
        return rdma(left_hbm, lw.at[pl.ds(16, 16)], l_ssem.at[0], l_rsem.at[0], sib)

    def l_dir(i, part):
        rows = pl.ds(0, 256) if part == 0 else pl.ds(128, 128)
        return rdma(left_hbm.at[pl.ds(8 * y + 2 * i, 2), rows, pl.ds(128 * part, 128)],
                    lx.at[pl.ds(2 * i, 2), pl.ds(256 * part, 256 - 128 * part), :],
                    l_ssem.at[1 + 2 * i + part], l_rsem.at[1 + 2 * i + part], xnb)

    def l_step(i, kind):
        src, dst, dev = ((0, 8, sib), (0, 16, ynb), (16, 24, sib))[kind]
        return rdma(lx.at[pl.ds(src + 2 * i, 2)], lx.at[pl.ds(dst + 2 * i, 2)],
                    lx_ssem.at[kind, i], lx_rsem.at[kind, i], dev)

    def l_take(i):
        for part in range(2):
            l_dir(i, part).wait_recv()
        l_step(i, 0).start()
        l_step(i, 1).start()

    def l_unpack(k, s):
        src = 16 * (s - 2) + k
        dst = 16 * s + k
        low = lx[src, pl.ds(128, 128), :]
        lw[dst, pl.ds(0, 128), pl.ds(0, 128)] = lx[src, pl.ds(0, 128), :]
        lw[dst, pl.ds(128, 128), pl.ds(0, 128)] = low
        lw[dst, pl.ds(0, 128), pl.ds(128, 128)] = low.astype(F32).T.astype(BF16)
        lw[dst, pl.ds(128, 128), pl.ds(128, 128)] = lx[src, pl.ds(256, 128), :]
        return s

    def r_send(i):
        first, rows, dst, dev = (
            (0, 2 * x + (1 - c), 16, sib),
            (8 * y, 2 * (1 - x) + c, 32, xnb),
            (8 * y, 2 * (1 - x) + (1 - c), 40, xno),
            (8 * (1 - y), 2 * (1 - x) + c, 48, xnb),
            (8 * (1 - y), 2 * (1 - x) + (1 - c), 56, xno),
        )[i]
        n = 16 if i == 0 else 8
        return rdma(right_hbm.at[pl.ds(first, n), pl.ds(32 * rows, 32), :], rw.at[pl.ds(dst, n)],
                    r_ssem.at[i], r_rsem.at[i], dev)

    for i in range(4):
        for part in range(2):
            l_dir(i, part).start()
    for i in range(5):
        r_send(i).start()
    l_sib().start()

    row16 = lax.broadcasted_iota(jnp.int32, (PAIR, BOND), 0)
    lane16 = lax.broadcasted_iota(jnp.int32, (PAIR, BOND), 1)
    packed = jnp.zeros((PAIR, BOND), F32)
    for k in range(16):
        place = (lane16 == row16 + 16 * k).astype(F32).astype(BF16)
        packed = packed + jnp.dot(two_ref[k], place, preferred_element_type=F32)
    wt[0] = packed.astype(BF16)

    def w_send(i):
        return rdma(wt.at[0], wt.at[1 + i], w_ssem.at[i], w_rsem.at[i], (sib, xnb, xno)[i])

    for i in range(3):
        w_send(i).start()

    rr = lax.broadcasted_iota(jnp.int32, (BOND, BOND), 0) % 16
    cc = lax.broadcasted_iota(jnp.int32, (BOND, BOND), 1) % 16
    mask[...] = (rr == cc).astype(F32)

    cp_wf.wait()

    def sumsq(i, s):
        blk = wfv[pl.ds(pl.multiple_of(i * 256, 256), 256), :]
        return s + jnp.sum((blk * blk).reshape(32, 8, 128), axis=0)

    total = lax.fori_loop(0, 32, sumsq, jnp.zeros((8, 128), F32))
    total = jnp.sum(jnp.sum(total, axis=1, keepdims=True), axis=0, keepdims=True)
    scale = jnp.broadcast_to(jnp.sqrt(total * (1.0 / ELEMS)), (1, 128))

    wfo = wfv.at[pl.ds(pl.multiple_of(2048 * t, 2048), 2048), :]
    own = pl.ds(pl.multiple_of(32 * t, 32), 32)
    for p in range(PAIR):
        for h in range(2):
            for bt in range(2):
                first = 4096 * h + (p // 4) * 8 + bt * 4 + p % 4
                blk = (wfv[pl.ds(first, 128, stride=32), :] / scale).T
                tmp[bt] = blk
                uT[h, p, pl.ds(128 * bt, 128), :] = blk.astype(BF16)
            vb[0, p, :, pl.ds(128 * h, 128)] = tmp[y, own, :]
        first = (p // 4) * 8 + p % 4
        lo = wfo[pl.ds(first, 64, stride=32), :]
        hi = wfo[pl.ds(first + 4, 64, stride=32), :]
        osb[0, pl.ds(p, 64, stride=16), :] = jnp.where(y == 0, lo, hi) / scale
    vb[2] = jnp.zeros((PAIR, COLS, BOND), F32)
    betas[...] = jnp.zeros((1, 128), F32)
    one_ref[...] = jnp.ones((1, 128), F32)

    def out_copy(j):
        return pltpu.make_async_copy(osb.at[j % 2], kry_hbm.at[j], o_sem.at[j % 2])

    out_copy(0).start()

    def u_part(h, m, dev):
        return uT.at[h, pl.ds(4 * m, 4), pl.ds(pl.multiple_of(32 * dev, 32), 32), :]

    def u_own(h, m, s):
        part = u_part(h, m, me)
        return rdma(part, part, u_ssem.at[h, m, s], u_rsem.at[h, m, s], (xnb, ynb, diag, sib)[s])

    def u_got(h, m, s):
        part = u_part(h, m, (near + (me + flip,))[s])
        return rdma(part, part, u_ssem.at[h, m, s], u_rsem.at[h, m, s], (xnb, ynb, diag, sib)[s])

    def u_relay(h, m, s):
        part = u_part(h, m, near[s])
        return rdma(part, part, f_ssem.at[h, m, s], f_rsem.at[h, m, s], sib)

    def u_relayed(h, m, s):
        part = u_part(h, m, near[s] + flip)
        return rdma(part, part, f_ssem.at[h, m, s], f_rsem.at[h, m, s], sib)

    def relay_all(h, m):
        for s in range(3):
            u_got(h, m, s).wait_recv()
            u_relay(h, m, s).start()

    def r_stage(h, k0, nk, n):
        lhs = rw[pl.ds(k0, nk)].reshape(nk * COLS, BOND)
        rhs = jnp.concatenate([uT[h, 2 * n], uT[h, 2 * n + 1]], axis=1)
        res = jnp.dot(lhs, rhs, preferred_element_type=F32).astype(BF16)
        yb[pl.ds(k0, nk), 2 * n] = res[:, :HALF].reshape(nk, COLS, HALF)
        yb[pl.ds(k0, nk), 2 * n + 1] = res[:, HALF:].reshape(nk, COLS, HALF)

    def wl_stage(h, s, buf=0):
        k0 = s * BLOCK
        for k in range(BLOCK):
            rhs = jnp.concatenate(
                [yb[k0 + k, :, pl.ds(16 * i, 16), :].reshape(BOND, HALF) for i in range(2)], axis=1)
            res = jnp.dot(bd[k0 + k], rhs, preferred_element_type=F32).astype(BF16)
            for i in range(2):
                zb[buf, :, pl.ds(16 * i, 16), pl.ds(HALF * k, HALF)] = (
                    res[:, HALF * i:HALF * (i + 1)].reshape(PAIR, 16, HALF))
        lhs = zb[buf].reshape(PAIR * COLS, BLOCK * HALF)
        rhs = lw[pl.ds(k0, BLOCK), pl.ds(pl.multiple_of(HALF * h, HALF), HALF), :].reshape(BLOCK * HALF, BOND)
        res = jnp.dot(lhs, rhs, preferred_element_type=F32)
        acc[...] = acc[...] + res.reshape(PAIR, COLS, BOND)

    def build_bd(g):
        slot = (g // 4) * 2 + (1 - g // 4) * (g // 2) + (g // 4) * (g % 2)
        part = (1 - g // 4) * (g % 2) + (g // 4) * ((y + (g - 4 * (g // 4)) // 2) % 2)
        lanes = pl.multiple_of(128 * part, 128)
        ops = wt[slot, :, pl.ds(lanes, 128)].astype(F32).T.astype(BF16)
        e_t = (lax.broadcasted_iota(jnp.int32, (PAIR, BOND), 1) // 16
               == lax.broadcasted_iota(jnp.int32, (PAIR, BOND), 0)).astype(F32).astype(BF16)
        e = (lax.broadcasted_iota(jnp.int32, (BOND, PAIR), 0) // 16
             == lax.broadcasted_iota(jnp.int32, (BOND, PAIR), 1)).astype(F32).astype(BF16)
        wide = jnp.dot(ops, e_t, preferred_element_type=F32).astype(BF16)
        for k in range(8):
            full = jnp.dot(e, wide[16 * k:16 * (k + 1), :], preferred_element_type=F32)
            bd[g * 8 + k] = (full * mask[...]).astype(BF16)

    def bd_group(i, s):
        build_bd(2 * s + i)
        return s

    def first_block(s, carry):
        @pl.when(s == 0)
        def _():
            cp_r.wait()
            cp_l.wait()

        @pl.when(s == 1)
        def _():
            w_send(0).wait_recv()
            r_send(0).wait_recv()
            l_sib().wait_recv()

        @pl.when(s == 2)
        def _():
            w_send(1).wait_recv()
            w_send(2).wait_recv()

        for i in range(1, 3):
            @pl.when(s == i)
            def _(i=i):
                l_take(i)

        @pl.when(s == 3)
        def _():
            for i in range(4):
                l_step(i, 1).wait_recv()
                l_step(i, 2).start()

        lax.fori_loop(0, 2, bd_group, s)

        @pl.when(s == 0)
        def _():
            l_take(0)

        @pl.when(s == 2)
        def _():
            l_take(3)
            for i in range(4):
                l_step(i, 0).wait_recv()
            lax.fori_loop(0, 16, l_unpack, s)
            r_send(1).wait_recv()
            r_send(2).wait_recv()

        @pl.when(s == 3)
        def _():
            for i in range(4):
                l_step(i, 2).wait_recv()
            lax.fori_loop(0, 16, l_unpack, s)
            r_send(3).wait_recv()
            r_send(4).wait_recv()

        def half(h, carry):
            for n in range(8):
                r_stage(h, s * BLOCK, BLOCK, n)
            wl_stage(h, s)
            return carry

        lax.fori_loop(0, 2, half, 0)
        return carry

    def gather_r(i, carry):
        @pl.when(i < 4)
        def _():
            relay_all(0, i)

        @pl.when(i >= 1)
        def _():
            later_r(0, i - 1)

        return carry

    def later_r(h, m):
        u_got(h, m, 3).wait_recv()
        for s in range(3):
            u_relayed(h, m, s).wait_recv()
        for n in range(2):
            r_stage(h, 0, TERMS, 2 * m + n)

    def gather_wl(s, carry):
        relay_all(1, s)
        wl_stage(0, s)
        return carry

    def second_r(m, carry):
        later_r(1, m)
        for h in range(2):
            for s in range(4):
                u_own(h, m, s).wait_send()
            for s in range(3):
                u_relay(h, m, s).wait_send()
        return carry

    def x_copy(par, q):
        dest = (t + q) % 4
        return rdma(xs.at[dest], xr.at[par, t], x_ssem.at[q - 1], x_rsem.at[par, q - 1], (y, dest))

    def x_recv(par, q):
        rdma(xs.at[0], xr.at[par, (t + 4 - q) % 4], x_ssem.at[q - 1], x_rsem.at[par, q - 1], sib).wait_recv()

    def put_out(vec, par):
        for d in range(2):
            for i in range(4):
                blk = jnp.concatenate(
                    [vec[4 * i + k, :, pl.ds(128 * d, 128)] for k in range(4)], axis=0).T
                xs[2 * d, i] = blk[:64]
                xs[2 * d + 1, i] = blk[64:]
        xr[par, t] = xs[t]

    def x_start(par):
        for q in range(1, 4):
            x_copy(par, q).start()

    def x_wait_send(par):
        for q in range(1, 4):
            x_copy(par, q).wait_send()

    def merged(par):
        seg = lax.broadcasted_iota(jnp.int32, (64, 128), 1) // 32
        for i in range(4):
            parts = [xr[par, src, i] for src in range(4)]
            for k in range(4):
                res = parts[k]
                for src in range(4):
                    if src != k:
                        res = jnp.where(seg == src, pltpu.roll(parts[src], (32 * (src - k)) % 128, 1), res)
                yield 4 * i + k, res

    def merge_out(j, par):
        for q in range(1, 4):
            x_recv(par, q)

        @pl.when(j > 1)
        def _():
            out_copy(j - 2).wait()

        for p, res in merged(par):
            osb[j % 2, pl.ds(p, 64, stride=16), :] = res
        out_copy(j).start()

    def everywhere(s):
        s = jnp.sum(jnp.sum(s, axis=1, keepdims=True), axis=0, keepdims=True)
        return jnp.broadcast_to(s, (1, 128))

    def fold(v):
        v = v[:, :HALF] + v[:, HALF:]
        return jnp.sum(v.reshape(COLS // 8, 8, 128), axis=0)

    def wide(row):
        return jnp.concatenate([row, row], axis=1)

    def step(j, carry):
        acc[...] = jnp.zeros((PAIR, COLS, BOND), F32)

        @pl.when(j == 0)
        def _():
            lax.fori_loop(0, 4, first_block, 0)

        @pl.when(j > 0)
        def _():
            lax.fori_loop(0, 5, gather_r, 0)
            lax.fori_loop(0, 4, gather_wl, 0)
            x_start((j + 1) % 2)
            lax.fori_loop(0, 4, second_r, 0)
            for s in range(4):
                wl_stage(1, s, s % 2)

        cur = j % 3
        prev = (j + 2) % 3
        nxt = (j + 1) % 3
        par = j % 2

        @pl.when(j == STEPS - 1)
        def _():
            x_wait_send(1 - par)
            put_out(acc, par)
            x_start(par)

        beta_prev = wide(betas[...])
        zero = jnp.zeros((8, 128), F32)

        def pass1(p, s):
            a_s, t_s, v_s = s
            w = acc[p]
            v = vb[cur, p]
            r = w - beta_prev * vb[prev, p]
            vb[nxt, p] = r
            return a_s + fold(w * v), t_s + fold(r * v), v_s + fold(v * v)

        a_s, t_s, v_s = lax.fori_loop(0, PAIR, pass1, (zero, zero, zero))
        a_d, t_d, v_d = everywhere(a_s), everywhere(t_s), everywhere(v_s)
        shift = jnp.where(v_d > 0.0, t_d / jnp.where(v_d > 0.0, v_d, 1.0), 0.0)
        shift_w = wide(shift)

        def pass2(p, s):
            q_s, p_s = s
            v = vb[cur, p]
            r = vb[nxt, p] - shift_w * v
            vb[nxt, p] = r
            return q_s + fold(r * r), p_s + fold(r * v)

        q_s, p_s = lax.fori_loop(0, PAIR, pass2, (zero, zero))
        st[par, me] = jnp.concatenate(
            [a_d, shift, v_d, everywhere(q_s), everywhere(p_s), jnp.zeros((3, 128), F32)], axis=0)

        def st_copy(q):
            d = (me + q) % 8
            return rdma(st.at[par, me], st.at[par, me], st_ssem.at[q - 1], st_rsem.at[q - 1], (d // 4, d % 4))

        for q in range(1, 8):
            st_copy(q).start()

        @pl.when(j > 0)
        def _():
            merge_out(j, 1 - par)

        for q in range(1, 8):
            src = (me + 8 - q) % 8
            rdma(st.at[par, me], st.at[par, src], st_ssem.at[q - 1], st_rsem.at[q - 1], sib).wait_recv()

        alpha = st[par, 0][0:1]
        for d in range(1, 8):
            alpha = alpha + st[par, d][0:1]
        alpha = alpha * (1.0 / ELEMS)
        beta2 = jnp.zeros((1, 128), F32)
        for d in range(8):
            tile = st[par, d]
            gap = alpha - tile[1:2]
            beta2 = beta2 + (tile[3:4] - 2.0 * gap * tile[4:5] + gap * gap * tile[2:3])
        beta = jnp.sqrt(beta2 * (1.0 / ELEMS))
        betas[...] = beta
        coef[0] = alpha
        coef[1] = beta_prev[:, :HALF]
        ab_ref[j] = jnp.concatenate([alpha, beta, jnp.zeros((6, 128), F32)], axis=0)
        gap_w = wide(alpha - shift)
        beta_w = wide(beta)
        rows = pl.ds(pl.multiple_of(32 * me, 32), 32)

        def pass3(m, carry):
            for i in range(4):
                p = 4 * m + i
                v = (vb[nxt, p] - gap_w * vb[cur, p]) / beta_w
                vb[nxt, p] = v
                uT[0, p, rows, :] = v[:, :HALF].astype(BF16)
                uT[1, p, rows, :] = v[:, HALF:].astype(BF16)

            for s in (2, 0, 1, 3):
                u_own(0, m, s).start()
            return carry

        @pl.when(j < STEPS - 1)
        def _():
            lax.fori_loop(0, 4, pass3, 0)
            for m in range(4):
                for s in (2, 0, 1, 3):
                    u_own(1, m, s).start()

        @pl.when((j > 0) & (j < STEPS - 1))
        def _():
            x_wait_send(1 - par)

        @pl.when(j < STEPS - 1)
        def _():
            put_out(vb.at[nxt], par)

        for q in range(1, 8):
            st_copy(q).wait_send()
        return carry

    lax.fori_loop(0, STEPS, step, 0)

    last = (STEPS - 1) % 2
    for q in range(1, 4):
        x_recv(last, q)
    out_copy(STEPS - 2).wait()
    for p, res in merged(last):
        at = pl.ds(p, 64, stride=16)
        res = res - coef[0] * osb[(STEPS - 1) % 2, at, :] - coef[1] * osb[STEPS % 2, at, :]
        osb[STEPS % 2, at, :] = res / betas[...]
    out_copy(STEPS).start()
    x_wait_send(last)
    out_copy(STEPS - 1).wait()
    out_copy(STEPS).wait()

    l_sib().wait_send()
    for i in range(3):
        w_send(i).wait_send()
    for i in range(5):
        r_send(i).wait_send()
    for i in range(4):
        for part in range(2):
            l_dir(i, part).wait_send()
        for kind in range(3):
            l_step(i, kind).wait_send()


def solution(mesh):
    def body_fn(wavefunc, left_loc, two_loc, right_loc):
        bond, phys = wavefunc.shape[0], wavefunc.shape[1]
        wf = wavefunc.reshape(bond, phys, phys, 2, 128).transpose(0, 1, 3, 2, 4).reshape(-1, 128)
        dma = pltpu.SemaphoreType.DMA
        kry, ab, one = pl.pallas_call(
            lanczos_kernel,
            out_shape=(
                jax.ShapeDtypeStruct((STEPS + 1, 64 * PAIR, 128), F32),
                jax.ShapeDtypeStruct((STEPS, 8, 128), F32),
                jax.ShapeDtypeStruct((1, 128), F32),
            ),
            in_specs=[
                pl.BlockSpec(memory_space=pl.ANY),
                pl.BlockSpec(memory_space=pl.ANY),
                pl.BlockSpec(memory_space=pltpu.VMEM),
                pl.BlockSpec(memory_space=pl.ANY),
            ],
            out_specs=(pl.BlockSpec(memory_space=pl.ANY), pl.BlockSpec(memory_space=pltpu.VMEM),
                       pl.BlockSpec(memory_space=pltpu.VMEM)),
            scratch_shapes=[
                pltpu.VMEM((8192, 128), F32),
                pltpu.VMEM((TERMS, COLS, BOND), BF16),
                pltpu.VMEM((TERMS, BOND, BOND), BF16),
                pltpu.VMEM((32, 384, 128), BF16),
                pltpu.VMEM((TERMS, BOND, BOND), BF16),
                pltpu.VMEM((4, PAIR, BOND), BF16),
                pltpu.VMEM((BOND, BOND), F32),
                pltpu.VMEM((TERMS, PAIR, COLS, HALF), BF16),
                pltpu.VMEM((2, PAIR, COLS, BLOCK * HALF), BF16),
                pltpu.VMEM((2, PAIR, BOND, HALF), BF16),
                pltpu.VMEM((PAIR, COLS, BOND), F32),
                pltpu.VMEM((3, PAIR, COLS, BOND), F32),
                pltpu.VMEM((2, 128, 128), F32),
                pltpu.VMEM((2, 8, 8, 128), F32),
                pltpu.VMEM((1, 128), F32),
                pltpu.VMEM((2, 1, 128), F32),
                pltpu.VMEM((4, 4, 64, 128), F32),
                pltpu.VMEM((2, 4, 4, 64, 128), F32),
                pltpu.VMEM((2, 64 * PAIR, 128), F32),
                dma((3,)),
                dma((3,)), dma((3,)),
                dma((5,)), dma((5,)),
                dma((9,)), dma((9,)),
                dma((3, 4)), dma((3, 4)),
                dma((2, 4, 4)), dma((2, 4, 4)),
                dma((2, 4, 3)), dma((2, 4, 3)),
                dma((7,)), dma((7,)),
                dma((3,)), dma((2, 3)),
                dma((2,)),
            ],
            compiler_params=pltpu.CompilerParams(
                collective_id=0, has_side_effects=True, vmem_limit_bytes=66 * 1000 * 1000),
        )(wf, left_loc, two_loc, right_loc)
        kry = kry * one
        krylov = kry.reshape(STEPS + 1, 64, phys, phys, 128)
        return krylov, ab[:, 0, 0], ab[:, 1, 0]

    return jax.shard_map(
        body_fn, mesh=mesh,
        in_specs=(P(), P('terms'), P('terms'), P('terms', 'rows')),
        out_specs=(P(None, 'terms', None, None, 'rows'), P(), P()), check_vma=False)
```
